128 devices in a mesh: graph: 1, col: 16 (over z, y), row: 8 (over x, core).
Axes of the slice: x: 4, y: 4, z: 4, core: 2. Of those that a mesh axis runs over, the one named last changes fastest.
Arguments:
- flow_init: float32 [8192, 8192], P(('graph', 'row'), 'col')
- flow_graph: float32 [8192, 8192], P(('graph', 'row'), 'col')
Outputs:
- output: float32 [8192, 8192], P(('graph', 'row'), 'col')
All inputs are finite; a program needn't handle non-finite values.
Results may differ from the reference program's by a relative error of at most 0.001.
Values are sent between devices in bfloat16 or wider.
A program may use at most 1 GiB of HBM per device.

```python
import jax
import jax.numpy as jnp
from jax import lax

N = 8192
ITERATIONS = 3


def draw_flow(key, floor_level):
    key_width, key_noise = jax.random.split(key)
    node_index = jnp.arange(N, dtype=jnp.float32)
    band_width = N * jax.random.uniform(key_width, (N,), minval=0.01, maxval=0.15)
    raw_offset = jnp.abs(node_index[:, None] - node_index[None, :])
    cyclic_dist = jnp.minimum(raw_offset, N - raw_offset)
    noise_fac = jax.random.uniform(key_noise, (N, N), minval=0.5, maxval=1.5)
    weight = (floor_level + jnp.exp(-cyclic_dist / band_width[None, :])) * noise_fac
    return weight / jnp.sum(weight, axis=0, keepdims=True)


def setup_inputs(seed: int = 0, part: int = 0) -> dict:
    key = jax.random.fold_in(jax.random.key(seed), part)
    key_init, key_graph = jax.random.split(key)
    flow_init = N * draw_flow(key_init, 0.05)
    flow_graph = draw_flow(key_graph, 0.1)
    return {"flow_init": flow_init.astype(jnp.float32), "flow_graph": flow_graph.astype(jnp.float32)}


def reference(flow_init, flow_graph):
    graph_bf = flow_graph.astype(jnp.bfloat16)

    def iteration(flow_cur, unused):
        expanded = jnp.dot(flow_cur.astype(jnp.bfloat16), graph_bf, preferred_element_type=jnp.float32)
        inflated = expanded * expanded
        col_sum = jnp.sum(inflated, axis=0)
        return inflated * (N / col_sum), None

    flow_out, _ = lax.scan(iteration, flow_init, None, length=ITERATIONS)
    return flow_out
```

```python
import functools

import jax
import jax.numpy as jnp
from jax import lax
from jax.experimental import pallas as pl
from jax.experimental.pallas import tpu as pltpu
from jax.sharding import PartitionSpec as P

MESH = pl.DeviceIdType.MESH
BF = jnp.bfloat16
F32 = jnp.float32
N = 8192
PLANE, PIECE, BLK, ROWS, LANE = 2048, 1024, 512, 256, 128
XM, XP, YP = 224, 448, 736
ROWS3 = ((0, 64), (64, 64), (128, 64), (192, 64))


def mcl_kernel(
    init_ref, graph_ref, out_ref,
    g, a, stage, acc1, acc2, moved, got, s1a, s2a, s1b, s2b,
    g_send, g_recv, d_recv, t_send, t_recv, az_send, az_recv, az2_recv,
    a1_send, a1_recv, a1_recv2, a2_send, a2_recv, a2_recv2,
    r_send, r_recv1, r_recv2, o_send, o_recv,
):
    col, row = lax.axis_index("col"), lax.axis_index("row")
    z, y = lax.div(col, 4), lax.rem(col, 4)
    x, c = lax.div(row, 2), lax.rem(row, 2)

    def plus(v, d):
        return lax.rem(v + d, 4)

    def dev(dx=0, dy=0, dz=0, dc=0):
        return {"col": plus(z, dz) * 4 + plus(y, dy), "row": plus(x, dx) * 2 + lax.rem(c + dc, 2)}

    XPOS, XNEG, YPOS, YNEG = dev(dx=1), dev(dx=3), dev(dy=1), dev(dy=3)
    ZPOS, ZNEG, MATE = dev(dz=1), dev(dz=3), dev(dc=1)

    def send(src, dst, ssem, rsem, device):
        pltpu.make_async_remote_copy(
            src_ref=src, dst_ref=dst, send_sem=ssem, recv_sem=rsem, device_id=device, device_id_type=MESH
        ).start()

    def await_recv(ref, sem):
        pltpu.make_async_remote_copy(
            src_ref=ref, dst_ref=ref, send_sem=sem, recv_sem=sem, device_id=MATE, device_id_type=MESH
        ).wait_recv()

    def await_send(ref, sem):
        pltpu.make_async_remote_copy(
            src_ref=ref, dst_ref=ref, send_sem=sem, recv_sem=sem, device_id=MATE, device_id_type=MESH
        ).wait_send()

    barrier = pltpu.get_barrier_semaphore()
    peers = [dev(dx=dx, dc=dc) for dx in range(4) for dc in range(2) if (dx, dc) != (0, 0)]
    peers += [dev(dy=dy) for dy in (1, 2, 3)] + [ZPOS, ZNEG]
    for peer in peers:
        pl.semaphore_signal(barrier, inc=1, device_id=peer, device_id_type=MESH)

    def cast_graph(q):
        base = pl.multiple_of((x * 2 + c) * PIECE, PIECE)
        for qr in range(4):
            for yy in range(2):
                g[q, y, pl.ds(base + qr * ROWS + yy * LANE, LANE), :] = graph_ref[
                    pl.ds(yy * BLK + qr * LANE, LANE), pl.ds(q * LANE, LANE)
                ].astype(BF)

    own_rows = pl.ds(pl.multiple_of(y * ROWS, ROWS), ROWS)
    for q in range(4):
        a[0, z, lax.div(y, 2), q, lax.rem(y, 2)] = init_ref[own_rows, pl.ds(q * LANE, LANE)].astype(BF)
    for t in range(4):
        for q in range(4):
            stage[t, q] = init_ref[pl.ds(t * ROWS, ROWS), pl.ds(q * LANE, LANE)].astype(BF)
    cast_graph(0)
    pl.semaphore_wait(barrier, len(peers))

    def a0_block(dz, dy, lo=0, n=4):
        yy = plus(y, dy)
        return a.at[0, plus(z, dz), lax.div(yy, 2), pl.ds(lo, n), lax.rem(yy, 2)]

    def a0_spread(group, dys):
        for dy in dys:
            for where in (ZPOS, ZNEG):
                send(a0_block(0, dy), a0_block(0, dy), az_send, az_recv.at[group], where)

    def a0_relay(group, dys):
        await_recv(a.at[0, 0, pl.ds(0, len(dys))], az_recv.at[group])
        for dy in dys:
            send(a0_block(3, dy, 0, 2), a0_block(3, dy, 0, 2), az_send, az2_recv, ZPOS)
            send(a0_block(1, dy, 2, 2), a0_block(1, dy, 2, 2), az_send, az2_recv, ZNEG)

    def a0_exchange():
        for dy in (1, 3, 2):
            send(stage.at[plus(y, dy)], a0_block(0, 0), t_send, t_recv.at[dy - 1], dev(dy=dy))

    def piece(q, dx, dy, lo=0, hi=PIECE):
        base = (plus(x, dx) * 2 + c) * PIECE
        return g.at[q, plus(y, dy), pl.ds(pl.multiple_of(base + lo, 32), hi - lo), :]

    def hop(q, depth, where, dx, dy, lo=0, hi=PIECE):
        ref = piece(q, dx, dy, lo, hi)
        send(ref, ref, g_send.at[q], g_recv.at[q, depth], where)

    def mate(q, *offsets):
        for dx, dy in offsets:
            ref = piece(q, dx, dy)
            send(ref, ref, g_send.at[q], d_recv.at[q], MATE)

    def arrived(q, depth):
        rows = (4096, 2 * (BLK + 2 * (PIECE - XP)) + 2 * (BLK + 2 * XP), 4096, PIECE)[depth]
        await_recv(g.at[q, 0, pl.ds(0, rows), :], g_recv.at[q, depth])

    def g1(q):
        for where in (XPOS, XNEG, YPOS, YNEG):
            hop(q, 0, where, 0, 0)
        mate(q, (0, 0))

    def g2(q):
        arrived(q, 0)
        hop(q, 1, XPOS, 3, 0, XM, YP)
        hop(q, 1, YPOS, 0, 3, XM, YP)
        for lo, hi in ((0, XM), (YP, PIECE)):
            hop(q, 1, XNEG, 1, 0, lo, hi)
            hop(q, 1, YNEG, 0, 1, lo, hi)
        for d in (1, 3):
            for where in (XPOS, XNEG):
                hop(q, 1, where, 0, d, XP, PIECE)
            for where in (YPOS, YNEG):
                hop(q, 1, where, d, 0, 0, XP)
        mate(q, (1, 0), (3, 0), (0, 1), (0, 3))

    def g3(q):
        arrived(q, 1)
        for where in (XPOS, XNEG):
            hop(q, 2, where, 0, 2, XP, PIECE)
        for where in (YPOS, YNEG):
            hop(q, 2, where, 2, 0, 0, XP)
        for d in (1, 3):
            hop(q, 2, XPOS, 3, d, XP, YP)
            hop(q, 2, XNEG, 1, d, YP, PIECE)
            hop(q, 2, YPOS, d, 3, XM, XP)
            hop(q, 2, YNEG, d, 1, 0, XM)
        mate(q, (2, 0), (0, 2), (1, 1), (1, 3), (3, 1), (3, 3))

    def g4(q):
        arrived(q, 2)
        hop(q, 3, XPOS, 3, 2, XP, YP)
        hop(q, 3, XNEG, 1, 2, YP, PIECE)
        hop(q, 3, YPOS, 2, 3, XM, XP)
        hop(q, 3, YNEG, 2, 1, 0, XM)
        mate(q, (1, 2), (3, 2), (2, 1), (2, 3))

    def g5(q):
        arrived(q, 3)
        mate(q, (2, 2))

    def g_whole(q):
        await_recv(g.at[q, pl.ds(0, 2)], d_recv.at[q])

    def g_rows(nq, start, n):
        return jnp.concatenate([g[nq, t, pl.ds(start, n), :] for t in range(4)], axis=1)

    def c1(q):
        def step(zz, carry):
            lhs = jnp.concatenate(
                [a[0, zz, cc, qr, yy] for cc in range(2) for qr in range(4) for yy in range(2)], axis=1
            )
            prod = jnp.dot(lhs, g_rows(q, pl.multiple_of(zz * PLANE, PLANE), PLANE), preferred_element_type=F32)
            acc1[q] = jnp.where(zz == 0, prod, acc1[q] + prod)
            return carry

        acc1[q] = jnp.zeros((ROWS, BLK), F32)
        lax.fori_loop(0, 4, step, 0)

    def square_sum(ref, q):
        v = ref[q]
        return jnp.sum(v * v, axis=0, keepdims=True)

    def sum_first(s1, i, k):
        me = x * 2 + c
        for dx in range(4):
            for dc in range(2):
                if (dx, dc) != (0, 0):
                    send(s1.at[i, me], s1.at[i, me], r_send.at[0, k], r_recv1.at[k], dev(dx=dx, dc=dc))

    def sum_second(s1, s2, i, k):
        await_recv(s1.at[i, pl.ds(0, 7)], r_recv1.at[k])
        s2[i, y] = jnp.sum(s1[i], axis=0)
        for dy in (1, 2, 3):
            send(s2.at[i, y], s2.at[i, y], r_send.at[1, k], r_recv2.at[k], dev(dy=dy))

    def sum_last(s2, i, k):
        await_recv(s2.at[i, pl.ds(0, 3)], r_recv2.at[k])

    def c1_sums(q):
        s1a[q, x * 2 + c] = square_sum(acc1, q)
        sum_first(s1a, q, q)

    def c1_second(q):
        sum_second(s1a, s2a, q, q)

    def a1_chunk(dz, q, lo=0, n=2):
        return a.at[1, plus(z, dz), pl.ds(lo, n), q]

    def a1_spread(q):
        sum_last(s2a, q, q)
        scale = N / jnp.sum(s2a[q], axis=0)
        for t in range(4):
            v = acc1[q, :, pl.ds(t * LANE, LANE)]
            a[1, z, t // 2, q, t % 2] = (v * v * scale[:, t * LANE : t * LANE + LANE]).astype(BF)
        for where in (ZPOS, ZNEG):
            send(a1_chunk(0, q), a1_chunk(0, q), a1_send, a1_recv.at[q], where)

    def a1_relay(q):
        await_recv(a.at[1, 0, :, pl.ds(0, 2)], a1_recv.at[q])
        send(a1_chunk(3, q, 0, 1), a1_chunk(3, q, 0, 1), a1_send, a1_recv2.at[q], ZPOS)
        send(a1_chunk(1, q, 1, 1), a1_chunk(1, q, 1, 1), a1_send, a1_recv2.at[q], ZNEG)

    def c2(q, dz, first=False):
        zz = plus(z, dz)
        lhs = jnp.concatenate([a[1, zz, cc, q, yy] for cc in range(2) for yy in range(2)], axis=1)
        base = pl.multiple_of(zz * PLANE, PLANE)
        for nq in range(4):
            rhs = jnp.concatenate([g_rows(nq, base + cc * PIECE + q * ROWS, ROWS) for cc in range(2)], axis=0)
            prod = jnp.dot(lhs, rhs, preferred_element_type=F32)
            acc2[nq] = prod if first else acc2[nq] + prod

    def c2_near(q):
        for dz in (1, 3):
            c2(q, dz)

    def c2_far(q):
        await_recv(a.at[1, 0, :, 0], a1_recv2.at[q])
        c2(q, 2)

    def c2_sums():
        for q in range(4):
            s1b[0, x * 2 + c, :, pl.ds(q * BLK, BLK)] = square_sum(acc2, q)
        sum_first(s1b, 0, 4)

    def c2_second():
        sum_second(s1b, s2b, 0, 4)

    def a2_rows(dz, p, lo=0, n=2):
        start, rows = ROWS3[p]
        return a.at[2, plus(z, dz), pl.ds(lo, n), :, :, pl.ds(start, rows), :]

    def a2_spread(p):
        start, rows = ROWS3[p]
        scale = N / jnp.sum(s2b[0], axis=0)
        for q in range(4):
            for t in range(4):
                v = acc2[q, pl.ds(start, rows), pl.ds(t * LANE, LANE)]
                s = scale[:, q * BLK + t * LANE : q * BLK + t * LANE + LANE]
                a[2, z, t // 2, q, t % 2, pl.ds(start, rows), :] = (v * v * s).astype(BF)
        for where in (ZPOS, ZNEG):
            send(a2_rows(0, p), a2_rows(0, p), a2_send.at[p], a2_recv.at[p], where)

    def a2_relay(p):
        start, rows = ROWS3[p]
        await_recv(a.at[2, pl.ds(0, 2), :, :, :, pl.ds(start, rows), :], a2_recv.at[p])
        send(a2_rows(3, p, 0, 1), a2_rows(3, p, 0, 1), a2_send.at[p], a2_recv2.at[p], ZPOS)
        send(a2_rows(1, p, 1, 1), a2_rows(1, p, 1, 1), a2_send.at[p], a2_recv2.at[p], ZNEG)

    def c3_part(zz, start, rows, nq):
        lhs = jnp.concatenate(
            [a[2, zz, cc, qr, yy, pl.ds(start, rows), :] for cc in range(2) for qr in range(4) for yy in range(2)],
            axis=1,
        )
        return jnp.dot(lhs, g_rows(nq, pl.multiple_of(zz * PLANE, PLANE), PLANE), preferred_element_type=F32)

    def c3_own():
        def step(nq, carry):
            acc1[nq] = c3_part(z, 0, ROWS, nq)
            return carry

        lax.fori_loop(0, 4, step, 0)

    def c3_near(p):
        start, rows = ROWS3[p]

        def step(nq, carry):
            acc1[nq, pl.ds(start, rows), :] += c3_part(plus(z, 1), start, rows, nq)
            acc1[nq, pl.ds(start, rows), :] += c3_part(plus(z, 3), start, rows, nq)
            return carry

        lax.fori_loop(0, 4, step, 0)

    def c3_far(p):
        start, rows = ROWS3[p]
        await_recv(a.at[2, 0, :, :, :, pl.ds(start, rows), :], a2_recv2.at[p])
        for nq in range(4):
            v = acc1[nq, pl.ds(start, rows), :] + c3_part(plus(z, 2), start, rows, nq)
            v = v * v
            part = jnp.sum(v, axis=0, keepdims=True)
            lanes = pl.ds(nq * BLK, BLK)
            if p == 0:
                s1b[1, x * 2 + c, :, lanes] = part
            else:
                s1b[1, x * 2 + c, :, lanes] += part
            for t in range(4):
                moved[t, pl.ds(start, rows), pl.ds(nq * LANE, LANE)] = v[:, t * LANE : t * LANE + LANE]
        for dy in (2, 1, 3):
            send(
                moved.at[plus(y, dy), pl.ds(start, rows), :],
                got.at[y, pl.ds(start, rows), :],
                o_send, o_recv, dev(dy=dy),
            )

    def finish():
        await_recv(got.at[pl.ds(0, 3)], o_recv)
        for nq in range(4):
            lanes = pl.ds(pl.multiple_of(nq * BLK + y * LANE, LANE), LANE)
            scale = N / jnp.sum(s2b[1, :, :, lanes], axis=0)
            here = pl.ds(nq * LANE, LANE)
            for dy in range(4):
                t = plus(y, dy)
                v = got[t, :, here] if dy else moved[t, :, here]
                out_ref[pl.ds(pl.multiple_of(t * ROWS, ROWS), ROWS), here] = v * scale

    a0_spread(0, (0,))
    a0_exchange()
    g1(0)
    cast_graph(1)
    g1(1)
    await_recv(stage.at[0], t_recv.at[0])
    await_recv(stage.at[0], t_recv.at[2])
    a0_spread(1, (1, 3))
    await_recv(stage.at[0], t_recv.at[1])
    a0_spread(2, (2,))
    a0_relay(0, (0,))
    cast_graph(2)
    cast_graph(3)
    g2(0)
    g1(2)
    a0_relay(1, (1, 3))
    g2(1)
    g3(0)
    g1(3)
    a0_relay(2, (2,))
    g2(2)
    g3(1)
    g4(0)
    await_recv(a.at[0, 0], az2_recv)
    g5(0)
    g_whole(0)
    c1(0)
    c1_sums(0)
    g2(3)
    g3(2)
    g4(1)
    c1_second(0)
    g5(1)
    g_whole(1)
    c1(1)
    c1_sums(1)
    a1_spread(0)
    g3(3)
    g4(2)
    a1_relay(0)
    c1_second(1)
    g5(2)
    g_whole(2)
    g4(3)
    a1_spread(1)
    c1(2)
    c1_sums(2)
    a1_relay(1)
    c1_second(2)
    g5(3)
    a1_spread(2)
    g_whole(3)
    c1(3)
    c1_sums(3)
    a1_relay(2)
    c2(0, 0, first=True)
    c2(1, 0)
    c1_second(3)
    c2(2, 0)
    a1_spread(3)
    c2(3, 0)
    for q in (0, 1, 2):
        c2_near(q)
        c2_far(q)
    a1_relay(3)
    c2_near(3)
    c2_far(3)
    c2_sums()
    c2_second()
    sum_last(s2b, 0, 4)
    for p in range(4):
        a2_spread(p)
    c3_own()
    for p in range(4):
        a2_relay(p)
        c3_near(p)
        c3_far(p)
    sum_first(s1b, 1, 5)
    sum_second(s1b, s2b, 1, 5)
    sum_last(s2b, 1, 5)
    finish()

    for q in range(4):
        await_send(g.at[q, :, pl.ds(0, 7936), :], g_send.at[q])
    await_send(stage.at[pl.ds(0, 3)], t_send)
    await_send(a.at[0, pl.ds(0, 3)], az_send)
    await_send(a.at[1, pl.ds(0, 3)], a1_send)
    for p, (start, rows) in enumerate(ROWS3):
        await_send(a.at[2, pl.ds(0, 3), :, :, :, pl.ds(start, rows), :], a2_send.at[p])
    for s1, s2, base in ((s1a, s2a, 0), (s1b, s2b, 4)):
        for i in range(s1.shape[0]):
            await_send(s1.at[i, pl.ds(0, 7)], r_send.at[0, base + i])
            await_send(s2.at[i, pl.ds(0, 3)], r_send.at[1, base + i])
    await_send(got.at[pl.ds(0, 3)], o_send)


def solution(mesh):
    block_spec = P(("graph", "row"), "col")
    vmem = pl.BlockSpec(memory_space=pltpu.VMEM)
    dma = pltpu.SemaphoreType.DMA

    def device_step(init_blk, graph_blk):
        return pl.pallas_call(
            mcl_kernel,
            out_shape=jax.ShapeDtypeStruct((PIECE, BLK), F32),
            in_specs=[vmem, vmem],
            out_specs=vmem,
            scratch_shapes=[
                pltpu.VMEM((4, 4, N, LANE), BF),
                pltpu.VMEM((3, 4, 2, 4, 2, ROWS, LANE), BF),
                pltpu.VMEM((4, 4, ROWS, LANE), BF),
                pltpu.VMEM((4, ROWS, BLK), F32),
                pltpu.VMEM((4, ROWS, BLK), F32),
                pltpu.VMEM((4, ROWS, BLK), F32),
                pltpu.VMEM((4, ROWS, BLK), F32),
                pltpu.VMEM((4, 8, 1, BLK), F32),
                pltpu.VMEM((4, 4, 1, BLK), F32),
                pltpu.VMEM((2, 8, 1, PLANE), F32),
                pltpu.VMEM((2, 4, 1, PLANE), F32),
                dma((4,)), dma((4, 4)), dma((4,)),
                dma(()), dma((3,)),
                dma(()), dma((3,)), dma(()),
                dma(()), dma((4,)), dma((4,)),
                dma((4,)), dma((4,)), dma((4,)),
                dma((2, 6)), dma((6,)), dma((6,)),
                dma(()), dma(()),
            ],
            compiler_params=pltpu.CompilerParams(
                collective_id=0, has_side_effects=True, vmem_limit_bytes=67043328
            ),
        )(init_blk, graph_blk)

    return jax.shard_map(device_step, mesh=mesh, in_specs=(block_spec, block_spec), out_specs=block_spec, check_vma=False)
```

```python
import functools

import jax
import jax.numpy as jnp
from jax import lax
from jax.experimental import pallas as pl
from jax.experimental.pallas import tpu as pltpu
from jax.sharding import PartitionSpec as P

MESH = pl.DeviceIdType.MESH
BF = jnp.bfloat16
F32 = jnp.float32
N = 8192
PLANE, PIECE, BLK, ROWS, LANE = 2048, 1024, 512, 256, 128
Q = 4
Q0, Q1, Q2, Q3 = range(Q)
NEAR = (1, 3)
XM, XP, YP = 288, 448, 752
ROWS3 = ((0, 80), (80, 64), (144, 64), (208, 48))


def mcl_kernel(
    init_hbm, graph_hbm, out_hbm, scale_ref,
    init_ref, graph_ref,
    g, a, stage, acc1, acc2, moved, got, s1a, s2a, s1b, s2b,
    g_send, g_recv, d_recv, t_send, t_recv, az_send, az_recv, az2_recv,
    a1_send, a1_recv, a1_recv2, a2_send, a2_recv, a2_recv2,
    r_send, r_recv1, r_recv2, o_send, o_recv, i_sem, w_sem,
):
    col, row = lax.axis_index("col"), lax.axis_index("row")
    z, y = lax.div(col, 4), lax.rem(col, 4)
    x, c = lax.div(row, 2), lax.rem(row, 2)

    def plus(v, d):
        return lax.rem(v + d, 4)

    def dev(dx=0, dy=0, dz=0, dc=0):
        return {"col": plus(z, dz) * 4 + plus(y, dy), "row": plus(x, dx) * 2 + lax.rem(c + dc, 2)}

    XPOS, XNEG, YPOS, YNEG = dev(dx=1), dev(dx=3), dev(dy=1), dev(dy=3)
    ZPOS, ZNEG, MATE = dev(dz=1), dev(dz=3), dev(dc=1)

    def send(src, dst, ssem, rsem, device):
        pltpu.make_async_remote_copy(
            src_ref=src, dst_ref=dst, send_sem=ssem, recv_sem=rsem, device_id=device, device_id_type=MESH
        ).start()

    def await_recv(ref, sem):
        pltpu.make_async_remote_copy(
            src_ref=ref, dst_ref=ref, send_sem=sem, recv_sem=sem, device_id=MATE, device_id_type=MESH
        ).wait_recv()

    def await_send(ref, sem):
        pltpu.make_async_remote_copy(
            src_ref=ref, dst_ref=ref, send_sem=sem, recv_sem=sem, device_id=MATE, device_id_type=MESH
        ).wait_send()

    barrier = pltpu.get_barrier_semaphore()
    peers = [dev(dx=dx, dc=dc) for dx in range(Q) for dc in range(2) if (dx, dc) != (0, 0)]
    peers += [dev(dy=dy) for dy in (1, 2, 3)] + [ZPOS, ZNEG]
    for peer in peers:
        pl.semaphore_signal(barrier, inc=1, device_id=peer, device_id_type=MESH)

    copies = [pltpu.make_async_copy(init_hbm, init_ref, i_sem.at[Q])]
    for q in range(Q):
        lanes = pl.ds(q * LANE, LANE)
        copies.append(pltpu.make_async_copy(graph_hbm.at[:, lanes], graph_ref.at[:, lanes], i_sem.at[q]))
    for copy in copies:
        copy.start()

    def cast_graph(q):
        copies[q + 1].wait()
        base = pl.multiple_of((x * 2 + c) * PIECE, PIECE)
        for qr in range(Q):
            for yy in range(2):
                g[q, y, pl.ds(base + qr * ROWS + yy * LANE, LANE), :] = graph_ref[
                    pl.ds(yy * BLK + qr * LANE, LANE), pl.ds(q * LANE, LANE)
                ].astype(BF)

    copies[0].wait()
    own_rows = pl.ds(pl.multiple_of(y * ROWS, ROWS), ROWS)
    for q in range(Q):
        a[0, z, lax.div(y, 2), q, lax.rem(y, 2)] = init_ref[own_rows, pl.ds(q * LANE, LANE)].astype(BF)
    for t in range(Q):
        for q in range(Q):
            stage[t, q] = init_ref[pl.ds(t * ROWS, ROWS), pl.ds(q * LANE, LANE)].astype(BF)
    cast_graph(0)
    pl.semaphore_wait(barrier, len(peers))

    def a0_block(dz, dy, lo=0, n=4):
        yy = plus(y, dy)
        return a.at[0, plus(z, dz), lax.div(yy, 2), pl.ds(lo, n), lax.rem(yy, 2)]

    def a0_spread(group, dys):
        for dy in dys:
            for where in (ZPOS, ZNEG):
                send(a0_block(0, dy), a0_block(0, dy), az_send, az_recv.at[group], where)

    def a0_wait_near():
        for k in (0, 2):
            await_recv(stage.at[0], t_recv.at[k])

    def a0_wait_far():
        await_recv(stage.at[0], t_recv.at[1])

    def a0_done():
        await_recv(a.at[0, 0], az2_recv)

    def a0_relay(group, dys):
        await_recv(a.at[0, 0, pl.ds(0, len(dys))], az_recv.at[group])
        for dy in dys:
            send(a0_block(3, dy, 0, 2), a0_block(3, dy, 0, 2), az_send, az2_recv, ZPOS)
            send(a0_block(1, dy, 2, 2), a0_block(1, dy, 2, 2), az_send, az2_recv, ZNEG)

    def a0_exchange():
        for dy in (1, 3, 2):
            send(stage.at[plus(y, dy)], a0_block(0, 0), t_send, t_recv.at[dy - 1], dev(dy=dy))

    def piece(q, dx, dy, lo=0, hi=PIECE):
        base = (plus(x, dx) * 2 + c) * PIECE
        return g.at[q, plus(y, dy), pl.ds(pl.multiple_of(base + lo, 16), hi - lo), :]

    def hop(q, depth, where, dx, dy, lo=0, hi=PIECE):
        ref = piece(q, dx, dy, lo, hi)
        send(ref, ref, g_send.at[q], g_recv.at[q, depth], where)

    def mate(q, *offsets):
        for dx, dy in offsets:
            ref = piece(q, dx, dy)
            send(ref, ref, g_send.at[q], d_recv.at[q], MATE)

    def arrived(q, depth):
        rows = (4096, 2 * (BLK + 2 * (PIECE - XP)) + 2 * (BLK + 2 * XP), 4096, PIECE)[depth]
        await_recv(g.at[q, 0, pl.ds(0, rows), :], g_recv.at[q, depth])

    def g1(q):
        for where in (XPOS, XNEG, YPOS, YNEG):
            hop(q, 0, where, 0, 0)
        mate(q, (0, 0))

    def g2(q):
        arrived(q, 0)
        hop(q, 1, XPOS, 3, 0, XM, YP)
        hop(q, 1, YPOS, 0, 3, XM, YP)
        for lo, hi in ((0, XM), (YP, PIECE)):
            hop(q, 1, XNEG, 1, 0, lo, hi)
            hop(q, 1, YNEG, 0, 1, lo, hi)
        for d in (1, 3):
            for where in (XPOS, XNEG):
                hop(q, 1, where, 0, d, XP, PIECE)
            for where in (YPOS, YNEG):
                hop(q, 1, where, d, 0, 0, XP)
        mate(q, (1, 0), (3, 0), (0, 1), (0, 3))

    def g3(q):
        arrived(q, 1)
        for where in (XPOS, XNEG):
            hop(q, 2, where, 0, 2, XP, PIECE)
        for where in (YPOS, YNEG):
            hop(q, 2, where, 2, 0, 0, XP)
        for d in (1, 3):
            hop(q, 2, XPOS, 3, d, XP, YP)
            hop(q, 2, XNEG, 1, d, YP, PIECE)
            hop(q, 2, YPOS, d, 3, XM, XP)
            hop(q, 2, YNEG, d, 1, 0, XM)
        mate(q, (2, 0), (0, 2), (1, 1), (1, 3), (3, 1), (3, 3))

    def g4(q):
        arrived(q, 2)
        hop(q, 3, XPOS, 3, 2, XP, YP)
        hop(q, 3, XNEG, 1, 2, YP, PIECE)
        hop(q, 3, YPOS, 2, 3, XM, XP)
        hop(q, 3, YNEG, 2, 1, 0, XM)
        mate(q, (1, 2), (3, 2), (2, 1), (2, 3))

    def g5(q):
        arrived(q, 3)
        mate(q, (2, 2))

    def g_whole(q):
        await_recv(g.at[q, pl.ds(0, 2)], d_recv.at[q])

    def g_rows(nq, start, n):
        return jnp.concatenate([g[nq, t, pl.ds(start, n), :] for t in range(Q)], axis=1)

    def c1(q):
        def step(zz, carry):
            lhs = jnp.concatenate(
                [a[0, zz, cc, qr, yy] for cc in range(2) for qr in range(Q) for yy in range(2)], axis=1
            )
            prod = jnp.dot(lhs, g_rows(q, pl.multiple_of(zz * PLANE, PLANE), PLANE), preferred_element_type=F32)
            acc1[q] = jnp.where(zz == 0, prod, acc1[q] + prod)
            return carry

        acc1[q] = jnp.zeros((ROWS, BLK), F32)
        lax.fori_loop(0, 4, step, 0)

    def square_sum(ref, q):
        v = ref[q]
        return jnp.sum(v * v, axis=0, keepdims=True)

    def sum_first(s1, i, k):
        me = x * 2 + c
        for dx in range(Q):
            for dc in range(2):
                if (dx, dc) != (0, 0):
                    send(s1.at[i, me], s1.at[i, me], r_send.at[0, k], r_recv1.at[k], dev(dx=dx, dc=dc))

    def sum_second(s1, s2, i, k):
        await_recv(s1.at[i, pl.ds(0, 7)], r_recv1.at[k])
        s2[i, y] = jnp.sum(s1[i], axis=0)
        for dy in (1, 2, 3):
            send(s2.at[i, y], s2.at[i, y], r_send.at[1, k], r_recv2.at[k], dev(dy=dy))

    def sum_last(s2, i, k):
        await_recv(s2.at[i, pl.ds(0, 3)], r_recv2.at[k])

    def c1_sums(q):
        s1a[q, x * 2 + c] = square_sum(acc1, q)
        sum_first(s1a, q, q)

    def c1_second(q):
        sum_second(s1a, s2a, q, q)

    def a1_chunk(dz, q, lo=0, n=2):
        return a.at[1, plus(z, dz), pl.ds(lo, n), q]

    def a1_spread(q):
        sum_last(s2a, q, q)
        scale = N / jnp.sum(s2a[q], axis=0)
        for t in range(Q):
            v = acc1[q, :, pl.ds(t * LANE, LANE)]
            a[1, z, t // 2, q, t % 2] = (v * v * scale[:, t * LANE : t * LANE + LANE]).astype(BF)
        for half in range(2):
            for where, n in ((ZPOS, half), (ZNEG, 1 - half)):
                send(a1_chunk(0, q, n, 1), a1_chunk(0, q, n, 1), a1_send, a1_recv.at[half, q], where)

    def a1_relay(q):
        await_recv(a.at[1, 0, :, 0], a1_recv.at[0, q])
        send(a1_chunk(3, q, 0, 1), a1_chunk(3, q, 0, 1), a1_send, a1_recv2.at[q], ZPOS)
        send(a1_chunk(1, q, 1, 1), a1_chunk(1, q, 1, 1), a1_send, a1_recv2.at[q], ZNEG)

    def c2(q, dz, first=False):
        zz = plus(z, dz)
        lhs = jnp.concatenate([a[1, zz, cc, q, yy] for cc in range(2) for yy in range(2)], axis=1)
        base = pl.multiple_of(zz * PLANE, PLANE)
        for nq in range(Q):
            rhs = jnp.concatenate([g_rows(nq, base + cc * PIECE + q * ROWS, ROWS) for cc in range(2)], axis=0)
            prod = jnp.dot(lhs, rhs, preferred_element_type=F32)
            acc2[nq] = prod if first else acc2[nq] + prod

    def c2_near(q):
        await_recv(a.at[1, 0, :, 0], a1_recv.at[1, q])
        for dz in NEAR:
            c2(q, dz)

    def c2_far(q):
        await_recv(a.at[1, 0, :, 0], a1_recv2.at[q])
        c2(q, 2)

    def c2_sums():
        for q in range(Q):
            s1b[0, x * 2 + c, :, pl.ds(q * BLK, BLK)] = square_sum(acc2, q)
        sum_first(s1b, 0, 4)

    def c2_second():
        sum_second(s1b, s2b, 0, 4)

    def a2_rows(dz, p, lo=0, n=2):
        start, rows = ROWS3[p]
        return a.at[2, plus(z, dz), pl.ds(lo, n), :, :, pl.ds(start, rows), :]

    def a2_scale(p):
        start, rows = ROWS3[p]
        scale = N / jnp.sum(s2b[0], axis=0)
        for q in range(Q):
            for t in range(Q):
                v = acc2[q, pl.ds(start, rows), pl.ds(t * LANE, LANE)]
                s = scale[:, q * BLK + t * LANE : q * BLK + t * LANE + LANE]
                a[2, z, t // 2, q, t % 2, pl.ds(start, rows), :] = (v * v * s).astype(BF)

    def a2_spread(p):
        for half in range(2):
            for where, n in ((ZPOS, half), (ZNEG, 1 - half)):
                send(a2_rows(0, p, n, 1), a2_rows(0, p, n, 1), a2_send.at[p], a2_recv.at[half, p], where)

    def a2_relay(p):
        start, rows = ROWS3[p]
        await_recv(a.at[2, 0, :, :, :, pl.ds(start, rows), :], a2_recv.at[0, p])
        send(a2_rows(3, p, 0, 1), a2_rows(3, p, 0, 1), a2_send.at[p], a2_recv2.at[p], ZPOS)
        send(a2_rows(1, p, 1, 1), a2_rows(1, p, 1, 1), a2_send.at[p], a2_recv2.at[p], ZNEG)

    def c3_part(zz, start, rows, nq):
        lhs = jnp.concatenate(
            [a[2, zz, cc, qr, yy, pl.ds(start, rows), :] for cc in range(2) for qr in range(Q) for yy in range(2)],
            axis=1,
        )
        return jnp.dot(lhs, g_rows(nq, pl.multiple_of(zz * PLANE, PLANE), PLANE), preferred_element_type=F32)

    def c3_own():
        def step(nq, carry):
            acc1[nq] = c3_part(z, 0, ROWS, nq)
            return carry

        lax.fori_loop(0, 4, step, 0)

    def c3_near(p):
        start, rows = ROWS3[p]
        await_recv(a.at[2, 0, :, :, :, pl.ds(start, rows), :], a2_recv.at[1, p])

        def step(nq, carry):
            acc1[nq, pl.ds(start, rows), :] += c3_part(plus(z, 1), start, rows, nq)
            acc1[nq, pl.ds(start, rows), :] += c3_part(plus(z, 3), start, rows, nq)
            return carry

        lax.fori_loop(0, 4, step, 0)

    def c3_far(p):
        start, rows = ROWS3[p]
        await_recv(a.at[2, 0, :, :, :, pl.ds(start, rows), :], a2_recv2.at[p])
        for nq in range(Q):
            v = acc1[nq, pl.ds(start, rows), :] + c3_part(plus(z, 2), start, rows, nq)
            v = v * v
            part = jnp.sum(v, axis=0, keepdims=True)
            lanes = pl.ds(nq * BLK, BLK)
            if p == 0:
                s1b[1, x * 2 + c, :, lanes] = part
            else:
                s1b[1, x * 2 + c, :, lanes] += part
            for t in range(Q):
                moved[t, pl.ds(start, rows), pl.ds(nq * LANE, LANE)] = v[:, t * LANE : t * LANE + LANE]
        for dy in (2, 1, 3):
            send(
                moved.at[plus(y, dy), pl.ds(start, rows), :],
                got.at[y, pl.ds(start, rows), :],
                o_send, o_recv, dev(dy=dy),
            )

    def c3_sums():
        sum_first(s1b, 1, Q + 1)

    def c3_second():
        sum_second(s1b, s2b, 1, Q + 1)

    def result_out():
        await_recv(got.at[pl.ds(0, 3)], o_recv)
        for dy in range(Q):
            t = plus(y, dy)
            ref = (got if dy else moved).at[t]
            rows = pl.ds(pl.multiple_of(t * ROWS, ROWS), ROWS)
            outs.append(pltpu.make_async_copy(ref, out_hbm.at[rows, :], w_sem.at[dy]))
            outs[-1].start()

    def finish():
        for nq in range(Q):
            lanes = pl.ds(pl.multiple_of(nq * BLK + y * LANE, LANE), LANE)
            scale_ref[:, pl.ds(nq * LANE, LANE)] = N / jnp.sum(s2b[1, :, :, lanes], axis=0)
        for copy in outs:
            copy.wait()

    outs = []
    g1(Q0)
    a0_spread(0, (0,))
    cast_graph(Q1)
    g1(Q1)
    cast_graph(Q2)
    cast_graph(Q3)
    g2(Q0)
    g1(Q2)
    a0_exchange()
    g2(Q1)
    a0_relay(0, (0,))
    g3(Q0)
    g3(Q1)
    a0_wait_near()
    a0_spread(1, NEAR)
    a0_wait_far()
    a0_spread(2, (2,))
    g2(Q2)
    g4(Q0)
    a0_relay(1, NEAR)
    g1(Q3)
    a0_relay(2, (2,))
    g4(Q1)
    g3(Q2)
    g5(Q0)
    g2(Q3)
    a0_done()
    g5(Q1)
    g_whole(Q0)
    c1(Q0)
    c1_sums(Q0)
    g4(Q2)
    g_whole(Q1)
    c1_second(Q0)
    c1(Q1)
    c1_sums(Q1)
    a1_spread(Q0)
    g3(Q3)
    g5(Q2)
    c1_second(Q1)
    a1_relay(Q0)
    g_whole(Q2)
    a1_spread(Q1)
    c1(Q2)
    c1_sums(Q2)
    g4(Q3)
    c1_second(Q2)
    g5(Q3)
    a1_relay(Q1)
    a1_spread(Q2)
    g_whole(Q3)
    c1(Q3)
    c1_sums(Q3)
    c2(Q0, 0, True)
    c2(Q1, 0)
    a1_relay(Q2)
    c2(Q2, 0)
    c1_second(Q3)
    c2_near(Q0)
    a1_spread(Q3)
    c2_far(Q0)
    c2_near(Q1)
    c2(Q3, 0)
    a1_relay(Q3)
    c2_far(Q1)
    c2_near(Q2)
    c2_far(Q2)
    c2_near(Q3)
    c2_far(Q3)
    c2_sums()
    c2_second()
    sum_last(s2b, 0, Q)
    a2_scale(Q0)
    a2_spread(Q0)
    for p in (Q1, Q2, Q3):
        a2_scale(p)
    c3_own()
    a2_relay(Q0)
    a2_spread(Q1)
    c3_near(Q0)
    c3_far(Q0)
    a2_relay(Q1)
    a2_spread(Q2)
    c3_near(Q1)
    c3_far(Q1)
    a2_relay(Q2)
    a2_spread(Q3)
    c3_near(Q2)
    c3_far(Q2)
    a2_relay(Q3)
    c3_near(Q3)
    c3_far(Q3)
    c3_sums()
    c3_second()
    result_out()
    sum_last(s2b, 1, Q + 1)
    finish()

    for q in range(Q):
        await_send(g.at[q, :, pl.ds(0, 7936), :], g_send.at[q])
    await_send(stage.at[pl.ds(0, 3)], t_send)
    await_send(a.at[0, pl.ds(0, 3)], az_send)
    await_send(a.at[1, pl.ds(0, 3)], a1_send)
    for p, (start, rows) in enumerate(ROWS3):
        await_send(a.at[2, pl.ds(0, 3), :, :, :, pl.ds(start, rows), :], a2_send.at[p])
    for s1, s2, base in ((s1a, s2a, 0), (s1b, s2b, 4)):
        for i in range(s1.shape[0]):
            await_send(s1.at[i, pl.ds(0, 7)], r_send.at[0, base + i])
            await_send(s2.at[i, pl.ds(0, 3)], r_send.at[1, base + i])
    await_send(got.at[pl.ds(0, 3)], o_send)


def solution(mesh):
    block_spec = P(("graph", "row"), "col")
    hbm = pl.BlockSpec(memory_space=pl.ANY)
    dma = pltpu.SemaphoreType.DMA

    def device_step(init_blk, graph_blk):
        moved, scale = pl.pallas_call(
            mcl_kernel,
            out_shape=(jax.ShapeDtypeStruct((PIECE, BLK), F32), jax.ShapeDtypeStruct((1, BLK), F32)),
            in_specs=[hbm, hbm],
            out_specs=(hbm, pl.BlockSpec(memory_space=pltpu.VMEM)),
            scratch_shapes=[
                pltpu.VMEM((PIECE, BLK), F32), pltpu.VMEM((PIECE, BLK), F32),
                pltpu.VMEM((4, 4, N, LANE), BF),
                pltpu.VMEM((3, 4, 2, 4, 2, ROWS, LANE), BF),
                pltpu.VMEM((4, 4, ROWS, LANE), BF),
                pltpu.VMEM((4, ROWS, BLK), F32),
                pltpu.VMEM((4, ROWS, BLK), F32),
                pltpu.VMEM((4, ROWS, BLK), F32),
                pltpu.VMEM((4, ROWS, BLK), F32),
                pltpu.VMEM((4, 8, 1, BLK), F32),
                pltpu.VMEM((4, 4, 1, BLK), F32),
                pltpu.VMEM((2, 8, 1, PLANE), F32),
                pltpu.VMEM((2, 4, 1, PLANE), F32),
                dma((4,)), dma((4, 4)), dma((4,)),
                dma(()), dma((3,)),
                dma(()), dma((3,)), dma(()),
                dma(()), dma((2, Q)), dma((Q,)),
                dma((Q,)), dma((2, Q)), dma((Q,)),
                dma((2, 6)), dma((6,)), dma((6,)),
                dma(()), dma(()),
                dma((Q + 1,)), dma((Q,)),
            ],
            compiler_params=pltpu.CompilerParams(
                collective_id=0, has_side_effects=True, vmem_limit_bytes=67043328
            ),
        )(init_blk, graph_blk)
        return moved * scale

    return jax.shard_map(device_step, mesh=mesh, in_specs=(block_spec, block_spec), out_specs=block_spec, check_vma=False)
```

```python
import functools

import jax
import jax.numpy as jnp
from jax import lax
from jax.experimental import pallas as pl
from jax.experimental.pallas import tpu as pltpu
from jax.sharding import PartitionSpec as P

MESH = pl.DeviceIdType.MESH
BF = jnp.bfloat16
F32 = jnp.float32
N = 8192
PLANE, PIECE, BLK, ROWS, LANE = 2048, 1024, 512, 256, 128
Q = 4
Q0, Q1, Q2, Q3 = range(Q)
NEAR = (1, 3)
XM, XP, YP = 224, 448, 736
ROWS3 = ((0, 80), (80, 64), (144, 64), (208, 48))


def mcl_kernel(
    init_hbm, graph_hbm, out_hbm, scale_ref,
    init_ref, graph_ref,
    g, a, stage, hold, acc1, acc2, moved, got, s1a, s2a, s1b, s2b,
    g_send, g_recv, d_recv, t_send, t_recv, h_recv, az_send, az_recv, az2_recv,
    a1_send, a1_recv, a1_recv2, a2_send, a2_recv, a2_recv2,
    r_send, r_recv1, r_recv2, o_send, o_recv, i_sem, w_sem,
):
    col, row = lax.axis_index("col"), lax.axis_index("row")
    z, y = lax.div(col, 4), lax.rem(col, 4)
    x, c = lax.div(row, 2), lax.rem(row, 2)

    def plus(v, d):
        return lax.rem(v + d, 4)

    def dev(dx=0, dy=0, dz=0, dc=0):
        return {"col": plus(z, dz) * 4 + plus(y, dy), "row": plus(x, dx) * 2 + lax.rem(c + dc, 2)}

    XPOS, XNEG, YPOS, YNEG = dev(dx=1), dev(dx=3), dev(dy=1), dev(dy=3)
    ZPOS, ZNEG, MATE = dev(dz=1), dev(dz=3), dev(dc=1)

    def send(src, dst, ssem, rsem, device):
        pltpu.make_async_remote_copy(
            src_ref=src, dst_ref=dst, send_sem=ssem, recv_sem=rsem, device_id=device, device_id_type=MESH
        ).start()

    def await_recv(ref, sem):
        pltpu.make_async_remote_copy(
            src_ref=ref, dst_ref=ref, send_sem=sem, recv_sem=sem, device_id=MATE, device_id_type=MESH
        ).wait_recv()

    def await_send(ref, sem):
        pltpu.make_async_remote_copy(
            src_ref=ref, dst_ref=ref, send_sem=sem, recv_sem=sem, device_id=MATE, device_id_type=MESH
        ).wait_send()

    barrier = pltpu.get_barrier_semaphore()
    peers = [dev(dx=dx, dc=dc) for dx in range(Q) for dc in range(2) if (dx, dc) != (0, 0)]
    peers += [dev(dy=dy) for dy in (1, 2, 3)] + [ZPOS, ZNEG]
    for peer in peers:
        pl.semaphore_signal(barrier, inc=1, device_id=peer, device_id_type=MESH)

    copies = [pltpu.make_async_copy(init_hbm, init_ref, i_sem.at[Q])]
    for q in range(Q):
        lanes = pl.ds(q * LANE, LANE)
        copies.append(pltpu.make_async_copy(graph_hbm.at[:, lanes], graph_ref.at[:, lanes], i_sem.at[q]))
    for copy in copies:
        copy.start()

    def cast_graph(q):
        copies[q + 1].wait()
        base = pl.multiple_of((x * 2 + c) * PIECE, PIECE)
        for qr in range(Q):
            for yy in range(2):
                g[q, y, pl.ds(base + qr * ROWS + yy * LANE, LANE), :] = graph_ref[
                    pl.ds(yy * BLK + qr * LANE, LANE), pl.ds(q * LANE, LANE)
                ].astype(BF)

    copies[0].wait()
    own_rows = pl.ds(pl.multiple_of(y * ROWS, ROWS), ROWS)
    for q in range(Q):
        a[0, z, lax.div(y, 2), q, lax.rem(y, 2)] = init_ref[own_rows, pl.ds(q * LANE, LANE)].astype(BF)
    for t in range(Q):
        for q in range(Q):
            stage[t, q] = init_ref[pl.ds(t * ROWS, ROWS), pl.ds(q * LANE, LANE)].astype(BF)
    cast_graph(0)
    pl.semaphore_wait(barrier, len(peers))

    def a0_block(dz, dy, lo=0, n=4):
        yy = plus(y, dy)
        return a.at[0, plus(z, dz), lax.div(yy, 2), pl.ds(lo, n), lax.rem(yy, 2)]

    def a0_spread(group, dys):
        for dy in dys:
            for where in (ZPOS, ZNEG):
                send(a0_block(0, dy), a0_block(0, dy), az_send, az_recv.at[group], where)

    def a0_wait_near():
        for k in range(2):
            await_recv(stage.at[0], t_recv.at[k])

    def a0_wait_far():
        await_recv(stage.at[0], t_recv.at[2])

    def a0_done():
        await_recv(a.at[0, 0], az2_recv)

    def a0_relay(group, dys):
        await_recv(a.at[0, 0, pl.ds(0, len(dys))], az_recv.at[group])
        for dy in dys:
            send(a0_block(3, dy, 0, 2), a0_block(3, dy, 0, 2), az_send, az2_recv, ZPOS)
            send(a0_block(1, dy, 2, 2), a0_block(1, dy, 2, 2), az_send, az2_recv, ZNEG)

    def a0_exchange():
        far = plus(y, 2)
        for side, where in enumerate((YPOS, YNEG)):
            send(stage.at[far, pl.ds(2 * side, 2)], hold.at[side], t_send, h_recv, where)
            send(stage.at[plus(y, NEAR[side])], a0_block(0, 0), t_send, t_recv.at[side], where)

    def a0_pass():
        await_recv(hold, h_recv)
        for side, where in enumerate((YPOS, YNEG)):
            ref = a0_block(0, NEAR[1 - side], 2 * side, 2)
            send(hold.at[side], ref, t_send, t_recv.at[2], where)

    def piece(q, dx, dy, lo=0, hi=PIECE):
        base = (plus(x, dx) * 2 + c) * PIECE
        return g.at[q, plus(y, dy), pl.ds(pl.multiple_of(base + lo, 16), hi - lo), :]

    def hop(q, depth, where, dx, dy, lo=0, hi=PIECE):
        ref = piece(q, dx, dy, lo, hi)
        send(ref, ref, g_send.at[q], g_recv.at[q, depth], where)

    def mate(q, *offsets, last=0):
        for dx, dy in offsets:
            ref = piece(q, dx, dy)
            send(ref, ref, g_send.at[q], d_recv.at[last, q], MATE)

    def arrived(q, depth):
        rows = (4096, 2 * (BLK + 2 * (PIECE - XP)) + 2 * (BLK + 2 * XP), 4096, PIECE)[depth]
        await_recv(g.at[q, 0, pl.ds(0, rows), :], g_recv.at[q, depth])

    def g1(q):
        for where in (XPOS, XNEG, YPOS, YNEG):
            hop(q, 0, where, 0, 0)
        mate(q, (0, 0))

    def g2(q):
        arrived(q, 0)
        hop(q, 1, XPOS, 3, 0, XM, YP)
        hop(q, 1, YPOS, 0, 3, XM, YP)
        for lo, hi in ((0, XM), (YP, PIECE)):
            hop(q, 1, XNEG, 1, 0, lo, hi)
            hop(q, 1, YNEG, 0, 1, lo, hi)
        for d in (1, 3):
            for where in (XPOS, XNEG):
                hop(q, 1, where, 0, d, XP, PIECE)
            for where in (YPOS, YNEG):
                hop(q, 1, where, d, 0, 0, XP)
        mate(q, (1, 0), (3, 0), (0, 1), (0, 3))

    def g3(q):
        arrived(q, 1)
        for where in (XPOS, XNEG):
            hop(q, 2, where, 0, 2, XP, PIECE)
        for where in (YPOS, YNEG):
            hop(q, 2, where, 2, 0, 0, XP)
        for d in (1, 3):
            hop(q, 2, XPOS, 3, d, XP, YP)
            hop(q, 2, XNEG, 1, d, YP, PIECE)
            hop(q, 2, YPOS, d, 3, XM, XP)
            hop(q, 2, YNEG, d, 1, 0, XM)
        mate(q, (2, 0), (0, 2), (1, 1), (1, 3), (3, 1), (3, 3))

    def g4(q):
        arrived(q, 2)
        hop(q, 3, XPOS, 3, 2, XP, YP)
        hop(q, 3, XNEG, 1, 2, YP, PIECE)
        hop(q, 3, YPOS, 2, 3, XM, XP)
        hop(q, 3, YNEG, 2, 1, 0, XM)
        mate(q, (1, 2), (3, 2), (2, 1), (2, 3))

    def g5(q):
        arrived(q, 3)
        mate(q, (2, 2), last=1)

    def g_most(q):
        await_recv(g.at[q, pl.ds(0, 3), pl.ds(0, 5 * PIECE)], d_recv.at[0, q])

    def g_whole(q):
        await_recv(g.at[q, 0, pl.ds(0, PIECE)], d_recv.at[1, q])

    def g_rows(nq, start, n):
        return jnp.concatenate([g[nq, t, pl.ds(start, n), :] for t in range(Q)], axis=1)

    def c1_part(q, zz):
        lhs = jnp.concatenate(
            [a[0, zz, cc, qr, yy] for cc in range(2) for qr in range(Q) for yy in range(2)], axis=1
        )
        acc1[q] += jnp.dot(lhs, g_rows(q, pl.multiple_of(zz * PLANE, PLANE), PLANE), preferred_element_type=F32)

    def c1_most(q):
        def step(i, carry):
            c1_part(q, plus(x, i + lax.div(i, 2)))
            return carry

        acc1[q] = jnp.zeros((ROWS, BLK), F32)
        lax.fori_loop(0, 3, step, 0)

    def c1_rest(q):
        c1_part(q, plus(x, 2))

    def square_sum(ref, q):
        v = ref[q]
        return jnp.sum(v * v, axis=0, keepdims=True)

    def sum_first(s1, i, k):
        me = x * 2 + c
        for dx in range(Q):
            for dc in range(2):
                if (dx, dc) != (0, 0):
                    send(s1.at[i, me], s1.at[i, me], r_send.at[0, k], r_recv1.at[k], dev(dx=dx, dc=dc))

    def sum_second(s1, s2, i, k):
        await_recv(s1.at[i, pl.ds(0, 7)], r_recv1.at[k])
        s2[i, y] = jnp.sum(s1[i], axis=0)
        for dy in (1, 2, 3):
            send(s2.at[i, y], s2.at[i, y], r_send.at[1, k], r_recv2.at[k], dev(dy=dy))

    def sum_last(s2, i, k):
        await_recv(s2.at[i, pl.ds(0, 3)], r_recv2.at[k])

    def c1_sums(q):
        s1a[q, x * 2 + c] = square_sum(acc1, q)
        sum_first(s1a, q, q)

    def c1_second(q):
        sum_second(s1a, s2a, q, q)

    def a1_chunk(dz, q, lo=0, n=2):
        return a.at[1, plus(z, dz), pl.ds(lo, n), q]

    def a1_spread(q):
        sum_last(s2a, q, q)
        scale = N / jnp.sum(s2a[q], axis=0)
        for t in range(Q):
            v = acc1[q, :, pl.ds(t * LANE, LANE)]
            a[1, z, t // 2, q, t % 2] = (v * v * scale[:, t * LANE : t * LANE + LANE]).astype(BF)
        for half in range(2):
            for where, n in ((ZPOS, half), (ZNEG, 1 - half)):
                send(a1_chunk(0, q, n, 1), a1_chunk(0, q, n, 1), a1_send, a1_recv.at[half, q], where)

    def a1_relay(q):
        await_recv(a.at[1, 0, :, 0], a1_recv.at[0, q])
        send(a1_chunk(3, q, 0, 1), a1_chunk(3, q, 0, 1), a1_send, a1_recv2.at[q], ZPOS)
        send(a1_chunk(1, q, 1, 1), a1_chunk(1, q, 1, 1), a1_send, a1_recv2.at[q], ZNEG)

    def c2(q, dz, first=False):
        zz = plus(z, dz)
        lhs = jnp.concatenate([a[1, zz, cc, q, yy] for cc in range(2) for yy in range(2)], axis=1)
        base = pl.multiple_of(zz * PLANE, PLANE)
        for nq in range(Q):
            rhs = jnp.concatenate([g_rows(nq, base + cc * PIECE + q * ROWS, ROWS) for cc in range(2)], axis=0)
            prod = jnp.dot(lhs, rhs, preferred_element_type=F32)
            acc2[nq] = prod if first else acc2[nq] + prod

    def c2_near(q):
        await_recv(a.at[1, 0, :, 0], a1_recv.at[1, q])
        for dz in NEAR:
            c2(q, dz)

    def c2_far(q):
        await_recv(a.at[1, 0, :, 0], a1_recv2.at[q])
        c2(q, 2)

    def c2_sums():
        for q in range(Q):
            s1b[0, x * 2 + c, :, pl.ds(q * BLK, BLK)] = square_sum(acc2, q)
        sum_first(s1b, 0, 4)

    def c2_second():
        sum_second(s1b, s2b, 0, 4)

    def a2_rows(dz, p, lo=0, n=2):
        start, rows = ROWS3[p]
        return a.at[2, plus(z, dz), pl.ds(lo, n), :, :, pl.ds(start, rows), :]

    def a2_scale(p):
        start, rows = ROWS3[p]
        scale = N / jnp.sum(s2b[0], axis=0)
        for q in range(Q):
            for t in range(Q):
                v = acc2[q, pl.ds(start, rows), pl.ds(t * LANE, LANE)]
                s = scale[:, q * BLK + t * LANE : q * BLK + t * LANE + LANE]
                a[2, z, t // 2, q, t % 2, pl.ds(start, rows), :] = (v * v * s).astype(BF)

    def a2_spread(p):
        for half in range(2):
            for where, n in ((ZPOS, half), (ZNEG, 1 - half)):
                send(a2_rows(0, p, n, 1), a2_rows(0, p, n, 1), a2_send.at[p], a2_recv.at[half, p], where)

    def a2_relay(p):
        start, rows = ROWS3[p]
        await_recv(a.at[2, 0, :, :, :, pl.ds(start, rows), :], a2_recv.at[0, p])
        send(a2_rows(3, p, 0, 1), a2_rows(3, p, 0, 1), a2_send.at[p], a2_recv2.at[p], ZPOS)
        send(a2_rows(1, p, 1, 1), a2_rows(1, p, 1, 1), a2_send.at[p], a2_recv2.at[p], ZNEG)

    def c3_part(zz, start, rows, nq):
        lhs = jnp.concatenate(
            [a[2, zz, cc, qr, yy, pl.ds(start, rows), :] for cc in range(2) for qr in range(Q) for yy in range(2)],
            axis=1,
        )
        return jnp.dot(lhs, g_rows(nq, pl.multiple_of(zz * PLANE, PLANE), PLANE), preferred_element_type=F32)

    def c3_own():
        def step(nq, carry):
            acc1[nq] = c3_part(z, 0, ROWS, nq)
            return carry

        lax.fori_loop(0, 4, step, 0)

    def c3_near(p):
        start, rows = ROWS3[p]
        await_recv(a.at[2, 0, :, :, :, pl.ds(start, rows), :], a2_recv.at[1, p])

        def step(nq, carry):
            acc1[nq, pl.ds(start, rows), :] += c3_part(plus(z, 1), start, rows, nq)
            acc1[nq, pl.ds(start, rows), :] += c3_part(plus(z, 3), start, rows, nq)
            return carry

        lax.fori_loop(0, 4, step, 0)

    def c3_far(p):
        start, rows = ROWS3[p]
        await_recv(a.at[2, 0, :, :, :, pl.ds(start, rows), :], a2_recv2.at[p])
        for nq in range(Q):
            v = acc1[nq, pl.ds(start, rows), :] + c3_part(plus(z, 2), start, rows, nq)
            v = v * v
            part = jnp.sum(v, axis=0, keepdims=True)
            lanes = pl.ds(nq * BLK, BLK)
            if p == 0:
                s1b[1, x * 2 + c, :, lanes] = part
            else:
                s1b[1, x * 2 + c, :, lanes] += part
            for t in range(Q):
                moved[t, pl.ds(start, rows), pl.ds(nq * LANE, LANE)] = v[:, t * LANE : t * LANE + LANE]
        for dy in (2, 1, 3):
            send(
                moved.at[plus(y, dy), pl.ds(start, rows), :],
                got.at[y, pl.ds(start, rows), :],
                o_send, o_recv, dev(dy=dy),
            )

    def c3_sums():
        sum_first(s1b, 1, Q + 1)

    def c3_second():
        sum_second(s1b, s2b, 1, Q + 1)

    def result_out():
        await_recv(got.at[pl.ds(0, 3)], o_recv)
        for dy in range(Q):
            t = plus(y, dy)
            ref = (got if dy else moved).at[t]
            rows = pl.ds(pl.multiple_of(t * ROWS, ROWS), ROWS)
            outs.append(pltpu.make_async_copy(ref, out_hbm.at[rows, :], w_sem.at[dy]))
            outs[-1].start()

    def finish():
        for nq in range(Q):
            lanes = pl.ds(pl.multiple_of(nq * BLK + y * LANE, LANE), LANE)
            scale_ref[:, pl.ds(nq * LANE, LANE)] = N / jnp.sum(s2b[1, :, :, lanes], axis=0)
        for copy in outs:
            copy.wait()

    outs = []
    g1(Q0)
    a0_spread(0, (0,))
    a0_exchange()
    cast_graph(Q2)
    g1(Q2)
    g2(Q0)
    a0_wait_near()
    a0_spread(1, NEAR)
    cast_graph(Q1)
    g1(Q1)
    a0_pass()
    g2(Q2)
    a0_relay(0, (0,))
    g3(Q0)
    g2(Q1)
    a0_wait_far()
    a0_spread(2, (2,))
    a0_relay(1, NEAR)
    cast_graph(Q3)
    g1(Q3)
    g4(Q0)
    g3(Q1)
    g3(Q2)
    g5(Q0)
    g_most(Q0)
    a0_relay(2, (2,))
    a0_done()
    g4(Q1)
    c1_most(Q0)
    g2(Q3)
    g_whole(Q0)
    c1_rest(Q0)
    c1_sums(Q0)
    g4(Q2)
    g_most(Q1)
    c1_most(Q1)
    c1_second(Q0)
    g5(Q1)
    g_whole(Q1)
    c1_rest(Q1)
    c1_sums(Q1)
    g_most(Q2)
    a1_spread(Q0)
    g3(Q3)
    a1_relay(Q0)
    c1_second(Q1)
    g5(Q2)
    c1_most(Q2)
    g_whole(Q2)
    c1_rest(Q2)
    c1_sums(Q2)
    a1_spread(Q1)
    g4(Q3)
    c1_second(Q2)
    a1_relay(Q1)
    a1_spread(Q2)
    g_most(Q3)
    g5(Q3)
    c1_most(Q3)
    g_whole(Q3)
    c1_rest(Q3)
    c1_sums(Q3)
    c2(Q0, 0, True)
    c1_second(Q3)
    a1_relay(Q2)
    c2_near(Q0)
    a1_spread(Q3)
    c2(Q1, 0)
    c2_near(Q2)
    c2_near(Q1)
    c2_far(Q1)
    a1_relay(Q3)
    c2_far(Q2)
    c2(Q3, 0)
    c2_far(Q0)
    c2_near(Q3)
    c2(Q2, 0)
    c2_far(Q3)
    c2_sums()
    c2_second()
    sum_last(s2b, 0, Q)
    a2_scale(Q0)
    a2_spread(Q0)
    for p in (Q1, Q2, Q3):
        a2_scale(p)
    c3_own()
    a2_relay(Q0)
    a2_spread(Q1)
    c3_near(Q0)
    c3_far(Q0)
    a2_relay(Q1)
    a2_spread(Q2)
    c3_near(Q1)
    c3_far(Q1)
    a2_relay(Q2)
    a2_spread(Q3)
    c3_near(Q2)
    c3_far(Q2)
    a2_relay(Q3)
    c3_near(Q3)
    c3_far(Q3)
    c3_sums()
    c3_second()
    result_out()
    sum_last(s2b, 1, Q + 1)
    finish()

    for q in range(Q):
        await_send(g.at[q, :, pl.ds(0, 7936), :], g_send.at[q])
    await_send(stage, t_send)
    await_send(a.at[0, pl.ds(0, 3)], az_send)
    await_send(a.at[1, pl.ds(0, 3)], a1_send)
    for p, (start, rows) in enumerate(ROWS3):
        await_send(a.at[2, pl.ds(0, 3), :, :, :, pl.ds(start, rows), :], a2_send.at[p])
    for s1, s2, base in ((s1a, s2a, 0), (s1b, s2b, 4)):
        for i in range(s1.shape[0]):
            await_send(s1.at[i, pl.ds(0, 7)], r_send.at[0, base + i])
            await_send(s2.at[i, pl.ds(0, 3)], r_send.at[1, base + i])
    await_send(got.at[pl.ds(0, 3)], o_send)


def solution(mesh):
    block_spec = P(("graph", "row"), "col")
    hbm = pl.BlockSpec(memory_space=pl.ANY)
    dma = pltpu.SemaphoreType.DMA

    def device_step(init_blk, graph_blk):
        moved, scale = pl.pallas_call(
            mcl_kernel,
            out_shape=(jax.ShapeDtypeStruct((PIECE, BLK), F32), jax.ShapeDtypeStruct((1, BLK), F32)),
            in_specs=[hbm, hbm],
            out_specs=(hbm, pl.BlockSpec(memory_space=pltpu.VMEM)),
            scratch_shapes=[
                pltpu.VMEM((PIECE, BLK), F32), pltpu.VMEM((PIECE, BLK), F32),
                pltpu.VMEM((4, 4, N, LANE), BF),
                pltpu.VMEM((3, 4, 2, 4, 2, ROWS, LANE), BF),
                pltpu.VMEM((4, 4, ROWS, LANE), BF),
                pltpu.VMEM((2, 2, ROWS, LANE), BF),
                pltpu.VMEM((4, ROWS, BLK), F32),
                pltpu.VMEM((4, ROWS, BLK), F32),
                pltpu.VMEM((4, ROWS, BLK), F32),
                pltpu.VMEM((4, ROWS, BLK), F32),
                pltpu.VMEM((4, 8, 1, BLK), F32),
                pltpu.VMEM((4, 4, 1, BLK), F32),
                pltpu.VMEM((2, 8, 1, PLANE), F32),
                pltpu.VMEM((2, 4, 1, PLANE), F32),
                dma((Q,)), dma((Q, Q)), dma((2, Q)),
                dma(()), dma((3,)), dma(()),
                dma(()), dma((3,)), dma(()),
                dma(()), dma((2, Q)), dma((Q,)),
                dma((Q,)), dma((2, Q)), dma((Q,)),
                dma((2, 6)), dma((6,)), dma((6,)),
                dma(()), dma(()),
                dma((Q + 1,)), dma((Q,)),
            ],
            compiler_params=pltpu.CompilerParams(
                collective_id=0, has_side_effects=True, vmem_limit_bytes=67043328
            ),
        )(init_blk, graph_blk)
        return moved * scale

    return jax.shard_map(device_step, mesh=mesh, in_specs=(block_spec, block_spec), out_specs=block_spec, check_vma=False)
```

```python
import functools

import jax
import jax.numpy as jnp
from jax import lax
from jax.experimental import pallas as pl
from jax.experimental.pallas import tpu as pltpu
from jax.sharding import PartitionSpec as P

MESH = pl.DeviceIdType.MESH
VMEM_BYTES = 58 << 20
BF = jnp.bfloat16
F32 = jnp.float32
N = 8192
PLANE, PIECE, BLK, ROWS, LANE = 2048, 1024, 512, 256, 128
Q = 4
Q0, Q1, Q2, Q3 = range(Q)
NEAR = (1, 3)
XM, XP, YP = 224, 448, 736
ROWS3 = ((0, 80), (80, 64), (144, 64), (208, 48))


def mcl_kernel(
    init_hbm, graph_hbm, out_ref,
    moved, got,
    g, a, stage, hold, acc1, acc2, s1a, s2a, s1b, s2b, s3, s4,
    g_send, g_recv, d_recv, t_send, t_recv, h_recv, az_send, az_recv, az2_recv,
    a1_send, a1_recv, a1_recv2, a2_send, a2_recv, a2_recv2,
    r_send, r_recv1, r_recv2, o_send, o_recv, f_send, f_recv, i_sem,
):
    col, row = lax.axis_index("col"), lax.axis_index("row")
    z, y = lax.div(col, 4), lax.rem(col, 4)
    x, c = lax.div(row, 2), lax.rem(row, 2)

    def plus(v, d):
        return lax.rem(v + d, 4)

    def dev(dx=0, dy=0, dz=0, dc=0):
        return {"col": plus(z, dz) * 4 + plus(y, dy), "row": plus(x, dx) * 2 + lax.rem(c + dc, 2)}

    XPOS, XNEG, YPOS, YNEG = dev(dx=1), dev(dx=3), dev(dy=1), dev(dy=3)
    ZPOS, ZNEG, MATE = dev(dz=1), dev(dz=3), dev(dc=1)

    def send(src, dst, ssem, rsem, device):
        pltpu.make_async_remote_copy(
            src_ref=src, dst_ref=dst, send_sem=ssem, recv_sem=rsem, device_id=device, device_id_type=MESH
        ).start()

    def await_recv(ref, sem):
        pltpu.make_async_remote_copy(
            src_ref=ref, dst_ref=ref, send_sem=sem, recv_sem=sem, device_id=MATE, device_id_type=MESH
        ).wait_recv()

    def await_send(ref, sem):
        pltpu.make_async_remote_copy(
            src_ref=ref, dst_ref=ref, send_sem=sem, recv_sem=sem, device_id=MATE, device_id_type=MESH
        ).wait_send()

    barrier = pltpu.get_barrier_semaphore()
    peers = [dev(dx=dx, dc=dc) for dx in range(Q) for dc in range(2) if (dx, dc) != (0, 0)]
    peers += [dev(dy=dy) for dy in (1, 2, 3)] + [ZPOS, ZNEG]
    for peer in peers:
        pl.semaphore_signal(barrier, inc=1, device_id=peer, device_id_type=MESH)

    init_ref, graph_ref = moved, got
    copies = []
    for q in range(Q + 1):
        lanes = pl.ds(q * LANE, LANE)
        parts = []
        for t in range(Q):
            rows = pl.ds(t * ROWS, ROWS)
            if q == Q:
                parts.append(pltpu.make_async_copy(init_hbm.at[rows], init_ref.at[t], i_sem.at[q, t]))
            else:
                parts.append(
                    pltpu.make_async_copy(graph_hbm.at[rows, lanes], graph_ref.at[t, :, lanes], i_sem.at[q, t])
                )
        copies.append(parts)
    for q in (Q, Q0, Q1, Q2, Q3):
        for copy in copies[q]:
            copy.start()

    def cast_graph(q):
        for copy in copies[q]:
            copy.wait()
        base = pl.multiple_of((x * 2 + c) * PIECE, PIECE)
        lanes = pl.ds(q * LANE, LANE)
        for qr in range(Q):
            for yy in range(2):
                block = graph_ref[yy * 2 + qr // 2, pl.ds(qr % 2 * LANE, LANE), lanes]
                g[q, y, pl.ds(base + qr * ROWS + yy * LANE, LANE), :] = block.astype(BF)

    cast_graph(Q0)
    for copy in copies[Q]:
        copy.wait()
    for q in range(Q):
        a[0, z, lax.div(y, 2), q, lax.rem(y, 2)] = init_ref[y, :, pl.ds(q * LANE, LANE)].astype(BF)
    for t in range(Q):
        for q in range(Q):
            stage[t, q] = init_ref[t, :, pl.ds(q * LANE, LANE)].astype(BF)
    pl.semaphore_wait(barrier, len(peers))

    def a0_block(dz, dy, lo=0, n=4):
        yy = plus(y, dy)
        return a.at[0, plus(z, dz), lax.div(yy, 2), pl.ds(lo, n), lax.rem(yy, 2)]

    def a0_spread(group, dys):
        for dy in dys:
            for where in (ZPOS, ZNEG):
                send(a0_block(0, dy), a0_block(0, dy), az_send, az_recv.at[group], where)

    def a0_wait_near():
        for k in range(2):
            await_recv(stage.at[0], t_recv.at[k])

    def a0_wait_far():
        await_recv(stage.at[0], t_recv.at[2])

    def a0_done():
        await_recv(a.at[0, 0], az2_recv)

    def a0_relay(group, dys):
        await_recv(a.at[0, 0, pl.ds(0, len(dys))], az_recv.at[group])
        for dy in dys:
            send(a0_block(3, dy, 0, 2), a0_block(3, dy, 0, 2), az_send, az2_recv, ZPOS)
            send(a0_block(1, dy, 2, 2), a0_block(1, dy, 2, 2), az_send, az2_recv, ZNEG)

    def a0_exchange():
        far = plus(y, 2)
        for side, where in enumerate((YPOS, YNEG)):
            send(stage.at[far, pl.ds(2 * side, 2)], hold.at[side], t_send, h_recv, where)
            send(stage.at[plus(y, NEAR[side])], a0_block(0, 0), t_send, t_recv.at[side], where)

    def a0_pass():
        await_recv(hold, h_recv)
        for side, where in enumerate((YPOS, YNEG)):
            ref = a0_block(0, NEAR[1 - side], 2 * side, 2)
            send(hold.at[side], ref, t_send, t_recv.at[2], where)

    def piece(q, dx, dy, lo=0, hi=PIECE):
        base = (plus(x, dx) * 2 + c) * PIECE
        return g.at[q, plus(y, dy), pl.ds(pl.multiple_of(base + lo, 16), hi - lo), :]

    def hop(q, depth, where, dx, dy, lo=0, hi=PIECE):
        ref = piece(q, dx, dy, lo, hi)
        send(ref, ref, g_send.at[q], g_recv.at[q, depth], where)

    def mate(q, *offsets, last=0):
        for dx, dy in offsets:
            ref = piece(q, dx, dy)
            send(ref, ref, g_send.at[q], d_recv.at[last, q], MATE)

    def arrived(q, depth):
        rows = (4096, 2 * (BLK + 2 * (PIECE - XP)) + 2 * (BLK + 2 * XP), 4096, PIECE)[depth]
        await_recv(g.at[q, 0, pl.ds(0, rows), :], g_recv.at[q, depth])

    def g1(q):
        for where in (XPOS, XNEG, YPOS, YNEG):
            hop(q, 0, where, 0, 0)
        mate(q, (0, 0))

    def g2(q):
        arrived(q, 0)
        hop(q, 1, XPOS, 3, 0, XM, YP)
        hop(q, 1, YPOS, 0, 3, XM, YP)
        for lo, hi in ((0, XM), (YP, PIECE)):
            hop(q, 1, XNEG, 1, 0, lo, hi)
            hop(q, 1, YNEG, 0, 1, lo, hi)
        for d in (1, 3):
            for where in (XPOS, XNEG):
                hop(q, 1, where, 0, d, XP, PIECE)
            for where in (YPOS, YNEG):
                hop(q, 1, where, d, 0, 0, XP)
        mate(q, (1, 0), (3, 0), (0, 1), (0, 3))

    def g3(q):
        arrived(q, 1)
        for where in (XPOS, XNEG):
            hop(q, 2, where, 0, 2, XP, PIECE)
        for where in (YPOS, YNEG):
            hop(q, 2, where, 2, 0, 0, XP)
        for d in (1, 3):
            hop(q, 2, XPOS, 3, d, XP, YP)
            hop(q, 2, XNEG, 1, d, YP, PIECE)
            hop(q, 2, YPOS, d, 3, XM, XP)
            hop(q, 2, YNEG, d, 1, 0, XM)
        mate(q, (2, 0), (0, 2), (1, 1), (1, 3), (3, 1), (3, 3))

    def g4(q):
        arrived(q, 2)
        hop(q, 3, XPOS, 3, 2, XP, YP)
        hop(q, 3, XNEG, 1, 2, YP, PIECE)
        hop(q, 3, YPOS, 2, 3, XM, XP)
        hop(q, 3, YNEG, 2, 1, 0, XM)
        mate(q, (1, 2), (3, 2), (2, 1), (2, 3))

    def g5(q):
        arrived(q, 3)
        mate(q, (2, 2), last=1)

    def g_most(q):
        await_recv(g.at[q, pl.ds(0, 3), pl.ds(0, 5 * PIECE)], d_recv.at[0, q])

    def g_whole(q):
        await_recv(g.at[q, 0, pl.ds(0, PIECE)], d_recv.at[1, q])

    def g_rows(nq, start, n):
        return jnp.concatenate([g[nq, t, pl.ds(start, n), :] for t in range(Q)], axis=1)

    def c1_part(q, zz):
        lhs = jnp.concatenate(
            [a[0, zz, cc, qr, yy] for cc in range(2) for qr in range(Q) for yy in range(2)], axis=1
        )
        acc1[q] += jnp.dot(lhs, g_rows(q, pl.multiple_of(zz * PLANE, PLANE), PLANE), preferred_element_type=F32)

    def c1_most(q):
        def step(i, carry):
            c1_part(q, plus(x, i + lax.div(i, 2)))
            return carry

        acc1[q] = jnp.zeros((ROWS, BLK), F32)
        lax.fori_loop(0, 3, step, 0)

    def c1_rest(q):
        c1_part(q, plus(x, 2))

    def square_sum(ref, q):
        v = ref[q]
        return jnp.sum(v * v, axis=0, keepdims=True)

    def sum_first(s1, i, k):
        me = x * 2 + c
        for dx in range(Q):
            for dc in range(2):
                if (dx, dc) != (0, 0):
                    send(s1.at[i, me], s1.at[i, me], r_send.at[0, k], r_recv1.at[k], dev(dx=dx, dc=dc))

    def sum_second(s1, s2, i, k):
        await_recv(s1.at[i, pl.ds(0, 7)], r_recv1.at[k])
        s2[i, y] = jnp.sum(s1[i], axis=0)
        for dy in (1, 2, 3):
            send(s2.at[i, y], s2.at[i, y], r_send.at[1, k], r_recv2.at[k], dev(dy=dy))

    def sum_last(s2, i, k):
        await_recv(s2.at[i, pl.ds(0, 3)], r_recv2.at[k])

    def c1_sums(q):
        s1a[q, x * 2 + c] = square_sum(acc1, q)
        sum_first(s1a, q, q)

    def c1_second(q):
        sum_second(s1a, s2a, q, q)

    def a1_chunk(dz, q, lo=0, n=2):
        return a.at[1, plus(z, dz), pl.ds(lo, n), q]

    def a1_spread(q):
        sum_last(s2a, q, q)
        scale = N / jnp.sum(s2a[q], axis=0)
        for t in range(Q):
            v = acc1[q, :, pl.ds(t * LANE, LANE)]
            a[1, z, t // 2, q, t % 2] = (v * v * scale[:, t * LANE : t * LANE + LANE]).astype(BF)
        for half in range(2):
            for where, n in ((ZPOS, half), (ZNEG, 1 - half)):
                send(a1_chunk(0, q, n, 1), a1_chunk(0, q, n, 1), a1_send, a1_recv.at[half, q], where)

    def a1_relay(q):
        await_recv(a.at[1, 0, :, 0], a1_recv.at[0, q])
        send(a1_chunk(3, q, 0, 1), a1_chunk(3, q, 0, 1), a1_send, a1_recv2.at[q], ZPOS)
        send(a1_chunk(1, q, 1, 1), a1_chunk(1, q, 1, 1), a1_send, a1_recv2.at[q], ZNEG)

    def c2(q, dz, first=False):
        zz = plus(z, dz)
        lhs = jnp.concatenate([a[1, zz, cc, q, yy] for cc in range(2) for yy in range(2)], axis=1)
        base = pl.multiple_of(zz * PLANE, PLANE)
        for nq in range(Q):
            rhs = jnp.concatenate([g_rows(nq, base + cc * PIECE + q * ROWS, ROWS) for cc in range(2)], axis=0)
            prod = jnp.dot(lhs, rhs, preferred_element_type=F32)
            acc2[nq] = prod if first else acc2[nq] + prod

    def c2_near(q):
        await_recv(a.at[1, 0, :, 0], a1_recv.at[1, q])
        for dz in NEAR:
            c2(q, dz)

    def c2_far(q):
        await_recv(a.at[1, 0, :, 0], a1_recv2.at[q])
        c2(q, 2)

    def c2_sums():
        for q in range(Q):
            s1b[0, x * 2 + c, :, pl.ds(q * BLK, BLK)] = square_sum(acc2, q)
        sum_first(s1b, 0, 4)

    def c2_second():
        sum_second(s1b, s2b, 0, 4)

    def a2_rows(dz, p, lo=0, n=2):
        start, rows = ROWS3[p]
        return a.at[2, plus(z, dz), pl.ds(lo, n), :, :, pl.ds(start, rows), :]

    def a2_scale(p):
        start, rows = ROWS3[p]
        scale = N / jnp.sum(s2b[0], axis=0)
        for q in range(Q):
            for t in range(Q):
                v = acc2[q, pl.ds(start, rows), pl.ds(t * LANE, LANE)]
                s = scale[:, q * BLK + t * LANE : q * BLK + t * LANE + LANE]
                a[2, z, t // 2, q, t % 2, pl.ds(start, rows), :] = (v * v * s).astype(BF)

    def a2_spread(p):
        for half in range(2):
            for where, n in ((ZPOS, half), (ZNEG, 1 - half)):
                send(a2_rows(0, p, n, 1), a2_rows(0, p, n, 1), a2_send.at[p], a2_recv.at[half, p], where)

    def a2_relay(p):
        start, rows = ROWS3[p]
        await_recv(a.at[2, 0, :, :, :, pl.ds(start, rows), :], a2_recv.at[0, p])
        send(a2_rows(3, p, 0, 1), a2_rows(3, p, 0, 1), a2_send.at[p], a2_recv2.at[p], ZPOS)
        send(a2_rows(1, p, 1, 1), a2_rows(1, p, 1, 1), a2_send.at[p], a2_recv2.at[p], ZNEG)

    def c3_part(zz, start, rows, nq):
        lhs = jnp.concatenate(
            [a[2, zz, cc, qr, yy, pl.ds(start, rows), :] for cc in range(2) for qr in range(Q) for yy in range(2)],
            axis=1,
        )
        return jnp.dot(lhs, g_rows(nq, pl.multiple_of(zz * PLANE, PLANE), PLANE), preferred_element_type=F32)

    def c3_own():
        def step(nq, carry):
            acc1[nq] = c3_part(z, 0, ROWS, nq)
            return carry

        lax.fori_loop(0, 4, step, 0)

    def c3_near(p):
        start, rows = ROWS3[p]
        await_recv(a.at[2, 0, :, :, :, pl.ds(start, rows), :], a2_recv.at[1, p])

        def step(nq, carry):
            acc1[nq, pl.ds(start, rows), :] += c3_part(plus(z, 1), start, rows, nq)
            acc1[nq, pl.ds(start, rows), :] += c3_part(plus(z, 3), start, rows, nq)
            return carry

        lax.fori_loop(0, 4, step, 0)

    def c3_far(p):
        start, rows = ROWS3[p]
        await_recv(a.at[2, 0, :, :, :, pl.ds(start, rows), :], a2_recv2.at[p])
        for nq in range(Q):
            v = acc1[nq, pl.ds(start, rows), :] + c3_part(plus(z, 2), start, rows, nq)
            v = v * v
            part = jnp.sum(v, axis=0, keepdims=True)
            here = pl.ds(nq * LANE, LANE)
            for t in range(Q):
                cut = slice(t * LANE, t * LANE + LANE)
                moved[t, pl.ds(start, rows), here] = v[:, cut]
                if p == 0:
                    s3[t, :, here] = part[:, cut]
                else:
                    s3[t, :, here] += part[:, cut]
        if p == Q3:
            c3_sums()
        for dy in (2, 1, 3):
            send(
                moved.at[plus(y, dy), pl.ds(start, rows), :],
                got.at[y, pl.ds(start, rows), :],
                o_send, o_recv, dev(dy=dy),
            )

    def c3_sums():
        me = y * 8 + x * 2 + c
        s4[me] = s3[y]
        for dy in (2, 1, 3, 0):
            for dx in (2, 1, 3, 0):
                for dc in range(2):
                    if dx + dy + dc:
                        send(s3.at[plus(y, dy)], s4.at[me], f_send, f_recv, dev(dx=dx, dy=dy, dc=dc))

    def finish():
        await_recv(s4.at[pl.ds(0, 31)], f_recv)
        scale = N / jnp.sum(s4[...], axis=0)
        out_ref[y] = moved[y] * scale
        await_recv(got.at[pl.ds(0, 3)], o_recv)
        for dy in (1, 2, 3):
            t = plus(y, dy)
            out_ref[t] = got[t] * scale

    g1(Q0)
    a0_spread(0, (0,))
    a0_exchange()
    cast_graph(Q2)
    g1(Q2)
    g2(Q0)
    a0_wait_near()
    a0_spread(1, NEAR)
    cast_graph(Q1)
    g1(Q1)
    a0_pass()
    g2(Q2)
    a0_relay(0, (0,))
    g3(Q0)
    g2(Q1)
    a0_wait_far()
    a0_spread(2, (2,))
    a0_relay(1, NEAR)
    cast_graph(Q3)
    g1(Q3)
    g4(Q0)
    g3(Q1)
    g3(Q2)
    g5(Q0)
    g_most(Q0)
    a0_relay(2, (2,))
    a0_done()
    g4(Q1)
    c1_most(Q0)
    g2(Q3)
    g_whole(Q0)
    c1_rest(Q0)
    c1_sums(Q0)
    g4(Q2)
    g_most(Q1)
    c1_most(Q1)
    c1_second(Q0)
    g5(Q1)
    g_whole(Q1)
    c1_rest(Q1)
    c1_sums(Q1)
    g_most(Q2)
    a1_spread(Q0)
    g3(Q3)
    a1_relay(Q0)
    c1_second(Q1)
    g5(Q2)
    c1_most(Q2)
    g_whole(Q2)
    c1_rest(Q2)
    c1_sums(Q2)
    a1_spread(Q1)
    g4(Q3)
    c1_second(Q2)
    a1_relay(Q1)
    a1_spread(Q2)
    g_most(Q3)
    g5(Q3)
    c1_most(Q3)
    g_whole(Q3)
    c1_rest(Q3)
    c1_sums(Q3)
    c2(Q0, 0, True)
    c1_second(Q3)
    a1_relay(Q2)
    c2_near(Q0)
    a1_spread(Q3)
    c2(Q1, 0)
    c2_near(Q2)
    c2_near(Q1)
    c2_far(Q1)
    a1_relay(Q3)
    c2_far(Q2)
    c2(Q3, 0)
    c2_far(Q0)
    c2_near(Q3)
    c2(Q2, 0)
    c2_far(Q3)
    c2_sums()
    c2_second()
    sum_last(s2b, 0, Q)
    a2_scale(Q0)
    a2_spread(Q0)
    for p in (Q1, Q2, Q3):
        a2_scale(p)
    c3_own()
    a2_relay(Q0)
    a2_spread(Q1)
    c3_near(Q0)
    c3_far(Q0)
    a2_relay(Q1)
    a2_spread(Q2)
    c3_near(Q1)
    c3_far(Q1)
    a2_relay(Q2)
    a2_spread(Q3)
    c3_near(Q2)
    c3_far(Q2)
    a2_relay(Q3)
    c3_near(Q3)
    c3_far(Q3)
    finish()

    for q in range(Q):
        await_send(g.at[q, :, pl.ds(0, 7936), :], g_send.at[q])
    await_send(stage, t_send)
    await_send(a.at[0, pl.ds(0, 3)], az_send)
    await_send(a.at[1, pl.ds(0, 3)], a1_send)
    for p, (start, rows) in enumerate(ROWS3):
        await_send(a.at[2, pl.ds(0, 3), :, :, :, pl.ds(start, rows), :], a2_send.at[p])
    for s1, s2, base in ((s1a, s2a, 0), (s1b, s2b, 4)):
        for i in range(s1.shape[0]):
            await_send(s1.at[i, pl.ds(0, 7)], r_send.at[0, base + i])
            await_send(s2.at[i, pl.ds(0, 3)], r_send.at[1, base + i])
    await_send(got.at[pl.ds(0, 3)], o_send)
    await_send(s4.at[pl.ds(0, 31)], f_send)


def solution(mesh):
    block_spec = P(("graph", "row"), "col")
    hbm = pl.BlockSpec(memory_space=pl.ANY)
    dma = pltpu.SemaphoreType.DMA

    def device_step(init_blk, graph_blk):
        result = pl.pallas_call(
            mcl_kernel,
            out_shape=pltpu.VMEM((Q, ROWS, BLK), F32),
            in_specs=[hbm, hbm],
            out_specs=pl.BlockSpec(memory_space=pltpu.VMEM),
            scratch_shapes=[
                pltpu.VMEM((Q, ROWS, BLK), F32), pltpu.VMEM((Q, ROWS, BLK), F32),
                pltpu.VMEM((4, 4, N, LANE), BF),
                pltpu.VMEM((3, 4, 2, 4, 2, ROWS, LANE), BF),
                pltpu.VMEM((4, 4, ROWS, LANE), BF),
                pltpu.VMEM((2, 2, ROWS, LANE), BF),
                pltpu.VMEM((4, ROWS, BLK), F32),
                pltpu.VMEM((4, ROWS, BLK), F32),
                pltpu.VMEM((4, 8, 1, BLK), F32),
                pltpu.VMEM((4, 4, 1, BLK), F32),
                pltpu.VMEM((1, 8, 1, PLANE), F32),
                pltpu.VMEM((1, 4, 1, PLANE), F32),
                pltpu.VMEM((Q, 1, BLK), F32), pltpu.VMEM((32, 1, BLK), F32),
                dma((Q,)), dma((Q, Q)), dma((2, Q)),
                dma(()), dma((3,)), dma(()),
                dma(()), dma((3,)), dma(()),
                dma(()), dma((2, Q)), dma((Q,)),
                dma((Q,)), dma((2, Q)), dma((Q,)),
                dma((2, 5)), dma((5,)), dma((5,)),
                dma(()), dma(()),
                dma(()), dma(()), dma((Q + 1, Q)),
            ],
            compiler_params=pltpu.CompilerParams(
                collective_id=0, has_side_effects=True, vmem_limit_bytes=VMEM_BYTES
            ),
        )(init_blk, graph_blk)
        return result.reshape(init_blk.shape)

    return jax.shard_map(device_step, mesh=mesh, in_specs=(block_spec, block_spec), out_specs=block_spec, check_vma=False)
```

```python
import functools

import jax
import jax.numpy as jnp
from jax import lax
from jax.experimental import pallas as pl
from jax.experimental.pallas import tpu as pltpu
from jax.sharding import PartitionSpec as P

MESH = pl.DeviceIdType.MESH
VMEM_BYTES = 58 << 20
BF = jnp.bfloat16
F32 = jnp.float32
N = 8192
PLANE, PIECE, BLK, ROWS, LANE = 2048, 1024, 512, 256, 128
Q = 4
Q0, Q1, Q2, Q3 = range(Q)
NEAR = (1, 3)
XM, XP, YP = 224, 448, 736
ROWS3 = ((0, 80), (80, 80), (160, 64), (224, 32))


def mcl_kernel(
    init_hbm, graph_hbm, out_ref,
    moved, got,
    g, a, stage, hold, acc1, acc2, s1a, s2a, s1b, s2b, s3, s4,
    g_send, g_recv, d_recv, t_send, t_recv, h_recv, az_send, az_recv, az2_recv,
    a1_send, a1_recv, a1_recv2, a2_send, a2_recv, a2_recv2,
    r_send, r_recv1, r_recv2, o_send, o_recv, f_send, f_recv, i_sem,
):
    col, row = lax.axis_index("col"), lax.axis_index("row")
    z, y = lax.div(col, 4), lax.rem(col, 4)
    x, c = lax.div(row, 2), lax.rem(row, 2)

    def plus(v, d):
        return lax.rem(v + d, 4)

    def dev(dx=0, dy=0, dz=0, dc=0):
        return {"col": plus(z, dz) * 4 + plus(y, dy), "row": plus(x, dx) * 2 + lax.rem(c + dc, 2)}

    XPOS, XNEG, YPOS, YNEG = dev(dx=1), dev(dx=3), dev(dy=1), dev(dy=3)
    ZPOS, ZNEG, MATE = dev(dz=1), dev(dz=3), dev(dc=1)

    def send(src, dst, ssem, rsem, device):
        pltpu.make_async_remote_copy(
            src_ref=src, dst_ref=dst, send_sem=ssem, recv_sem=rsem, device_id=device, device_id_type=MESH
        ).start()

    def await_recv(ref, sem):
        pltpu.make_async_remote_copy(
            src_ref=ref, dst_ref=ref, send_sem=sem, recv_sem=sem, device_id=MATE, device_id_type=MESH
        ).wait_recv()

    def await_send(ref, sem):
        pltpu.make_async_remote_copy(
            src_ref=ref, dst_ref=ref, send_sem=sem, recv_sem=sem, device_id=MATE, device_id_type=MESH
        ).wait_send()

    barrier = pltpu.get_barrier_semaphore()
    peers = [dev(dx=dx, dc=dc) for dx in range(Q) for dc in range(2) if (dx, dc) != (0, 0)]
    peers += [dev(dy=dy) for dy in (1, 2, 3)] + [ZPOS, ZNEG]
    for peer in peers:
        pl.semaphore_signal(barrier, inc=1, device_id=peer, device_id_type=MESH)

    init_ref, graph_ref = moved, got
    copies = []
    for q in range(Q + 1):
        lanes = pl.ds(q * LANE, LANE)
        parts = []
        for t in range(Q):
            rows = pl.ds(t * ROWS, ROWS)
            if q == Q:
                parts.append(pltpu.make_async_copy(init_hbm.at[rows], init_ref.at[t], i_sem.at[q, t]))
            else:
                parts.append(
                    pltpu.make_async_copy(graph_hbm.at[rows, lanes], graph_ref.at[t, :, lanes], i_sem.at[q, t])
                )
        copies.append(parts)
    for q in (Q0, Q, Q1, Q2, Q3):
        for copy in copies[q]:
            copy.start()

    def cast_graph(q):
        for copy in copies[q]:
            copy.wait()
        base = pl.multiple_of((x * 2 + c) * PIECE, PIECE)
        lanes = pl.ds(q * LANE, LANE)
        for qr in range(Q):
            for yy in range(2):
                block = graph_ref[yy * 2 + qr // 2, pl.ds(qr % 2 * LANE, LANE), lanes]
                g[q, y, pl.ds(base + qr * ROWS + yy * LANE, LANE), :] = block.astype(BF)

    def cast_init():
        for copy in copies[Q]:
            copy.wait()
        for q in range(Q):
            a[0, z, lax.div(y, 2), q, lax.rem(y, 2)] = init_ref[y, :, pl.ds(q * LANE, LANE)].astype(BF)
        for t in range(Q):
            for q in range(Q):
                stage[t, q] = init_ref[t, :, pl.ds(q * LANE, LANE)].astype(BF)

    cast_graph(Q0)
    pl.semaphore_wait(barrier, len(peers))

    def a0_block(dz, dy, lo=0, n=4):
        yy = plus(y, dy)
        return a.at[0, plus(z, dz), lax.div(yy, 2), pl.ds(lo, n), lax.rem(yy, 2)]

    def a0_spread(group, dys):
        for dy in dys:
            for where in (ZPOS, ZNEG):
                send(a0_block(0, dy), a0_block(0, dy), az_send, az_recv.at[group], where)

    def a0_wait_near():
        for k in range(2):
            await_recv(stage.at[0], t_recv.at[k])

    def a0_wait_far():
        await_recv(stage.at[0], t_recv.at[2])

    def a0_done():
        await_recv(a.at[0, 0], az2_recv)

    def a0_relay(group, dys):
        await_recv(a.at[0, 0, pl.ds(0, len(dys))], az_recv.at[group])
        for dy in dys:
            send(a0_block(3, dy, 0, 2), a0_block(3, dy, 0, 2), az_send, az2_recv, ZPOS)
            send(a0_block(1, dy, 2, 2), a0_block(1, dy, 2, 2), az_send, az2_recv, ZNEG)

    def a0_exchange():
        far = plus(y, 2)
        for side, where in enumerate((YPOS, YNEG)):
            send(stage.at[far, pl.ds(2 * side, 2)], hold.at[side], t_send, h_recv, where)
            send(stage.at[plus(y, NEAR[side])], a0_block(0, 0), t_send, t_recv.at[side], where)

    def a0_pass():
        await_recv(hold, h_recv)
        for side, where in enumerate((YPOS, YNEG)):
            ref = a0_block(0, NEAR[1 - side], 2 * side, 2)
            send(hold.at[side], ref, t_send, t_recv.at[2], where)

    def piece(q, dx, dy, lo=0, hi=PIECE):
        base = (plus(x, dx) * 2 + c) * PIECE
        return g.at[q, plus(y, dy), pl.ds(pl.multiple_of(base + lo, 16), hi - lo), :]

    def hop(q, depth, where, dx, dy, lo=0, hi=PIECE):
        ref = piece(q, dx, dy, lo, hi)
        send(ref, ref, g_send.at[q], g_recv.at[q, depth], where)

    def mate(q, *offsets, last=0):
        for dx, dy in offsets:
            ref = piece(q, dx, dy)
            send(ref, ref, g_send.at[q], d_recv.at[last, q], MATE)

    def arrived(q, depth):
        rows = (4096, 2 * (BLK + 2 * (PIECE - XP)) + 2 * (BLK + 2 * XP), 4096, PIECE)[depth]
        await_recv(g.at[q, 0, pl.ds(0, rows), :], g_recv.at[q, depth])

    def g1(q):
        for where in (XPOS, XNEG, YPOS, YNEG):
            hop(q, 0, where, 0, 0)
        mate(q, (0, 0))

    def g2(q):
        arrived(q, 0)
        hop(q, 1, XPOS, 3, 0, XM, YP)
        hop(q, 1, YPOS, 0, 3, XM, YP)
        for lo, hi in ((0, XM), (YP, PIECE)):
            hop(q, 1, XNEG, 1, 0, lo, hi)
            hop(q, 1, YNEG, 0, 1, lo, hi)
        for d in (1, 3):
            for where in (XPOS, XNEG):
                hop(q, 1, where, 0, d, XP, PIECE)
            for where in (YPOS, YNEG):
                hop(q, 1, where, d, 0, 0, XP)
        mate(q, (1, 0), (3, 0), (0, 1), (0, 3))

    def g3(q):
        arrived(q, 1)
        for where in (XPOS, XNEG):
            hop(q, 2, where, 0, 2, XP, PIECE)
        for where in (YPOS, YNEG):
            hop(q, 2, where, 2, 0, 0, XP)
        for d in (1, 3):
            hop(q, 2, XPOS, 3, d, XP, YP)
            hop(q, 2, XNEG, 1, d, YP, PIECE)
            hop(q, 2, YPOS, d, 3, XM, XP)
            hop(q, 2, YNEG, d, 1, 0, XM)
        mate(q, (2, 0), (0, 2), (1, 1), (1, 3), (3, 1), (3, 3))

    def g4(q):
        arrived(q, 2)
        hop(q, 3, XPOS, 3, 2, XP, YP)
        hop(q, 3, XNEG, 1, 2, YP, PIECE)
        hop(q, 3, YPOS, 2, 3, XM, XP)
        hop(q, 3, YNEG, 2, 1, 0, XM)
        mate(q, (1, 2), (3, 2), (2, 1), (2, 3))

    def g5(q):
        arrived(q, 3)
        mate(q, (2, 2), last=1)

    def g_most(q):
        await_recv(g.at[q, pl.ds(0, 3), pl.ds(0, 5 * PIECE)], d_recv.at[0, q])

    def g_whole(q):
        await_recv(g.at[q, 0, pl.ds(0, PIECE)], d_recv.at[1, q])

    def g_rows(nq, start, n):
        return jnp.concatenate([g[nq, t, pl.ds(start, n), :] for t in range(Q)], axis=1)

    def c1_part(q, zz):
        lhs = jnp.concatenate(
            [a[0, zz, cc, qr, yy] for cc in range(2) for qr in range(Q) for yy in range(2)], axis=1
        )
        acc1[q] += jnp.dot(lhs, g_rows(q, pl.multiple_of(zz * PLANE, PLANE), PLANE), preferred_element_type=F32)

    def c1_most(q):
        def step(i, carry):
            c1_part(q, plus(x, i + lax.div(i, 2)))
            return carry

        acc1[q] = jnp.zeros((ROWS, BLK), F32)
        lax.fori_loop(0, 3, step, 0)

    def c1_rest(q):
        c1_part(q, plus(x, 2))

    def square_sum(ref, q):
        v = ref[q]
        return jnp.sum(v * v, axis=0, keepdims=True)

    def sum_first(s1, i, k):
        me = x * 2 + c
        for dx in range(Q):
            for dc in range(2):
                if (dx, dc) != (0, 0):
                    send(s1.at[i, me], s1.at[i, me], r_send.at[0, k], r_recv1.at[k], dev(dx=dx, dc=dc))

    def sum_second(s1, s2, i, k):
        await_recv(s1.at[i, pl.ds(0, 7)], r_recv1.at[k])
        s2[i, y] = jnp.sum(s1[i], axis=0)
        for dy in (1, 2, 3):
            send(s2.at[i, y], s2.at[i, y], r_send.at[1, k], r_recv2.at[k], dev(dy=dy))

    def sum_last(s2, i, k):
        await_recv(s2.at[i, pl.ds(0, 3)], r_recv2.at[k])

    def c1_sums(q):
        s1a[q, x * 2 + c] = square_sum(acc1, q)
        sum_first(s1a, q, q)

    def c1_second(q):
        sum_second(s1a, s2a, q, q)

    def a1_chunk(dz, q, lo=0, n=2):
        return a.at[1, plus(z, dz), pl.ds(lo, n), q]

    def a1_spread(q):
        sum_last(s2a, q, q)
        scale = N / jnp.sum(s2a[q], axis=0)
        for t in range(Q):
            v = acc1[q, :, pl.ds(t * LANE, LANE)]
            a[1, z, t // 2, q, t % 2] = (v * v * scale[:, t * LANE : t * LANE + LANE]).astype(BF)
        for half in range(2):
            for where, n in ((ZPOS, half), (ZNEG, 1 - half)):
                send(a1_chunk(0, q, n, 1), a1_chunk(0, q, n, 1), a1_send, a1_recv.at[half, q], where)

    def a1_relay(q):
        await_recv(a.at[1, 0, :, 0], a1_recv.at[0, q])
        send(a1_chunk(3, q, 0, 1), a1_chunk(3, q, 0, 1), a1_send, a1_recv2.at[q], ZPOS)
        send(a1_chunk(1, q, 1, 1), a1_chunk(1, q, 1, 1), a1_send, a1_recv2.at[q], ZNEG)

    def c2(q, dz, first=False):
        zz = plus(z, dz)
        lhs = jnp.concatenate([a[1, zz, cc, q, yy] for cc in range(2) for yy in range(2)], axis=1)
        base = pl.multiple_of(zz * PLANE, PLANE)
        for nq in range(Q):
            rhs = jnp.concatenate([g_rows(nq, base + cc * PIECE + q * ROWS, ROWS) for cc in range(2)], axis=0)
            prod = jnp.dot(lhs, rhs, preferred_element_type=F32)
            acc2[nq] = prod if first else acc2[nq] + prod

    def c2_near(q):
        await_recv(a.at[1, 0, :, 0], a1_recv.at[1, q])
        for dz in NEAR:
            c2(q, dz)

    def c2_far(q):
        await_recv(a.at[1, 0, :, 0], a1_recv2.at[q])
        c2(q, 2)

    def c2_sums():
        for q in range(Q):
            s1b[0, x * 2 + c, :, pl.ds(q * BLK, BLK)] = square_sum(acc2, q)
        sum_first(s1b, 0, 4)

    def c2_second():
        sum_second(s1b, s2b, 0, 4)

    def a2_rows(dz, p, lo=0, n=2):
        start, rows = ROWS3[p]
        return a.at[2, plus(z, dz), pl.ds(lo, n), :, :, pl.ds(start, rows), :]

    def a2_scale(p):
        start, rows = ROWS3[p]
        scale = N / jnp.sum(s2b[0], axis=0)
        for q in range(Q):
            for t in range(Q):
                v = acc2[q, pl.ds(start, rows), pl.ds(t * LANE, LANE)]
                s = scale[:, q * BLK + t * LANE : q * BLK + t * LANE + LANE]
                a[2, z, t // 2, q, t % 2, pl.ds(start, rows), :] = (v * v * s).astype(BF)

    def a2_spread(p):
        for half in range(2):
            for where, n in ((ZPOS, half), (ZNEG, 1 - half)):
                send(a2_rows(0, p, n, 1), a2_rows(0, p, n, 1), a2_send.at[p], a2_recv.at[half, p], where)

    def a2_relay(p):
        start, rows = ROWS3[p]
        await_recv(a.at[2, 0, :, :, :, pl.ds(start, rows), :], a2_recv.at[0, p])
        send(a2_rows(3, p, 0, 1), a2_rows(3, p, 0, 1), a2_send.at[p], a2_recv2.at[p], ZPOS)
        send(a2_rows(1, p, 1, 1), a2_rows(1, p, 1, 1), a2_send.at[p], a2_recv2.at[p], ZNEG)

    def c3_part(zz, start, rows, nq, halves=(0, 1)):
        lhs = jnp.concatenate(
            [a[2, zz, cc, qr, yy, pl.ds(start, rows), :] for cc in halves for qr in range(Q) for yy in range(2)],
            axis=1,
        )
        depth = len(halves) * PIECE
        base = pl.multiple_of(zz * PLANE + halves[0] * PIECE, PIECE)
        return jnp.dot(lhs, g_rows(nq, base, depth), preferred_element_type=F32)

    def c3_own():
        def step(nq, carry):
            acc1[nq] = c3_part(z, 0, ROWS, nq)
            return carry

        lax.fori_loop(0, 4, step, 0)

    def c3_first(p, half=0):
        start, rows = ROWS3[p]

        def step(nq, carry):
            part = c3_part(plus(z, 3), start, rows, nq, (half,))
            acc1[nq, pl.ds(start, rows), :] += part + c3_part(plus(z, 1), start, rows, nq, (1 - half,))
            return carry

        lax.fori_loop(0, Q, step, 0)

    def c3_near(p):
        start, rows = ROWS3[p]
        await_recv(a.at[2, 0, :, :, :, pl.ds(start, rows), :], a2_recv.at[1, p])
        c3_first(p, 1)

    def c3_far(p):
        start, rows = ROWS3[p]
        await_recv(a.at[2, 0, :, :, :, pl.ds(start, rows), :], a2_recv2.at[p])
        for nq in range(Q):
            v = acc1[nq, pl.ds(start, rows), :] + c3_part(plus(z, 2), start, rows, nq)
            v = v * v
            part = jnp.sum(v, axis=0, keepdims=True)
            here = pl.ds(nq * LANE, LANE)
            for t in range(Q):
                cut = slice(t * LANE, t * LANE + LANE)
                moved[t, pl.ds(start, rows), here] = v[:, cut]
                if p == 0:
                    s3[t, :, here] = part[:, cut]
                else:
                    s3[t, :, here] += part[:, cut]
        if p == Q3:
            c3_sums()
        for dy in (2, 1, 3):
            send(
                moved.at[plus(y, dy), pl.ds(start, rows), :],
                got.at[y, pl.ds(start, rows), :],
                o_send, o_recv, dev(dy=dy),
            )

    def c3_sums():
        me = y * 8 + x * 2 + c
        s4[me] = s3[y]
        for dy in (2, 1, 3, 0):
            for dx in (2, 1, 3, 0):
                for dc in range(2):
                    if dx + dy + dc:
                        send(s3.at[plus(y, dy)], s4.at[me], f_send, f_recv, dev(dx=dx, dy=dy, dc=dc))

    def finish():
        await_recv(s4.at[pl.ds(0, 31)], f_recv)
        scale = N / jnp.sum(s4[...], axis=0)
        out_ref[y] = moved[y] * scale
        await_recv(got.at[pl.ds(0, 3)], o_recv)
        for dy in (1, 2, 3):
            t = plus(y, dy)
            out_ref[t] = got[t] * scale

    g1(Q0)
    cast_init()
    cast_graph(Q1)
    g1(Q1)
    a0_exchange()
    g2(Q0)
    g2(Q1)
    cast_graph(Q2)
    g1(Q2)
    a0_spread(0, (0,))
    a0_wait_near()
    a0_spread(1, NEAR)
    g3(Q0)
    a0_pass()
    g3(Q1)
    a0_relay(1, NEAR)
    g4(Q0)
    a0_relay(0, (0,))
    g2(Q2)
    a0_wait_far()
    a0_spread(2, (2,))
    g4(Q1)
    cast_graph(Q3)
    g1(Q3)
    g_most(Q0)
    g5(Q0)
    a0_relay(2, (2,))
    a0_done()
    g_whole(Q0)
    c1_most(Q0)
    c1_rest(Q0)
    c1_sums(Q0)
    g5(Q1)
    g_most(Q1)
    g3(Q2)
    g_whole(Q1)
    c1_most(Q1)
    c1_second(Q0)
    c1_rest(Q1)
    c1_sums(Q1)
    g2(Q3)
    a1_spread(Q0)
    c1_second(Q1)
    g4(Q2)
    g3(Q3)
    a1_relay(Q0)
    g5(Q2)
    a1_spread(Q1)
    g_whole(Q2)
    g_most(Q2)
    c1_most(Q2)
    c1_rest(Q2)
    c1_sums(Q2)
    g4(Q3)
    c1_second(Q2)
    a1_relay(Q1)
    g_most(Q3)
    c1_most(Q3)
    g5(Q3)
    a1_spread(Q2)
    g_whole(Q3)
    c1_rest(Q3)
    c1_sums(Q3)
    c1_second(Q3)
    a1_relay(Q2)
    c2(Q0, 0, True)
    a1_spread(Q3)
    c2(Q1, 0)
    c2_near(Q0)
    c2_far(Q0)
    c2(Q2, 0)
    c2_near(Q1)
    a1_relay(Q3)
    c2_far(Q1)
    c2_near(Q2)
    c2_near(Q3)
    c2(Q3, 0)
    c2_far(Q2)
    c2_far(Q3)
    c2_sums()
    c2_second()
    sum_last(s2b, 0, Q)
    a2_scale(Q0)
    a2_spread(Q0)
    for p in (Q1, Q2, Q3):
        a2_scale(p)
    c3_own()
    a2_relay(Q0)
    a2_spread(Q1)
    c3_first(Q0)
    c3_near(Q0)
    a2_relay(Q1)
    a2_spread(Q2)
    c3_far(Q0)
    c3_first(Q1)
    c3_near(Q1)
    a2_relay(Q2)
    a2_spread(Q3)
    c3_far(Q1)
    c3_first(Q2)
    a2_relay(Q3)
    c3_near(Q2)
    c3_far(Q2)
    c3_first(Q3)
    c3_near(Q3)
    c3_far(Q3)
    finish()

    for q in range(Q):
        await_send(g.at[q, :, pl.ds(0, 7936), :], g_send.at[q])
    await_send(stage, t_send)
    await_send(a.at[0, pl.ds(0, 3)], az_send)
    await_send(a.at[1, pl.ds(0, 3)], a1_send)
    for p, (start, rows) in enumerate(ROWS3):
        await_send(a.at[2, pl.ds(0, 3), :, :, :, pl.ds(start, rows), :], a2_send.at[p])
    for s1, s2, base in ((s1a, s2a, 0), (s1b, s2b, 4)):
        for i in range(s1.shape[0]):
            await_send(s1.at[i, pl.ds(0, 7)], r_send.at[0, base + i])
            await_send(s2.at[i, pl.ds(0, 3)], r_send.at[1, base + i])
    await_send(got.at[pl.ds(0, 3)], o_send)
    await_send(s4.at[pl.ds(0, 31)], f_send)


def solution(mesh):
    block_spec = P(("graph", "row"), "col")
    hbm = pl.BlockSpec(memory_space=pl.ANY)
    dma = pltpu.SemaphoreType.DMA

    def device_step(init_blk, graph_blk):
        result = pl.pallas_call(
            mcl_kernel,
            out_shape=pltpu.VMEM((Q, ROWS, BLK), F32),
            in_specs=[hbm, hbm],
            out_specs=pl.BlockSpec(memory_space=pltpu.VMEM),
            scratch_shapes=[
                pltpu.VMEM((Q, ROWS, BLK), F32), pltpu.VMEM((Q, ROWS, BLK), F32),
                pltpu.VMEM((4, 4, N, LANE), BF),
                pltpu.VMEM((3, 4, 2, 4, 2, ROWS, LANE), BF),
                pltpu.VMEM((4, 4, ROWS, LANE), BF),
                pltpu.VMEM((2, 2, ROWS, LANE), BF),
                pltpu.VMEM((4, ROWS, BLK), F32),
                pltpu.VMEM((4, ROWS, BLK), F32),
                pltpu.VMEM((4, 8, 1, BLK), F32),
                pltpu.VMEM((4, 4, 1, BLK), F32),
                pltpu.VMEM((1, 8, 1, PLANE), F32),
                pltpu.VMEM((1, 4, 1, PLANE), F32),
                pltpu.VMEM((Q, 1, BLK), F32), pltpu.VMEM((32, 1, BLK), F32),
                dma((Q,)), dma((Q, Q)), dma((2, Q)),
                dma(()), dma((3,)), dma(()),
                dma(()), dma((3,)), dma(()),
                dma(()), dma((2, Q)), dma((Q,)),
                dma((Q,)), dma((2, Q)), dma((Q,)),
                dma((2, 5)), dma((5,)), dma((5,)),
                dma(()), dma(()),
                dma(()), dma(()), dma((Q + 1, Q)),
            ],
            compiler_params=pltpu.CompilerParams(
                collective_id=0, has_side_effects=True, vmem_limit_bytes=VMEM_BYTES
            ),
        )(init_blk, graph_blk)
        return result.reshape(init_blk.shape)

    return jax.shard_map(device_step, mesh=mesh, in_specs=(block_spec, block_spec), out_specs=block_spec, check_vma=False)
```

```python
import functools

import jax
import jax.numpy as jnp
from jax import lax
from jax.experimental import pallas as pl
from jax.experimental.pallas import tpu as pltpu
from jax.sharding import PartitionSpec as P

MESH = pl.DeviceIdType.MESH
VMEM_BYTES = 58 << 20
BF = jnp.bfloat16
F32 = jnp.float32
N = 8192
PLANE, PIECE, BLK, ROWS, LANE = 2048, 1024, 512, 256, 128
Q = 4
Q0, Q1, Q2, Q3, Q4 = range(Q + 1)
NEAR = (1, 3)
XM, XP, YP = 224, 448, 736
EARLY = 32
ROWS3 = ((0, EARLY), (32, 80), (112, 64), (176, 48), (224, 32))


def mcl_kernel(
    init_hbm, graph_hbm, out_ref,
    moved, got,
    g, a, stage, hold, acc1, acc2, s1a, s2a, s1b, s2b, s3, s4, early, scales,
    g_send, g_recv, d_recv, t_send, t_recv, h_recv, az_send, az_recv, az2_recv,
    a1_send, a1_recv, a1_recv2, a2_send, a2_recv, a2_recv2,
    r_send, r_recv1, r_recv2, e_send, e_recv, v_send, v_recv, o_send, o_recv, f_send, f_recv, i_sem,
):
    col, row = lax.axis_index("col"), lax.axis_index("row")
    z, y = lax.div(col, 4), lax.rem(col, 4)
    x, c = lax.div(row, 2), lax.rem(row, 2)

    def plus(v, d):
        return lax.rem(v + d, 4)

    def dev(dx=0, dy=0, dz=0, dc=0):
        return {"col": plus(z, dz) * 4 + plus(y, dy), "row": plus(x, dx) * 2 + lax.rem(c + dc, 2)}

    XPOS, XNEG, YPOS, YNEG = dev(dx=1), dev(dx=3), dev(dy=1), dev(dy=3)
    ZPOS, ZNEG, MATE = dev(dz=1), dev(dz=3), dev(dc=1)

    def send(src, dst, ssem, rsem, device):
        pltpu.make_async_remote_copy(
            src_ref=src, dst_ref=dst, send_sem=ssem, recv_sem=rsem, device_id=device, device_id_type=MESH
        ).start()

    def await_recv(ref, sem):
        pltpu.make_async_remote_copy(
            src_ref=ref, dst_ref=ref, send_sem=sem, recv_sem=sem, device_id=MATE, device_id_type=MESH
        ).wait_recv()

    def await_send(ref, sem):
        pltpu.make_async_remote_copy(
            src_ref=ref, dst_ref=ref, send_sem=sem, recv_sem=sem, device_id=MATE, device_id_type=MESH
        ).wait_send()

    barrier = pltpu.get_barrier_semaphore()
    peers = [dev(dx=dx, dc=dc) for dx in range(Q) for dc in range(2) if (dx, dc) != (0, 0)]
    peers += [dev(dy=dy) for dy in (1, 2, 3)] + [ZPOS, ZNEG]
    for peer in peers:
        pl.semaphore_signal(barrier, inc=1, device_id=peer, device_id_type=MESH)

    init_ref, graph_ref = moved, got
    copies = []
    for q in range(Q + 1):
        lanes = pl.ds(q * LANE, LANE)
        parts = []
        for t in range(Q):
            rows = pl.ds(t * ROWS, ROWS)
            if q == Q:
                parts.append(pltpu.make_async_copy(init_hbm.at[rows], init_ref.at[t], i_sem.at[q, t]))
            else:
                parts.append(
                    pltpu.make_async_copy(graph_hbm.at[rows, lanes], graph_ref.at[t, :, lanes], i_sem.at[q, t])
                )
        copies.append(parts)
    for q in (Q0, Q, Q1, Q2, Q3):
        for copy in copies[q]:
            copy.start()

    def cast_graph(q):
        for copy in copies[q]:
            copy.wait()
        base = pl.multiple_of((x * 2 + c) * PIECE, PIECE)
        lanes = pl.ds(q * LANE, LANE)
        for qr in range(Q):
            for yy in range(2):
                block = graph_ref[yy * 2 + qr // 2, pl.ds(qr % 2 * LANE, LANE), lanes]
                g[q, y, pl.ds(base + qr * ROWS + yy * LANE, LANE), :] = block.astype(BF)

    def cast_init():
        for copy in copies[Q]:
            copy.wait()
        for q in range(Q):
            a[0, z, lax.div(y, 2), q, lax.rem(y, 2)] = init_ref[y, :, pl.ds(q * LANE, LANE)].astype(BF)
        for t in range(Q):
            for q in range(Q):
                stage[t, q] = init_ref[t, :, pl.ds(q * LANE, LANE)].astype(BF)

    cast_graph(Q0)
    pl.semaphore_wait(barrier, len(peers))

    def a0_block(dz, dy, lo=0, n=4):
        yy = plus(y, dy)
        return a.at[0, plus(z, dz), lax.div(yy, 2), pl.ds(lo, n), lax.rem(yy, 2)]

    def a0_spread(group, dys):
        for dy in dys:
            for where in (ZPOS, ZNEG):
                send(a0_block(0, dy), a0_block(0, dy), az_send, az_recv.at[group], where)

    def a0_wait_near():
        for k in range(2):
            await_recv(stage.at[0], t_recv.at[k])

    def a0_wait_far():
        await_recv(stage.at[0], t_recv.at[2])

    def a0_done():
        await_recv(a.at[0, 0], az2_recv)

    def a0_relay(group, dys):
        await_recv(a.at[0, 0, pl.ds(0, len(dys))], az_recv.at[group])
        for dy in dys:
            send(a0_block(3, dy, 0, 2), a0_block(3, dy, 0, 2), az_send, az2_recv, ZPOS)
            send(a0_block(1, dy, 2, 2), a0_block(1, dy, 2, 2), az_send, az2_recv, ZNEG)

    def a0_exchange():
        far = plus(y, 2)
        for side, where in enumerate((YPOS, YNEG)):
            send(stage.at[far, pl.ds(2 * side, 2)], hold.at[side], t_send, h_recv, where)
            send(stage.at[plus(y, NEAR[side])], a0_block(0, 0), t_send, t_recv.at[side], where)

    def a0_pass():
        await_recv(hold, h_recv)
        for side, where in enumerate((YPOS, YNEG)):
            ref = a0_block(0, NEAR[1 - side], 2 * side, 2)
            send(hold.at[side], ref, t_send, t_recv.at[2], where)

    def piece(q, dx, dy, lo=0, hi=PIECE):
        base = (plus(x, dx) * 2 + c) * PIECE
        return g.at[q, plus(y, dy), pl.ds(pl.multiple_of(base + lo, 16), hi - lo), :]

    def hop(q, depth, where, dx, dy, lo=0, hi=PIECE):
        ref = piece(q, dx, dy, lo, hi)
        send(ref, ref, g_send.at[q], g_recv.at[q, depth], where)

    def mate(q, *offsets, last=0):
        for dx, dy in offsets:
            ref = piece(q, dx, dy)
            send(ref, ref, g_send.at[q], d_recv.at[last, q], MATE)

    def arrived(q, depth):
        rows = (4096, 2 * (BLK + 2 * (PIECE - XP)) + 2 * (BLK + 2 * XP), 4096, PIECE)[depth]
        await_recv(g.at[q, 0, pl.ds(0, rows), :], g_recv.at[q, depth])

    def g1(q):
        for where in (XPOS, XNEG, YPOS, YNEG):
            hop(q, 0, where, 0, 0)
        mate(q, (0, 0))

    def g2(q):
        arrived(q, 0)
        hop(q, 1, XPOS, 3, 0, XM, YP)
        hop(q, 1, YPOS, 0, 3, XM, YP)
        for lo, hi in ((0, XM), (YP, PIECE)):
            hop(q, 1, XNEG, 1, 0, lo, hi)
            hop(q, 1, YNEG, 0, 1, lo, hi)
        for d in (1, 3):
            for where in (XPOS, XNEG):
                hop(q, 1, where, 0, d, XP, PIECE)
            for where in (YPOS, YNEG):
                hop(q, 1, where, d, 0, 0, XP)
        mate(q, (1, 0), (3, 0), (0, 1), (0, 3))

    def g3(q):
        arrived(q, 1)
        for where in (XPOS, XNEG):
            hop(q, 2, where, 0, 2, XP, PIECE)
        for where in (YPOS, YNEG):
            hop(q, 2, where, 2, 0, 0, XP)
        for d in (1, 3):
            hop(q, 2, XPOS, 3, d, XP, YP)
            hop(q, 2, XNEG, 1, d, YP, PIECE)
            hop(q, 2, YPOS, d, 3, XM, XP)
            hop(q, 2, YNEG, d, 1, 0, XM)
        mate(q, (2, 0), (0, 2), (1, 1), (1, 3), (3, 1), (3, 3))

    def g4(q):
        arrived(q, 2)
        hop(q, 3, XPOS, 3, 2, XP, YP)
        hop(q, 3, XNEG, 1, 2, YP, PIECE)
        hop(q, 3, YPOS, 2, 3, XM, XP)
        hop(q, 3, YNEG, 2, 1, 0, XM)
        mate(q, (1, 2), (3, 2), (2, 1), (2, 3))

    def g5(q):
        arrived(q, 3)
        mate(q, (2, 2), last=1)

    def g_most(q):
        await_recv(g.at[q, pl.ds(0, 3), pl.ds(0, 5 * PIECE)], d_recv.at[0, q])

    def g_whole(q):
        await_recv(g.at[q, 0, pl.ds(0, PIECE)], d_recv.at[1, q])

    def g_rows(nq, start, n):
        return jnp.concatenate([g[nq, t, pl.ds(start, n), :] for t in range(Q)], axis=1)

    def c1_part(q, zz):
        lhs = jnp.concatenate(
            [a[0, zz, cc, qr, yy] for cc in range(2) for qr in range(Q) for yy in range(2)], axis=1
        )
        acc1[q] += jnp.dot(lhs, g_rows(q, pl.multiple_of(zz * PLANE, PLANE), PLANE), preferred_element_type=F32)

    def c1_most(q):
        def step(i, carry):
            c1_part(q, plus(x, i + lax.div(i, 2)))
            return carry

        acc1[q] = jnp.zeros((ROWS, BLK), F32)
        lax.fori_loop(0, 3, step, 0)

    def c1_rest(q):
        c1_part(q, plus(x, 2))

    def square_sum(ref, q):
        v = ref[q]
        return jnp.sum(v * v, axis=0, keepdims=True)

    def sum_first(s1, i, k):
        me = x * 2 + c
        for dx in range(Q):
            for dc in range(2):
                if (dx, dc) != (0, 0):
                    send(s1.at[i, me], s1.at[i, me], r_send.at[0, k], r_recv1.at[k], dev(dx=dx, dc=dc))

    def sum_second(s1, s2, i, k):
        await_recv(s1.at[i, pl.ds(0, 7)], r_recv1.at[k])
        s2[i, y] = jnp.sum(s1[i], axis=0)
        for dy in (1, 2, 3):
            send(s2.at[i, y], s2.at[i, y], r_send.at[1, k], r_recv2.at[k], dev(dy=dy))

    def sum_last(s2, i, k):
        await_recv(s2.at[i, pl.ds(0, 3)], r_recv2.at[k])

    def c1_sums(q):
        s1a[q, x * 2 + c] = square_sum(acc1, q)
        sum_first(s1a, q, q)

    def c1_second(q):
        sum_second(s1a, s2a, q, q)

    def a1_chunk(dz, q, lo=0, n=2):
        return a.at[1, plus(z, dz), pl.ds(lo, n), q]

    def a1_spread(q):
        sum_last(s2a, q, q)
        scale = N / jnp.sum(s2a[q], axis=0)
        for t in range(Q):
            v = acc1[q, :, pl.ds(t * LANE, LANE)]
            a[1, z, t // 2, q, t % 2] = (v * v * scale[:, t * LANE : t * LANE + LANE]).astype(BF)
        for half in range(2):
            for where, n in ((ZPOS, half), (ZNEG, 1 - half)):
                send(a1_chunk(0, q, n, 1), a1_chunk(0, q, n, 1), a1_send, a1_recv.at[half, q], where)

    def a1_relay(q):
        await_recv(a.at[1, 0, :, 0], a1_recv.at[0, q])
        send(a1_chunk(3, q, 0, 1), a1_chunk(3, q, 0, 1), a1_send, a1_recv2.at[q], ZPOS)
        send(a1_chunk(1, q, 1, 1), a1_chunk(1, q, 1, 1), a1_send, a1_recv2.at[q], ZNEG)

    def c2(q, dz, first=False):
        zz = plus(z, dz)
        lhs = jnp.concatenate([a[1, zz, cc, q, yy] for cc in range(2) for yy in range(2)], axis=1)
        base = pl.multiple_of(zz * PLANE, PLANE)
        for nq in range(Q):
            rhs = jnp.concatenate([g_rows(nq, base + cc * PIECE + q * ROWS, ROWS) for cc in range(2)], axis=0)
            prod = jnp.dot(lhs, rhs, preferred_element_type=F32)
            acc2[nq] = prod if first else acc2[nq] + prod

    def c2_near(q):
        await_recv(a.at[1, 0, :, 0], a1_recv.at[1, q])
        for dz in NEAR:
            c2(q, dz)

    def c2_far(q):
        await_recv(a.at[1, 0, :, 0], a1_recv2.at[q])
        c2(q, 2)

    def c2_sums():
        for q in range(Q):
            s1b[0, x * 2 + c, :, pl.ds(q * BLK, BLK)] = square_sum(acc2, q)
        sum_first(s1b, 0, 4)

    def c2_second():
        sum_second(s1b, s2b, 0, 4)

    def early_part(dz, lo=0, n=2):
        return early.at[plus(z, dz), pl.ds(lo, n)]

    def early_spread():
        for half in range(2):
            for where, n in ((ZPOS, half), (ZNEG, 1 - half)):
                src = acc2.at[pl.ds(2 * n, 2), pl.ds(0, EARLY), :]
                send(src, early_part(0, 2 * n), e_send, e_recv.at[half], where)

    def early_relay():
        await_recv(early.at[0], e_recv.at[0])
        send(early_part(3), early_part(3), e_send, e_recv.at[2], ZPOS)
        send(early_part(1, 2), early_part(1, 2), e_send, e_recv.at[2], ZNEG)

    def a2_scales():
        sum_last(s2b, 0, Q)
        scales[z] = N / jnp.sum(s2b[0], axis=0)
        for dz in (2, 1, 3):
            send(scales.at[z], scales.at[z], v_send, v_recv, dev(dz=dz))

    def scaled(v, zz, q, t, rows):
        lanes = pl.ds(q * BLK + t * LANE, LANE)
        a[2, zz, t // 2, q, t % 2, rows, :] = (v * v * scales[zz, :, lanes]).astype(BF)

    def early_scale(dz):
        zz = plus(z, dz)
        for q in range(Q):
            for t in range(Q):
                scaled(early[zz, q, :, pl.ds(t * LANE, LANE)], zz, q, t, pl.ds(0, EARLY))

    def early_near():
        await_recv(early.at[0], e_recv.at[1])
        await_recv(scales.at[pl.ds(0, 3)], v_recv)
        for dz in NEAR:
            early_scale(dz)
        for half in range(2):
            c3_first(Q0, half)

    def early_far():
        await_recv(early.at[0], e_recv.at[2])
        early_scale(2)
        c3_far(Q0)

    def a2_rows(dz, p, lo=0, n=2):
        start, rows = ROWS3[p]
        return a.at[2, plus(z, dz), pl.ds(lo, n), :, :, pl.ds(start, rows), :]

    def a2_scale(p):
        rows = pl.ds(*ROWS3[p])
        for q in range(Q):
            for t in range(Q):
                scaled(acc2[q, rows, pl.ds(t * LANE, LANE)], z, q, t, rows)

    def a2_spread(p):
        for half in range(2):
            for where, n in ((ZPOS, half), (ZNEG, 1 - half)):
                send(a2_rows(0, p, n, 1), a2_rows(0, p, n, 1), a2_send.at[p], a2_recv.at[half, p], where)

    def a2_relay(p):
        start, rows = ROWS3[p]
        await_recv(a.at[2, 0, :, :, :, pl.ds(start, rows), :], a2_recv.at[0, p])
        send(a2_rows(3, p, 0, 1), a2_rows(3, p, 0, 1), a2_send.at[p], a2_recv2.at[p], ZPOS)
        send(a2_rows(1, p, 1, 1), a2_rows(1, p, 1, 1), a2_send.at[p], a2_recv2.at[p], ZNEG)

    def c3_part(zz, start, rows, nq, halves=(0, 1)):
        lhs = jnp.concatenate(
            [a[2, zz, cc, qr, yy, pl.ds(start, rows), :] for cc in halves for qr in range(Q) for yy in range(2)],
            axis=1,
        )
        depth = len(halves) * PIECE
        base = pl.multiple_of(zz * PLANE + halves[0] * PIECE, PIECE)
        return jnp.dot(lhs, g_rows(nq, base, depth), preferred_element_type=F32)

    def c3_own():
        def step(nq, carry):
            acc1[nq] = c3_part(z, 0, ROWS, nq)
            return carry

        lax.fori_loop(0, 4, step, 0)

    def c3_first(p, half=0):
        start, rows = ROWS3[p]

        def step(nq, carry):
            part = c3_part(plus(z, 3), start, rows, nq, (half,))
            acc1[nq, pl.ds(start, rows), :] += part + c3_part(plus(z, 1), start, rows, nq, (1 - half,))
            return carry

        lax.fori_loop(0, Q, step, 0)

    def c3_near(p):
        start, rows = ROWS3[p]
        await_recv(a.at[2, 0, :, :, :, pl.ds(start, rows), :], a2_recv.at[1, p])
        c3_first(p, 1)

    def c3_far(p):
        start, rows = ROWS3[p]
        if p:
            await_recv(a.at[2, 0, :, :, :, pl.ds(start, rows), :], a2_recv2.at[p])
        for nq in range(Q):
            v = acc1[nq, pl.ds(start, rows), :] + c3_part(plus(z, 2), start, rows, nq)
            v = v * v
            part = jnp.sum(v, axis=0, keepdims=True)
            here = pl.ds(nq * LANE, LANE)
            for t in range(Q):
                cut = slice(t * LANE, t * LANE + LANE)
                moved[t, pl.ds(start, rows), here] = v[:, cut]
                if p == 0:
                    s3[t, :, here] = part[:, cut]
                else:
                    s3[t, :, here] += part[:, cut]
        if p == Q4:
            c3_sums()
        for dy in (2, 1, 3):
            send(
                moved.at[plus(y, dy), pl.ds(start, rows), :],
                got.at[y, pl.ds(start, rows), :],
                o_send, o_recv, dev(dy=dy),
            )

    def c3_sums():
        me = y * 8 + x * 2 + c
        s4[me] = s3[y]
        for dy in (2, 1, 3, 0):
            for dx in (2, 1, 3, 0):
                for dc in range(2):
                    if dx + dy + dc:
                        send(s3.at[plus(y, dy)], s4.at[me], f_send, f_recv, dev(dx=dx, dy=dy, dc=dc))

    def finish():
        await_recv(s4.at[pl.ds(0, 31)], f_recv)
        scale = N / jnp.sum(s4[...], axis=0)
        out_ref[y] = moved[y] * scale
        await_recv(got.at[pl.ds(0, 3)], o_recv)
        for dy in (1, 2, 3):
            t = plus(y, dy)
            out_ref[t] = got[t] * scale

    g1(Q0)
    cast_init()
    cast_graph(Q1)
    g1(Q1)
    a0_exchange()
    g2(Q0)
    g2(Q1)
    cast_graph(Q2)
    g1(Q2)
    a0_spread(0, (0,))
    a0_wait_near()
    a0_spread(1, NEAR)
    g3(Q0)
    a0_pass()
    g3(Q1)
    a0_relay(1, NEAR)
    g4(Q0)
    a0_relay(0, (0,))
    g2(Q2)
    a0_wait_far()
    a0_spread(2, (2,))
    g4(Q1)
    cast_graph(Q3)
    g1(Q3)
    g_most(Q0)
    g5(Q0)
    a0_relay(2, (2,))
    a0_done()
    g_whole(Q0)
    c1_most(Q0)
    c1_rest(Q0)
    c1_sums(Q0)
    g5(Q1)
    g_most(Q1)
    g3(Q2)
    g_whole(Q1)
    c1_most(Q1)
    c1_second(Q0)
    c1_rest(Q1)
    c1_sums(Q1)
    g2(Q3)
    a1_spread(Q0)
    c1_second(Q1)
    g4(Q2)
    g3(Q3)
    a1_relay(Q0)
    g5(Q2)
    a1_spread(Q1)
    g_whole(Q2)
    g_most(Q2)
    c1_most(Q2)
    c1_rest(Q2)
    c1_sums(Q2)
    g4(Q3)
    c1_second(Q2)
    a1_relay(Q1)
    g_most(Q3)
    c1_most(Q3)
    g5(Q3)
    a1_spread(Q2)
    g_whole(Q3)
    c1_rest(Q3)
    c1_sums(Q3)
    c1_second(Q3)
    a1_relay(Q2)
    c2(Q0, 0, True)
    a1_spread(Q3)
    c2(Q1, 0)
    c2_near(Q0)
    c2_far(Q0)
    c2(Q2, 0)
    c2_near(Q1)
    a1_relay(Q3)
    c2_far(Q1)
    c2_near(Q2)
    c2_near(Q3)
    c2(Q3, 0)
    c2_far(Q2)
    c2_far(Q3)
    early_spread()
    c2_sums()
    c2_second()
    early_relay()
    a2_scales()
    a2_scale(Q1)
    a2_spread(Q1)
    for p in (Q0, Q2, Q3, Q4):
        a2_scale(p)
    c3_own()
    early_near()
    a2_relay(Q1)
    a2_spread(Q2)
    early_far()
    c3_first(Q1)
    c3_near(Q1)
    c3_far(Q1)
    a2_relay(Q2)
    a2_spread(Q3)
    c3_first(Q2)
    c3_near(Q2)
    c3_far(Q2)
    a2_relay(Q3)
    a2_spread(Q4)
    c3_first(Q3)
    c3_near(Q3)
    c3_far(Q3)
    a2_relay(Q4)
    c3_first(Q4)
    c3_near(Q4)
    c3_far(Q4)
    finish()

    for q in range(Q):
        await_send(g.at[q, :, pl.ds(0, 7936), :], g_send.at[q])
    await_send(stage, t_send)
    await_send(a.at[0, pl.ds(0, 3)], az_send)
    await_send(a.at[1, pl.ds(0, 3)], a1_send)
    await_send(early.at[pl.ds(0, 3)], e_send)
    await_send(scales.at[pl.ds(0, 3)], v_send)
    for p, (start, rows) in enumerate(ROWS3[1:], 1):
        await_send(a.at[2, pl.ds(0, 3), :, :, :, pl.ds(start, rows), :], a2_send.at[p])
    for s1, s2, base in ((s1a, s2a, 0), (s1b, s2b, 4)):
        for i in range(s1.shape[0]):
            await_send(s1.at[i, pl.ds(0, 7)], r_send.at[0, base + i])
            await_send(s2.at[i, pl.ds(0, 3)], r_send.at[1, base + i])
    await_send(got.at[pl.ds(0, 3)], o_send)
    await_send(s4.at[pl.ds(0, 31)], f_send)


def solution(mesh):
    block_spec = P(("graph", "row"), "col")
    hbm = pl.BlockSpec(memory_space=pl.ANY)
    dma = pltpu.SemaphoreType.DMA

    def device_step(init_blk, graph_blk):
        result = pl.pallas_call(
            mcl_kernel,
            out_shape=pltpu.VMEM((Q, ROWS, BLK), F32),
            in_specs=[hbm, hbm],
            out_specs=pl.BlockSpec(memory_space=pltpu.VMEM),
            scratch_shapes=[
                pltpu.VMEM((Q, ROWS, BLK), F32), pltpu.VMEM((Q, ROWS, BLK), F32),
                pltpu.VMEM((4, 4, N, LANE), BF),
                pltpu.VMEM((3, 4, 2, 4, 2, ROWS, LANE), BF),
                pltpu.VMEM((4, 4, ROWS, LANE), BF),
                pltpu.VMEM((2, 2, ROWS, LANE), BF),
                pltpu.VMEM((4, ROWS, BLK), F32),
                pltpu.VMEM((4, ROWS, BLK), F32),
                pltpu.VMEM((4, 8, 1, BLK), F32),
                pltpu.VMEM((4, 4, 1, BLK), F32),
                pltpu.VMEM((1, 8, 1, PLANE), F32),
                pltpu.VMEM((1, 4, 1, PLANE), F32),
                pltpu.VMEM((Q, 1, BLK), F32), pltpu.VMEM((32, 1, BLK), F32),
                pltpu.VMEM((Q, Q, EARLY, BLK), F32), pltpu.VMEM((Q, 1, PLANE), F32),
                dma((Q,)), dma((Q, Q)), dma((2, Q)),
                dma(()), dma((3,)), dma(()),
                dma(()), dma((3,)), dma(()),
                dma(()), dma((2, Q)), dma((Q,)),
                dma((Q + 1,)), dma((2, Q + 1)), dma((Q + 1,)),
                dma((2, 5)), dma((5,)), dma((5,)),
                dma(()), dma((3,)), dma(()), dma(()),
                dma(()), dma(()),
                dma(()), dma(()), dma((Q + 1, Q)),
            ],
            compiler_params=pltpu.CompilerParams(
                collective_id=0, has_side_effects=True, vmem_limit_bytes=VMEM_BYTES
            ),
        )(init_blk, graph_blk)
        return result.reshape(init_blk.shape)

    return jax.shard_map(device_step, mesh=mesh, in_specs=(block_spec, block_spec), out_specs=block_spec, check_vma=False)
```

```python
import functools

import jax
import jax.numpy as jnp
from jax import lax
from jax.experimental import pallas as pl
from jax.experimental.pallas import tpu as pltpu
from jax.sharding import PartitionSpec as P

MESH = pl.DeviceIdType.MESH
VMEM_BYTES = 58 << 20
BF = jnp.bfloat16
F32 = jnp.float32
N = 8192
PLANE, PIECE, BLK, ROWS, LANE = 2048, 1024, 512, 256, 128
Q = 4
Q0, Q1, Q2, Q3 = range(Q)
NEAR = (1, 3)
FAR_FIRST = (2, 1, 3, 0)
DIRECT = (Q2, Q3)
XM, XP, YP = 224, 448, 736
EARLY = 32
ROWS3 = ((0, EARLY), (32, 80), (112, 96), (208, 48))


def mcl_kernel(
    init_hbm, graph_hbm, out_ref,
    moved, got,
    g, a, stage, hold, acc1, acc2, s1a, s2a, s1b, s2b, s3, s4, early, scales,
    g_send, g_recv, d_recv, t_send, t_recv, h_recv, az_send, az_recv, az2_recv,
    a1_send, a1_recv, a1_recv2, a2_send, a2_recv, a2_recv2,
    r_send, r_recv1, r_recv2, e_send, e_recv, v_send, v_recv, o_send, o_recv, p_send, p_recv, i_sem,
):
    col, row = lax.axis_index("col"), lax.axis_index("row")
    z, y = lax.div(col, 4), lax.rem(col, 4)
    x, c = lax.div(row, 2), lax.rem(row, 2)

    def plus(v, d):
        return lax.rem(v + d, 4)

    def dev(dx=0, dy=0, dz=0, dc=0):
        return {"col": plus(z, dz) * 4 + plus(y, dy), "row": plus(x, dx) * 2 + lax.rem(c + dc, 2)}

    XPOS, XNEG, YPOS, YNEG = dev(dx=1), dev(dx=3), dev(dy=1), dev(dy=3)
    ZPOS, ZNEG, MATE = dev(dz=1), dev(dz=3), dev(dc=1)

    def send(src, dst, ssem, rsem, device):
        pltpu.make_async_remote_copy(
            src_ref=src, dst_ref=dst, send_sem=ssem, recv_sem=rsem, device_id=device, device_id_type=MESH
        ).start()

    def await_recv(ref, sem):
        pltpu.make_async_remote_copy(
            src_ref=ref, dst_ref=ref, send_sem=sem, recv_sem=sem, device_id=MATE, device_id_type=MESH
        ).wait_recv()

    def await_send(ref, sem):
        pltpu.make_async_remote_copy(
            src_ref=ref, dst_ref=ref, send_sem=sem, recv_sem=sem, device_id=MATE, device_id_type=MESH
        ).wait_send()

    barrier = pltpu.get_barrier_semaphore()
    peers = [dev(dx=dx, dc=dc) for dx in range(Q) for dc in range(2) if (dx, dc) != (0, 0)]
    peers += [dev(dy=dy) for dy in (1, 2, 3)] + [ZPOS, ZNEG]
    for peer in peers:
        pl.semaphore_signal(barrier, inc=1, device_id=peer, device_id_type=MESH)

    init_ref, graph_ref = moved, got
    copies = []
    for q in range(Q + 1):
        lanes = pl.ds(q * LANE, LANE)
        parts = []
        for t in range(Q):
            rows = pl.ds(t * ROWS, ROWS)
            if q == Q:
                parts.append(pltpu.make_async_copy(init_hbm.at[rows], init_ref.at[t], i_sem.at[q, t]))
            else:
                parts.append(
                    pltpu.make_async_copy(graph_hbm.at[rows, lanes], graph_ref.at[t, :, lanes], i_sem.at[q, t])
                )
        copies.append(parts)
    for q in (Q0, Q, Q1, Q2, Q3):
        for copy in copies[q]:
            copy.start()

    def cast_graph(q):
        for copy in copies[q]:
            copy.wait()
        base = pl.multiple_of((x * 2 + c) * PIECE, PIECE)
        lanes = pl.ds(q * LANE, LANE)
        for qr in range(Q):
            for yy in range(2):
                block = graph_ref[yy * 2 + qr // 2, pl.ds(qr % 2 * LANE, LANE), lanes]
                g[q, y, pl.ds(base + qr * ROWS + yy * LANE, LANE), :] = block.astype(BF)

    def cast_init():
        for copy in copies[Q]:
            copy.wait()
        for q in range(Q):
            a[0, z, lax.div(y, 2), q, lax.rem(y, 2)] = init_ref[y, :, pl.ds(q * LANE, LANE)].astype(BF)
        for t in range(Q):
            for q in range(Q):
                stage[t, q] = init_ref[t, :, pl.ds(q * LANE, LANE)].astype(BF)

    cast_graph(Q0)
    pl.semaphore_wait(barrier, len(peers))

    def a0_block(dz, dy, lo=0, n=4):
        yy = plus(y, dy)
        return a.at[0, plus(z, dz), lax.div(yy, 2), pl.ds(lo, n), lax.rem(yy, 2)]

    def a0_spread(group, dys):
        for dy in dys:
            for where in (ZPOS, ZNEG):
                send(a0_block(0, dy), a0_block(0, dy), az_send, az_recv.at[group], where)

    def a0_wait_near():
        for k in range(2):
            await_recv(stage.at[0], t_recv.at[k])

    def a0_wait_far():
        await_recv(stage.at[0], t_recv.at[2])

    def a0_done():
        await_recv(a.at[0, 0], az2_recv)

    def a0_relay(group, dys):
        await_recv(a.at[0, 0, pl.ds(0, len(dys))], az_recv.at[group])
        for dy in dys:
            send(a0_block(3, dy, 0, 2), a0_block(3, dy, 0, 2), az_send, az2_recv, ZPOS)
            send(a0_block(1, dy, 2, 2), a0_block(1, dy, 2, 2), az_send, az2_recv, ZNEG)

    def a0_exchange():
        far = plus(y, 2)
        for side, where in enumerate((YPOS, YNEG)):
            send(stage.at[far, pl.ds(2 * side, 2)], hold.at[side], t_send, h_recv, where)
            send(stage.at[plus(y, NEAR[side])], a0_block(0, 0), t_send, t_recv.at[side], where)

    def a0_pass():
        await_recv(hold, h_recv)
        for side, where in enumerate((YPOS, YNEG)):
            ref = a0_block(0, NEAR[1 - side], 2 * side, 2)
            send(hold.at[side], ref, t_send, t_recv.at[2], where)

    def piece(q, dx, dy, lo=0, hi=PIECE):
        base = (plus(x, dx) * 2 + c) * PIECE
        return g.at[q, plus(y, dy), pl.ds(pl.multiple_of(base + lo, 16), hi - lo), :]

    def hop(q, depth, where, dx, dy, lo=0, hi=PIECE):
        ref = piece(q, dx, dy, lo, hi)
        send(ref, ref, g_send.at[q], g_recv.at[q, depth], where)

    def mate(q, *offsets, last=0):
        for dx, dy in offsets:
            ref = piece(q, dx, dy)
            send(ref, ref, g_send.at[q], d_recv.at[last, q], MATE)

    def arrived(q, depth):
        rows = (4096, 2 * (BLK + 2 * (PIECE - XP)) + 2 * (BLK + 2 * XP), 4096, PIECE)[depth]
        await_recv(g.at[q, 0, pl.ds(0, rows), :], g_recv.at[q, depth])

    def g1(q):
        for where in (XPOS, XNEG, YPOS, YNEG):
            hop(q, 0, where, 0, 0)
        mate(q, (0, 0))

    def g2(q):
        arrived(q, 0)
        hop(q, 1, XPOS, 3, 0, XM, YP)
        hop(q, 1, YPOS, 0, 3, XM, YP)
        for lo, hi in ((0, XM), (YP, PIECE)):
            hop(q, 1, XNEG, 1, 0, lo, hi)
            hop(q, 1, YNEG, 0, 1, lo, hi)
        for d in (1, 3):
            for where in (XPOS, XNEG):
                hop(q, 1, where, 0, d, XP, PIECE)
            for where in (YPOS, YNEG):
                hop(q, 1, where, d, 0, 0, XP)
        mate(q, (1, 0), (3, 0), (0, 1), (0, 3))

    def g3(q):
        arrived(q, 1)
        for where in (XPOS, XNEG):
            hop(q, 2, where, 0, 2, XP, PIECE)
        for where in (YPOS, YNEG):
            hop(q, 2, where, 2, 0, 0, XP)
        for d in (1, 3):
            hop(q, 2, XPOS, 3, d, XP, YP)
            hop(q, 2, XNEG, 1, d, YP, PIECE)
            hop(q, 2, YPOS, d, 3, XM, XP)
            hop(q, 2, YNEG, d, 1, 0, XM)
        mate(q, (2, 0), (0, 2), (1, 1), (1, 3), (3, 1), (3, 3))

    def g4(q):
        arrived(q, 2)
        hop(q, 3, XPOS, 3, 2, XP, YP)
        hop(q, 3, XNEG, 1, 2, YP, PIECE)
        hop(q, 3, YPOS, 2, 3, XM, XP)
        hop(q, 3, YNEG, 2, 1, 0, XM)
        mate(q, (1, 2), (3, 2), (2, 1), (2, 3))

    def g5(q):
        arrived(q, 3)
        mate(q, (2, 2), last=1)

    def g_most(q):
        await_recv(g.at[q, pl.ds(0, 3), pl.ds(0, 5 * PIECE)], d_recv.at[0, q])

    def g_whole(q):
        await_recv(g.at[q, 0, pl.ds(0, PIECE)], d_recv.at[1, q])

    def g_rows(nq, start, n):
        return jnp.concatenate([g[nq, t, pl.ds(start, n), :] for t in range(Q)], axis=1)

    def c1_part(q, zz):
        lhs = jnp.concatenate(
            [a[0, zz, cc, qr, yy] for cc in range(2) for qr in range(Q) for yy in range(2)], axis=1
        )
        acc1[q] += jnp.dot(lhs, g_rows(q, pl.multiple_of(zz * PLANE, PLANE), PLANE), preferred_element_type=F32)

    def c1_most(q):
        def step(i, carry):
            c1_part(q, plus(x, i + lax.div(i, 2)))
            return carry

        acc1[q] = jnp.zeros((ROWS, BLK), F32)
        lax.fori_loop(0, 3, step, 0)

    def c1_rest(q):
        c1_part(q, plus(x, 2))

    def square_sum(ref, q):
        v = ref[q]
        return jnp.sum(v * v, axis=0, keepdims=True)

    def sum_first(s1, i, k):
        me = x * 2 + c
        for dx in FAR_FIRST:
            for dc in range(2):
                if dx + dc:
                    send(s1.at[i, me], s1.at[i, me], r_send.at[0, k], r_recv1.at[k], dev(dx=dx, dc=dc))

    def sum_second(s1, s2, i, k):
        await_recv(s1.at[i, pl.ds(0, 7)], r_recv1.at[k])
        s2[i, y] = jnp.sum(s1[i], axis=0)
        for dy in FAR_FIRST[:3]:
            send(s2.at[i, y], s2.at[i, y], r_send.at[1, k], r_recv2.at[k], dev(dy=dy))

    def sum_last(s2, i, k):
        await_recv(s2.at[i, pl.ds(0, 3)], r_recv2.at[k])

    me_plane = y * 8 + x * 2 + c

    def to_plane(source, dst, ssem, rsem):
        for dy in FAR_FIRST:
            for dx in FAR_FIRST:
                for dc in range(2):
                    if dx + dy + dc:
                        send(source(dy), dst.at[me_plane], ssem, rsem, dev(dx=dx, dy=dy, dc=dc))

    def c1_sums(q):
        if q in DIRECT:
            k = DIRECT.index(q)
            s4[k, me_plane] = square_sum(acc1, q)
            to_plane(lambda dy: s4.at[k, me_plane], s4.at[k], p_send.at[k], p_recv.at[k])
        else:
            s1a[q, x * 2 + c] = square_sum(acc1, q)
            sum_first(s1a, q, q)

    def c1_second(q):
        if q not in DIRECT:
            sum_second(s1a, s2a, q, q)

    def c1_scale(q):
        if q in DIRECT:
            k = DIRECT.index(q)
            await_recv(s4.at[k, pl.ds(0, 31)], p_recv.at[k])
            return N / jnp.sum(s4[k], axis=0)
        sum_last(s2a, q, q)
        return N / jnp.sum(s2a[q], axis=0)

    def a1_chunk(dz, q, lo=0, n=2):
        return a.at[1, plus(z, dz), pl.ds(lo, n), q]

    def a1_spread(q):
        scale = c1_scale(q)
        for t in range(Q):
            v = acc1[q, :, pl.ds(t * LANE, LANE)]
            a[1, z, t // 2, q, t % 2] = (v * v * scale[:, t * LANE : t * LANE + LANE]).astype(BF)
        for half in range(2):
            for where, n in ((ZPOS, half), (ZNEG, 1 - half)):
                send(a1_chunk(0, q, n, 1), a1_chunk(0, q, n, 1), a1_send, a1_recv.at[half, q], where)

    def a1_relay(q):
        await_recv(a.at[1, 0, :, 0], a1_recv.at[0, q])
        send(a1_chunk(3, q, 0, 1), a1_chunk(3, q, 0, 1), a1_send, a1_recv2.at[q], ZPOS)
        send(a1_chunk(1, q, 1, 1), a1_chunk(1, q, 1, 1), a1_send, a1_recv2.at[q], ZNEG)

    def c2(q, dz, first=False):
        zz = plus(z, dz)
        lhs = jnp.concatenate([a[1, zz, cc, q, yy] for cc in range(2) for yy in range(2)], axis=1)
        base = pl.multiple_of(zz * PLANE, PLANE)
        for nq in range(Q):
            rhs = jnp.concatenate([g_rows(nq, base + cc * PIECE + q * ROWS, ROWS) for cc in range(2)], axis=0)
            prod = jnp.dot(lhs, rhs, preferred_element_type=F32)
            acc2[nq] = prod if first else acc2[nq] + prod

    def c2_near(q):
        await_recv(a.at[1, 0, :, 0], a1_recv.at[1, q])
        for dz in NEAR:
            c2(q, dz)

    def c2_far(q):
        await_recv(a.at[1, 0, :, 0], a1_recv2.at[q])
        c2(q, 2)

    def c2_sums():
        for q in range(Q):
            s1b[0, x * 2 + c, :, pl.ds(q * BLK, BLK)] = square_sum(acc2, q)
        sum_first(s1b, 0, 4)

    def c2_second():
        sum_second(s1b, s2b, 0, 4)

    def early_part(dz, lo=0, n=2):
        return early.at[plus(z, dz), pl.ds(lo, n)]

    def early_spread():
        for half in range(2):
            for where, n in ((ZPOS, half), (ZNEG, 1 - half)):
                src = acc2.at[pl.ds(2 * n, 2), pl.ds(0, EARLY), :]
                send(src, early_part(0, 2 * n), e_send, e_recv.at[half], where)

    def early_relay():
        await_recv(early.at[0], e_recv.at[0])
        send(early_part(3), early_part(3), e_send, e_recv.at[2], ZPOS)
        send(early_part(1, 2), early_part(1, 2), e_send, e_recv.at[2], ZNEG)

    def a2_scales():
        sum_last(s2b, 0, Q)
        scales[z] = N / jnp.sum(s2b[0], axis=0)
        for dz in (2, 1, 3):
            send(scales.at[z], scales.at[z], v_send, v_recv, dev(dz=dz))

    def scaled(v, zz, q, t, rows):
        lanes = pl.ds(q * BLK + t * LANE, LANE)
        a[2, zz, t // 2, q, t % 2, rows, :] = (v * v * scales[zz, :, lanes]).astype(BF)

    def early_scale(dz):
        zz = plus(z, dz)
        for q in range(Q):
            for t in range(Q):
                scaled(early[zz, q, :, pl.ds(t * LANE, LANE)], zz, q, t, pl.ds(0, EARLY))

    def early_near():
        await_recv(early.at[0], e_recv.at[1])
        await_recv(scales.at[pl.ds(0, 3)], v_recv)
        for dz in NEAR:
            early_scale(dz)
        for half in range(2):
            c3_first(Q0, half)

    def early_far():
        await_recv(early.at[0], e_recv.at[2])
        early_scale(2)
        c3_far(Q0)

    def a2_rows(dz, p, lo=0, n=2):
        start, rows = ROWS3[p]
        return a.at[2, plus(z, dz), pl.ds(lo, n), :, :, pl.ds(start, rows), :]

    def a2_scale(p):
        rows = pl.ds(*ROWS3[p])
        for q in range(Q):
            for t in range(Q):
                scaled(acc2[q, rows, pl.ds(t * LANE, LANE)], z, q, t, rows)

    def a2_spread(p):
        for half in range(2):
            for where, n in ((ZPOS, half), (ZNEG, 1 - half)):
                send(a2_rows(0, p, n, 1), a2_rows(0, p, n, 1), a2_send.at[p], a2_recv.at[half, p], where)

    def a2_relay(p):
        start, rows = ROWS3[p]
        await_recv(a.at[2, 0, :, :, :, pl.ds(start, rows), :], a2_recv.at[0, p])
        send(a2_rows(3, p, 0, 1), a2_rows(3, p, 0, 1), a2_send.at[p], a2_recv2.at[p], ZPOS)
        send(a2_rows(1, p, 1, 1), a2_rows(1, p, 1, 1), a2_send.at[p], a2_recv2.at[p], ZNEG)

    def c3_part(zz, start, rows, nq, halves=(0, 1)):
        lhs = jnp.concatenate(
            [a[2, zz, cc, qr, yy, pl.ds(start, rows), :] for cc in halves for qr in range(Q) for yy in range(2)],
            axis=1,
        )
        depth = len(halves) * PIECE
        base = pl.multiple_of(zz * PLANE + halves[0] * PIECE, PIECE)
        return jnp.dot(lhs, g_rows(nq, base, depth), preferred_element_type=F32)

    def c3_own():
        def step(nq, carry):
            acc1[nq] = c3_part(z, 0, ROWS, nq)
            return carry

        lax.fori_loop(0, 4, step, 0)

    def c3_first(p, half=0):
        start, rows = ROWS3[p]

        def step(nq, carry):
            part = c3_part(plus(z, 3), start, rows, nq, (half,))
            acc1[nq, pl.ds(start, rows), :] += part + c3_part(plus(z, 1), start, rows, nq, (1 - half,))
            return carry

        lax.fori_loop(0, Q, step, 0)

    def c3_near(p):
        start, rows = ROWS3[p]
        await_recv(a.at[2, 0, :, :, :, pl.ds(start, rows), :], a2_recv.at[1, p])
        c3_first(p, 1)

    def c3_far(p):
        start, rows = ROWS3[p]
        if p:
            await_recv(a.at[2, 0, :, :, :, pl.ds(start, rows), :], a2_recv2.at[p])
        for nq in range(Q):
            v = acc1[nq, pl.ds(start, rows), :] + c3_part(plus(z, 2), start, rows, nq)
            v = v * v
            part = jnp.sum(v, axis=0, keepdims=True)
            here = pl.ds(nq * LANE, LANE)
            for t in range(Q):
                cut = slice(t * LANE, t * LANE + LANE)
                moved[t, pl.ds(start, rows), here] = v[:, cut]
                if p == 0:
                    s3[t, :, here] = part[:, cut]
                else:
                    s3[t, :, here] += part[:, cut]
        if p == Q3:
            c3_sums()
        for dy in (2, 1, 3):
            send(
                moved.at[plus(y, dy), pl.ds(start, rows), :],
                got.at[y, pl.ds(start, rows), :],
                o_send, o_recv, dev(dy=dy),
            )

    def c3_sums():
        to_plane(lambda dy: s3.at[plus(y, dy)], s4.at[2], p_send.at[2], p_recv.at[2])
        s4[2, me_plane] = s3[y]

    def finish():
        await_recv(s4.at[2, pl.ds(0, 31)], p_recv.at[2])
        scale = N / jnp.sum(s4[2], axis=0)
        out_ref[y] = moved[y] * scale
        await_recv(got.at[pl.ds(0, 3)], o_recv)
        for dy in (1, 2, 3):
            t = plus(y, dy)
            out_ref[t] = got[t] * scale

    g1(Q0)
    cast_init()
    cast_graph(Q1)
    g1(Q1)
    a0_exchange()
    g2(Q0)
    g2(Q1)
    cast_graph(Q2)
    g1(Q2)
    a0_spread(0, (0,))
    a0_wait_near()
    a0_spread(1, NEAR)
    g3(Q0)
    a0_pass()
    g3(Q1)
    a0_relay(1, NEAR)
    g4(Q0)
    a0_relay(0, (0,))
    g2(Q2)
    a0_wait_far()
    a0_spread(2, (2,))
    g4(Q1)
    cast_graph(Q3)
    g1(Q3)
    g_most(Q0)
    g5(Q0)
    a0_relay(2, (2,))
    a0_done()
    g_whole(Q0)
    c1_most(Q0)
    c1_rest(Q0)
    c1_sums(Q0)
    g5(Q1)
    g_most(Q1)
    g3(Q2)
    g_whole(Q1)
    c1_most(Q1)
    c1_second(Q0)
    c1_rest(Q1)
    c1_sums(Q1)
    g2(Q3)
    a1_spread(Q0)
    c1_second(Q1)
    g4(Q2)
    g3(Q3)
    a1_relay(Q0)
    g5(Q2)
    a1_spread(Q1)
    g_whole(Q2)
    g_most(Q2)
    c1_most(Q2)
    c1_rest(Q2)
    c1_sums(Q2)
    g4(Q3)
    c1_second(Q2)
    a1_relay(Q1)
    g_most(Q3)
    c1_most(Q3)
    g5(Q3)
    a1_spread(Q2)
    g_whole(Q3)
    c1_rest(Q3)
    c1_sums(Q3)
    c1_second(Q3)
    a1_relay(Q2)
    c2(Q0, 0, True)
    a1_spread(Q3)
    c2(Q1, 0)
    c2_near(Q0)
    c2_far(Q0)
    c2(Q2, 0)
    c2_near(Q1)
    a1_relay(Q3)
    c2_far(Q1)
    c2_near(Q2)
    c2_near(Q3)
    c2(Q3, 0)
    c2_far(Q2)
    c2_far(Q3)
    early_spread()
    c2_sums()
    c2_second()
    early_relay()
    a2_scales()
    a2_scale(Q1)
    a2_spread(Q1)
    for p in (Q0, Q2, Q3):
        a2_scale(p)
    c3_own()
    early_near()
    a2_relay(Q1)
    a2_spread(Q2)
    early_far()
    c3_first(Q1)
    c3_near(Q1)
    c3_far(Q1)
    a2_relay(Q2)
    a2_spread(Q3)
    c3_first(Q2)
    c3_near(Q2)
    c3_far(Q2)
    a2_relay(Q3)
    c3_first(Q3)
    c3_near(Q3)
    c3_far(Q3)
    finish()

    for q in range(Q):
        await_send(g.at[q, :, pl.ds(0, 7936), :], g_send.at[q])
    await_send(stage, t_send)
    await_send(a.at[0, pl.ds(0, 3)], az_send)
    await_send(a.at[1, pl.ds(0, 3)], a1_send)
    await_send(early.at[pl.ds(0, 3)], e_send)
    await_send(scales.at[pl.ds(0, 3)], v_send)
    for p, (start, rows) in enumerate(ROWS3[1:], 1):
        await_send(a.at[2, pl.ds(0, 3), :, :, :, pl.ds(start, rows), :], a2_send.at[p])
    for s1, s2, base, n in ((s1a, s2a, 0, Q2), (s1b, s2b, Q, 1)):
        for i in range(n):
            await_send(s1.at[i, pl.ds(0, 7)], r_send.at[0, base + i])
            await_send(s2.at[i, pl.ds(0, 3)], r_send.at[1, base + i])
    await_send(got.at[pl.ds(0, 3)], o_send)
    for k in range(3):
        await_send(s4.at[k, pl.ds(0, 31)], p_send.at[k])


def solution(mesh):
    block_spec = P(("graph", "row"), "col")
    hbm = pl.BlockSpec(memory_space=pl.ANY)
    dma = pltpu.SemaphoreType.DMA

    def device_step(init_blk, graph_blk):
        result = pl.pallas_call(
            mcl_kernel,
            out_shape=pltpu.VMEM((Q, ROWS, BLK), F32),
            in_specs=[hbm, hbm],
            out_specs=pl.BlockSpec(memory_space=pltpu.VMEM),
            scratch_shapes=[
                pltpu.VMEM((Q, ROWS, BLK), F32), pltpu.VMEM((Q, ROWS, BLK), F32),
                pltpu.VMEM((4, 4, N, LANE), BF),
                pltpu.VMEM((3, 4, 2, 4, 2, ROWS, LANE), BF),
                pltpu.VMEM((4, 4, ROWS, LANE), BF),
                pltpu.VMEM((2, 2, ROWS, LANE), BF),
                pltpu.VMEM((4, ROWS, BLK), F32),
                pltpu.VMEM((4, ROWS, BLK), F32),
                pltpu.VMEM((4, 8, 1, BLK), F32),
                pltpu.VMEM((4, 4, 1, BLK), F32),
                pltpu.VMEM((1, 8, 1, PLANE), F32),
                pltpu.VMEM((1, 4, 1, PLANE), F32),
                pltpu.VMEM((Q, 1, BLK), F32), pltpu.VMEM((3, 32, 1, BLK), F32),
                pltpu.VMEM((Q, Q, EARLY, BLK), F32), pltpu.VMEM((Q, 1, PLANE), F32),
                dma((Q,)), dma((Q, Q)), dma((2, Q)),
                dma(()), dma((3,)), dma(()),
                dma(()), dma((3,)), dma(()),
                dma(()), dma((2, Q)), dma((Q,)),
                dma((Q,)), dma((2, Q)), dma((Q,)),
                dma((2, 5)), dma((5,)), dma((5,)),
                dma(()), dma((3,)), dma(()), dma(()),
                dma(()), dma(()),
                dma((3,)), dma((3,)), dma((Q + 1, Q)),
            ],
            compiler_params=pltpu.CompilerParams(
                collective_id=0, has_side_effects=True, vmem_limit_bytes=VMEM_BYTES
            ),
        )(init_blk, graph_blk)
        return result.reshape(init_blk.shape)

    return jax.shard_map(device_step, mesh=mesh, in_specs=(block_spec, block_spec), out_specs=block_spec, check_vma=False)
```

```python
import functools

import jax
import jax.numpy as jnp
from jax import lax
from jax.experimental import pallas as pl
from jax.experimental.pallas import tpu as pltpu
from jax.sharding import PartitionSpec as P

MESH = pl.DeviceIdType.MESH
VMEM_BYTES = 58 << 20
BF = jnp.bfloat16
F32 = jnp.float32
N = 8192
PLANE, PIECE, BLK, ROWS, LANE = 2048, 1024, 512, 256, 128
Q = 4
Q0, Q1, Q2, Q3 = range(Q)
NEAR = (1, 3)
FAR_FIRST = (2, 1, 3, 0)
XM, XP, YP, HALF = 112, 224, 368, 512
LOW, HIGH = 0, 1
EARLY = 32
ROWS3 = ((0, EARLY), (32, 80), (112, 96), (208, 48))


def mcl_kernel(
    init_hbm, graph_hbm, out_ref,
    moved, got,
    g, a, stage, hold, acc1, acc2, s1b, s2b, s3, s4, early, scales,
    g_send, g_recv, d_recv, t_send, t_recv, h_recv, az_send, az_recv, az2_recv,
    a1_send, a1_recv, a1_recv2, a2_send, a2_recv, a2_recv2,
    r_send, r_recv, e_send, e_recv, v_send, v_recv, o_send, o_recv, p_send, p_recv, i_sem,
):
    col, row = lax.axis_index("col"), lax.axis_index("row")
    z, y = lax.div(col, 4), lax.rem(col, 4)
    x, c = lax.div(row, 2), lax.rem(row, 2)

    def plus(v, d):
        return lax.rem(v + d, 4)

    def dev(dx=0, dy=0, dz=0, dc=0):
        return {"col": plus(z, dz) * 4 + plus(y, dy), "row": plus(x, dx) * 2 + lax.rem(c + dc, 2)}

    XPOS, XNEG, YPOS, YNEG = dev(dx=1), dev(dx=3), dev(dy=1), dev(dy=3)
    ZPOS, ZNEG, MATE = dev(dz=1), dev(dz=3), dev(dc=1)

    def send(src, dst, ssem, rsem, device):
        pltpu.make_async_remote_copy(
            src_ref=src, dst_ref=dst, send_sem=ssem, recv_sem=rsem, device_id=device, device_id_type=MESH
        ).start()

    def await_recv(ref, sem):
        pltpu.make_async_remote_copy(
            src_ref=ref, dst_ref=ref, send_sem=sem, recv_sem=sem, device_id=MATE, device_id_type=MESH
        ).wait_recv()

    def await_send(ref, sem):
        pltpu.make_async_remote_copy(
            src_ref=ref, dst_ref=ref, send_sem=sem, recv_sem=sem, device_id=MATE, device_id_type=MESH
        ).wait_send()

    barrier = pltpu.get_barrier_semaphore()
    peers = [XPOS, XNEG, YPOS, YNEG, ZPOS, ZNEG, MATE]
    for peer in peers:
        pl.semaphore_signal(barrier, inc=1, device_id=peer, device_id_type=MESH)

    init_ref, graph_ref = moved, got
    copies = []
    for q in range(Q + 1):
        lanes = pl.ds(q * LANE, LANE)
        parts = []
        for t in range(Q):
            rows = pl.ds(t * ROWS, ROWS)
            if q == Q:
                parts.append(pltpu.make_async_copy(init_hbm.at[rows], init_ref.at[t], i_sem.at[q, t]))
            else:
                parts.append(
                    pltpu.make_async_copy(graph_hbm.at[rows, lanes], graph_ref.at[t, :, lanes], i_sem.at[q, t])
                )
        copies.append(parts)
    for q in (Q2, Q, Q0, Q1, Q3):
        for copy in copies[q]:
            copy.start()

    def cast_graph(q):
        for copy in copies[q]:
            copy.wait()
        base = pl.multiple_of((x * 2 + c) * PIECE, PIECE)
        lanes = pl.ds(q * LANE, LANE)
        for qr in range(Q):
            for yy in range(2):
                block = graph_ref[yy * 2 + qr // 2, pl.ds(qr % 2 * LANE, LANE), lanes]
                g[q, y, pl.ds(base + qr * ROWS + yy * LANE, LANE), :] = block.astype(BF)

    def cast_init():
        for copy in copies[Q]:
            copy.wait()
        for q in range(Q):
            a[0, z, lax.div(y, 2), q, lax.rem(y, 2)] = init_ref[y, :, pl.ds(q * LANE, LANE)].astype(BF)
        for t in range(Q):
            for q in range(Q):
                stage[t, q] = init_ref[t, :, pl.ds(q * LANE, LANE)].astype(BF)

    cast_graph(Q2)
    pl.semaphore_wait(barrier, len(peers))

    def a0_block(dz, dy, lo=0, n=4):
        yy = plus(y, dy)
        return a.at[0, plus(z, dz), lax.div(yy, 2), pl.ds(lo, n), lax.rem(yy, 2)]

    def a0_spread(group, dys):
        for dy in dys:
            for where in (ZPOS, ZNEG):
                send(a0_block(0, dy), a0_block(0, dy), az_send, az_recv.at[group], where)

    def a0_wait_near():
        for k in range(2):
            await_recv(stage.at[0], t_recv.at[k])

    def a0_wait_far():
        await_recv(stage.at[0], t_recv.at[2])

    def a0_done():
        await_recv(a.at[0, 0], az2_recv)

    def a0_relay(group, dys):
        await_recv(a.at[0, 0, pl.ds(0, len(dys))], az_recv.at[group])
        for dy in dys:
            send(a0_block(3, dy, 0, 2), a0_block(3, dy, 0, 2), az_send, az2_recv, ZPOS)
            send(a0_block(1, dy, 2, 2), a0_block(1, dy, 2, 2), az_send, az2_recv, ZNEG)

    def a0_exchange():
        far = plus(y, 2)
        for side, where in enumerate((YPOS, YNEG)):
            send(stage.at[far, pl.ds(2 * side, 2)], hold.at[side], t_send, h_recv, where)
            send(stage.at[plus(y, NEAR[side])], a0_block(0, 0), t_send, t_recv.at[side], where)

    def a0_pass():
        await_recv(hold, h_recv)
        for side, where in enumerate((YPOS, YNEG)):
            ref = a0_block(0, NEAR[1 - side], 2 * side, 2)
            send(hold.at[side], ref, t_send, t_recv.at[2], where)

    def piece(q, h, dx, dy, lo=0, hi=HALF):
        base = (plus(x, dx) * 2 + c) * PIECE + h * HALF
        return g.at[q, plus(y, dy), pl.ds(pl.multiple_of(base + lo, 16), hi - lo), :]

    def hop(q, h, depth, where, dx, dy, lo=0, hi=HALF):
        ref = piece(q, h, dx, dy, lo, hi)
        send(ref, ref, g_send.at[q], g_recv.at[q, h, depth], where)

    def mate(q, h, offsets, last=0):
        for dx, dy in offsets:
            ref = piece(q, h, dx, dy)
            send(ref, ref, g_send.at[q], d_recv.at[last, q], MATE)

    def arrived(q, h, depth):
        rows = (Q * HALF, 3 * PIECE, Q * HALF, HALF)[depth]
        await_recv(g.at[q, 0, pl.ds(0, rows), :], g_recv.at[q, h, depth])

    def g1(q, h):
        for where in (XPOS, XNEG, YPOS, YNEG):
            hop(q, h, 0, where, 0, 0)
        mate(q, h, ((0, 0),))

    def g2(q, h):
        arrived(q, h, 0)
        hop(q, h, 1, XPOS, 3, 0, XM, YP)
        hop(q, h, 1, YPOS, 0, 3, XM, YP)
        for lo, hi in ((0, XM), (YP, HALF)):
            hop(q, h, 1, XNEG, 1, 0, lo, hi)
            hop(q, h, 1, YNEG, 0, 1, lo, hi)
        for d in NEAR:
            for where in (XPOS, XNEG):
                hop(q, h, 1, where, 0, d, XP)
            for where in (YPOS, YNEG):
                hop(q, h, 1, where, d, 0, 0, XP)
        mate(q, h, ((1, 0), (3, 0), (0, 1), (0, 3)))

    def g3(q, h):
        arrived(q, h, 1)
        for where in (XPOS, XNEG):
            hop(q, h, 2, where, 0, 2, XP)
        for where in (YPOS, YNEG):
            hop(q, h, 2, where, 2, 0, 0, XP)
        for d in NEAR:
            hop(q, h, 2, XPOS, 3, d, XP, YP)
            hop(q, h, 2, XNEG, 1, d, YP)
            hop(q, h, 2, YPOS, d, 3, XM, XP)
            hop(q, h, 2, YNEG, d, 1, 0, XM)
        mate(q, h, ((2, 0), (0, 2)) + tuple((i, j) for i in NEAR for j in NEAR))

    def g4(q, h):
        arrived(q, h, 2)
        hop(q, h, 3, XPOS, 3, 2, XP, YP)
        hop(q, h, 3, XNEG, 1, 2, YP)
        hop(q, h, 3, YPOS, 2, 3, XM, XP)
        hop(q, h, 3, YNEG, 2, 1, 0, XM)
        mate(q, h, ((1, 2), (3, 2), (2, 1), (2, 3)))

    def g5(q, h):
        arrived(q, h, 3)
        mate(q, h, ((2, 2),), last=1)

    def g_most(q):
        await_recv(g.at[q, pl.ds(0, 3), pl.ds(0, 5 * PIECE)], d_recv.at[0, q])

    def g_whole(q):
        await_recv(g.at[q, 0, pl.ds(0, PIECE)], d_recv.at[1, q])

    def g_rows(nq, start, n):
        return jnp.concatenate([g[nq, t, pl.ds(start, n), :] for t in range(Q)], axis=1)

    def c1_part(q, zz, cc):
        lhs = jnp.concatenate([a[0, zz, cc, qr, yy] for qr in range(Q) for yy in range(2)], axis=1)
        base = pl.multiple_of(zz * PLANE + cc * PIECE, PIECE)
        acc1[q] += jnp.dot(lhs, g_rows(q, base, PIECE), preferred_element_type=F32)

    def c1_near(q, cc):
        def step(i, carry):
            c1_part(q, plus(x, i + lax.div(i, 2)), cc)
            return carry

        lax.fori_loop(0, 3, step, 0)

    def c1_own(q):
        acc1[q] = jnp.zeros((ROWS, BLK), F32)
        c1_near(q, c)

    def c1_mate(q):
        c1_near(q, 1 - c)

    def c1_far(q):
        c1_part(q, plus(x, 2), c)

    def c1_rest(q):
        c1_part(q, plus(x, 2), 1 - c)

    def square_sum(ref, q):
        v = ref[q]
        return jnp.sum(v * v, axis=0, keepdims=True)

    def c2_sums():
        me = x * 2 + c
        for q in range(Q):
            s1b[me, :, pl.ds(q * BLK, BLK)] = square_sum(acc2, q)
        for dx in FAR_FIRST:
            for dc in range(2):
                if dx + dc:
                    send(s1b.at[me], s1b.at[me], r_send.at[0], r_recv.at[0], dev(dx=dx, dc=dc))

    def c2_second():
        await_recv(s1b.at[pl.ds(0, 7)], r_recv.at[0])
        s2b[y] = jnp.sum(s1b[...], axis=0)
        for dy in FAR_FIRST[:3]:
            send(s2b.at[y], s2b.at[y], r_send.at[1], r_recv.at[1], dev(dy=dy))

    me_plane = y * 8 + x * 2 + c

    def to_plane(source, dst, ssem, rsem):
        for dy in FAR_FIRST:
            for dx in FAR_FIRST:
                for dc in range(2):
                    if dx + dy + dc:
                        send(source(dy), dst.at[me_plane], ssem, rsem, dev(dx=dx, dy=dy, dc=dc))

    def c1_sums(q):
        s4[q, me_plane] = square_sum(acc1, q)
        to_plane(lambda dy: s4.at[q, me_plane], s4.at[q], p_send.at[q], p_recv.at[q])

    def c1_scale(q):
        await_recv(s4.at[q, pl.ds(0, 31)], p_recv.at[q])
        return N / jnp.sum(s4[q], axis=0)

    def a1_chunk(dz, q, lo=0, n=2):
        return a.at[1, plus(z, dz), pl.ds(lo, n), q]

    def a1_spread(q):
        scale = c1_scale(q)
        for t in range(Q):
            v = acc1[q, :, pl.ds(t * LANE, LANE)]
            a[1, z, t // 2, q, t % 2] = (v * v * scale[:, t * LANE : t * LANE + LANE]).astype(BF)
        for half in range(2):
            for where, n in ((ZPOS, half), (ZNEG, 1 - half)):
                send(a1_chunk(0, q, n, 1), a1_chunk(0, q, n, 1), a1_send, a1_recv.at[half, q], where)

    def a1_relay(q):
        await_recv(a.at[1, 0, :, 0], a1_recv.at[0, q])
        send(a1_chunk(3, q, 0, 1), a1_chunk(3, q, 0, 1), a1_send, a1_recv2.at[q], ZPOS)
        send(a1_chunk(1, q, 1, 1), a1_chunk(1, q, 1, 1), a1_send, a1_recv2.at[q], ZNEG)

    def c2(q, dz, first=False):
        zz = plus(z, dz)
        lhs = jnp.concatenate([a[1, zz, cc, q, yy] for cc in range(2) for yy in range(2)], axis=1)
        base = pl.multiple_of(zz * PLANE, PLANE)
        for nq in range(Q):
            rhs = jnp.concatenate([g_rows(nq, base + cc * PIECE + q * ROWS, ROWS) for cc in range(2)], axis=0)
            prod = jnp.dot(lhs, rhs, preferred_element_type=F32)
            acc2[nq] = prod if first else acc2[nq] + prod

    def c2_near(q):
        await_recv(a.at[1, 0, :, 0], a1_recv.at[1, q])
        for dz in NEAR:
            c2(q, dz)

    def c2_far(q):
        await_recv(a.at[1, 0, :, 0], a1_recv2.at[q])
        c2(q, 2)

    def early_part(dz, lo=0, n=2):
        return early.at[plus(z, dz), pl.ds(lo, n)]

    def early_spread():
        for half in range(2):
            for where, n in ((ZPOS, half), (ZNEG, 1 - half)):
                src = acc2.at[pl.ds(2 * n, 2), pl.ds(0, EARLY), :]
                send(src, early_part(0, 2 * n), e_send, e_recv.at[half], where)

    def early_relay():
        await_recv(early.at[0], e_recv.at[0])
        send(early_part(3), early_part(3), e_send, e_recv.at[2], ZPOS)
        send(early_part(1, 2), early_part(1, 2), e_send, e_recv.at[2], ZNEG)

    def a2_scales():
        await_recv(s2b.at[pl.ds(0, 3)], r_recv.at[1])
        scales[z] = N / jnp.sum(s2b[...], axis=0)
        for dz in (2, 1, 3):
            send(scales.at[z], scales.at[z], v_send, v_recv, dev(dz=dz))

    def scaled(v, zz, q, t, rows):
        lanes = pl.ds(q * BLK + t * LANE, LANE)
        a[2, zz, t // 2, q, t % 2, rows, :] = (v * v * scales[zz, :, lanes]).astype(BF)

    def early_scale(dz):
        zz = plus(z, dz)
        for q in range(Q):
            for t in range(Q):
                scaled(early[zz, q, :, pl.ds(t * LANE, LANE)], zz, q, t, pl.ds(0, EARLY))

    def early_near():
        await_recv(early.at[0], e_recv.at[1])
        await_recv(scales.at[pl.ds(0, 3)], v_recv)
        for dz in NEAR:
            early_scale(dz)
        for half in range(2):
            c3_first(Q0, half)

    def early_far():
        await_recv(early.at[0], e_recv.at[2])
        early_scale(2)
        c3_far(Q0)

    def a2_rows(dz, p, lo=0, n=2):
        start, rows = ROWS3[p]
        return a.at[2, plus(z, dz), pl.ds(lo, n), :, :, pl.ds(start, rows), :]

    def a2_scale(p):
        rows = pl.ds(*ROWS3[p])
        for q in range(Q):
            for t in range(Q):
                scaled(acc2[q, rows, pl.ds(t * LANE, LANE)], z, q, t, rows)

    def a2_spread(p):
        for half in range(2):
            for where, n in ((ZPOS, half), (ZNEG, 1 - half)):
                send(a2_rows(0, p, n, 1), a2_rows(0, p, n, 1), a2_send.at[p], a2_recv.at[half, p], where)

    def a2_relay(p):
        start, rows = ROWS3[p]
        await_recv(a.at[2, 0, :, :, :, pl.ds(start, rows), :], a2_recv.at[0, p])
        send(a2_rows(3, p, 0, 1), a2_rows(3, p, 0, 1), a2_send.at[p], a2_recv2.at[p], ZPOS)
        send(a2_rows(1, p, 1, 1), a2_rows(1, p, 1, 1), a2_send.at[p], a2_recv2.at[p], ZNEG)

    def c3_part(zz, start, rows, nq, halves=(0, 1)):
        lhs = jnp.concatenate(
            [a[2, zz, cc, qr, yy, pl.ds(start, rows), :] for cc in halves for qr in range(Q) for yy in range(2)],
            axis=1,
        )
        depth = len(halves) * PIECE
        base = pl.multiple_of(zz * PLANE + halves[0] * PIECE, PIECE)
        return jnp.dot(lhs, g_rows(nq, base, depth), preferred_element_type=F32)

    def c3_own():
        def step(nq, carry):
            acc1[nq] = c3_part(z, 0, ROWS, nq)
            return carry

        lax.fori_loop(0, 4, step, 0)

    def c3_first(p, half=0):
        start, rows = ROWS3[p]

        def step(nq, carry):
            part = c3_part(plus(z, 3), start, rows, nq, (half,))
            acc1[nq, pl.ds(start, rows), :] += part + c3_part(plus(z, 1), start, rows, nq, (1 - half,))
            return carry

        lax.fori_loop(0, Q, step, 0)

    def c3_near(p):
        start, rows = ROWS3[p]
        await_recv(a.at[2, 0, :, :, :, pl.ds(start, rows), :], a2_recv.at[1, p])
        c3_first(p, 1)

    def c3_far(p):
        start, rows = ROWS3[p]
        if p:
            await_recv(a.at[2, 0, :, :, :, pl.ds(start, rows), :], a2_recv2.at[p])
        for nq in range(Q):
            v = acc1[nq, pl.ds(start, rows), :] + c3_part(plus(z, 2), start, rows, nq)
            v = v * v
            part = jnp.sum(v, axis=0, keepdims=True)
            here = pl.ds(nq * LANE, LANE)
            for t in range(Q):
                cut = slice(t * LANE, t * LANE + LANE)
                moved[t, pl.ds(start, rows), here] = v[:, cut]
                if p == 0:
                    s3[t, :, here] = part[:, cut]
                else:
                    s3[t, :, here] += part[:, cut]
        if p == Q3:
            c3_sums()
        for dy in (2, 1, 3):
            send(
                moved.at[plus(y, dy), pl.ds(start, rows), :],
                got.at[y, pl.ds(start, rows), :],
                o_send, o_recv, dev(dy=dy),
            )

    def c3_sums():
        to_plane(lambda dy: s3.at[plus(y, dy)], s4.at[Q], p_send.at[Q], p_recv.at[Q])
        s4[Q, me_plane] = s3[y]

    def finish():
        await_recv(s4.at[Q, pl.ds(0, 31)], p_recv.at[Q])
        scale = N / jnp.sum(s4[Q], axis=0)
        out_ref[y] = moved[y] * scale
        await_recv(got.at[pl.ds(0, 3)], o_recv)
        for dy in (1, 2, 3):
            t = plus(y, dy)
            out_ref[t] = got[t] * scale

    g1(Q2, LOW)
    cast_graph(Q1)
    g1(Q1, HIGH)
    cast_graph(Q0)
    g1(Q0, HIGH)
    cast_init()
    a0_exchange()
    g1(Q0, LOW)
    g2(Q0, HIGH)
    g1(Q1, LOW)
    g2(Q1, HIGH)
    a0_spread(0, (0,))
    g1(Q2, HIGH)
    g2(Q0, LOW)
    a0_wait_near()
    a0_spread(1, NEAR)
    g2(Q1, LOW)
    a0_relay(0, (0,))
    g3(Q1, HIGH)
    a0_pass()
    g3(Q0, HIGH)
    g3(Q0, LOW)
    g3(Q1, LOW)
    g2(Q2, HIGH)
    a0_relay(1, NEAR)
    a0_wait_far()
    a0_spread(2, (2,))
    g4(Q0, HIGH)
    g4(Q1, HIGH)
    g4(Q0, LOW)
    g2(Q2, LOW)
    g4(Q1, LOW)
    g_most(Q1)
    cast_graph(Q3)
    g1(Q3, LOW)
    a0_relay(2, (2,))
    a0_done()
    g3(Q2, HIGH)
    c1_own(Q0)
    g5(Q0, LOW)
    g3(Q2, LOW)
    g_most(Q0)
    g5(Q1, LOW)
    c1_mate(Q0)
    g5(Q0, HIGH)
    c1_far(Q0)
    g_whole(Q0)
    c1_rest(Q0)
    c1_sums(Q0)
    g1(Q3, HIGH)
    g5(Q1, HIGH)
    g4(Q2, HIGH)
    g2(Q3, LOW)
    c1_own(Q1)
    c1_mate(Q1)
    a1_spread(Q0)
    g_whole(Q1)
    c1_far(Q1)
    g5(Q2, HIGH)
    c1_rest(Q1)
    c1_sums(Q1)
    g4(Q2, LOW)
    g2(Q3, HIGH)
    c1_own(Q2)
    g_most(Q2)
    g5(Q2, LOW)
    c1_mate(Q2)
    c1_far(Q2)
    a1_relay(Q0)
    g_whole(Q2)
    c1_rest(Q2)
    c1_sums(Q2)
    g3(Q3, LOW)
    g3(Q3, HIGH)
    a1_spread(Q1)
    g4(Q3, LOW)
    a1_spread(Q2)
    a1_relay(Q1)
    g4(Q3, HIGH)
    c1_own(Q3)
    g_most(Q3)
    g5(Q3, LOW)
    g5(Q3, HIGH)
    c1_far(Q3)
    c1_mate(Q3)
    g_whole(Q3)
    a1_relay(Q2)
    c1_rest(Q3)
    c1_sums(Q3)
    c2(Q0, 0, True)
    c2_near(Q1)
    c2_near(Q0)
    c2(Q2, 0)
    a1_spread(Q3)
    a1_relay(Q3)
    c2(Q3, 0)
    c2_near(Q2)
    c2(Q1, 0)
    c2_far(Q1)
    c2_far(Q2)
    c2_far(Q0)
    c2_near(Q3)
    c2_far(Q3)
    early_spread()
    c2_sums()
    c2_second()
    early_relay()
    a2_scales()
    a2_scale(Q1)
    a2_spread(Q1)
    for p in (Q0, Q2, Q3):
        a2_scale(p)
    c3_own()
    early_near()
    a2_relay(Q1)
    a2_spread(Q2)
    early_far()
    c3_first(Q1)
    c3_near(Q1)
    c3_far(Q1)
    a2_relay(Q2)
    a2_spread(Q3)
    c3_first(Q2)
    c3_near(Q2)
    c3_far(Q2)
    a2_relay(Q3)
    c3_first(Q3)
    c3_near(Q3)
    c3_far(Q3)
    finish()

    for q in range(Q):
        await_send(g.at[q, :, pl.ds(0, 7936), :], g_send.at[q])
    await_send(stage, t_send)
    await_send(a.at[0, pl.ds(0, 3)], az_send)
    await_send(a.at[1, pl.ds(0, 3)], a1_send)
    await_send(early.at[pl.ds(0, 3)], e_send)
    await_send(scales.at[pl.ds(0, 3)], v_send)
    for p, (start, rows) in enumerate(ROWS3[1:], 1):
        await_send(a.at[2, pl.ds(0, 3), :, :, :, pl.ds(start, rows), :], a2_send.at[p])
    await_send(s1b.at[pl.ds(0, 7)], r_send.at[0])
    await_send(s2b.at[pl.ds(0, 3)], r_send.at[1])
    await_send(got.at[pl.ds(0, 3)], o_send)
    for k in range(Q + 1):
        await_send(s4.at[k, pl.ds(0, 31)], p_send.at[k])


def solution(mesh):
    block_spec = P(("graph", "row"), "col")
    hbm = pl.BlockSpec(memory_space=pl.ANY)
    dma = pltpu.SemaphoreType.DMA

    def device_step(init_blk, graph_blk):
        result = pl.pallas_call(
            mcl_kernel,
            out_shape=pltpu.VMEM((Q, ROWS, BLK), F32),
            in_specs=[hbm, hbm],
            out_specs=pl.BlockSpec(memory_space=pltpu.VMEM),
            scratch_shapes=[
                pltpu.VMEM((Q, ROWS, BLK), F32), pltpu.VMEM((Q, ROWS, BLK), F32),
                pltpu.VMEM((4, 4, N, LANE), BF),
                pltpu.VMEM((3, 4, 2, 4, 2, ROWS, LANE), BF),
                pltpu.VMEM((4, 4, ROWS, LANE), BF),
                pltpu.VMEM((2, 2, ROWS, LANE), BF),
                pltpu.VMEM((4, ROWS, BLK), F32),
                pltpu.VMEM((4, ROWS, BLK), F32),
                pltpu.VMEM((8, 1, PLANE), F32),
                pltpu.VMEM((4, 1, PLANE), F32),
                pltpu.VMEM((Q, 1, BLK), F32), pltpu.VMEM((Q + 1, 32, 1, BLK), F32),
                pltpu.VMEM((Q, Q, EARLY, BLK), F32), pltpu.VMEM((Q, 1, PLANE), F32),
                dma((Q,)), dma((Q, 2, Q)), dma((2, Q)),
                dma(()), dma((3,)), dma(()),
                dma(()), dma((3,)), dma(()),
                dma(()), dma((2, Q)), dma((Q,)),
                dma((Q,)), dma((2, Q)), dma((Q,)),
                dma((2,)), dma((2,)),
                dma(()), dma((3,)), dma(()), dma(()),
                dma(()), dma(()),
                dma((Q + 1,)), dma((Q + 1,)), dma((Q + 1, Q)),
            ],
            compiler_params=pltpu.CompilerParams(
                collective_id=0, has_side_effects=True, vmem_limit_bytes=VMEM_BYTES
            ),
        )(init_blk, graph_blk)
        return result.reshape(init_blk.shape)

    return jax.shard_map(device_step, mesh=mesh, in_specs=(block_spec, block_spec), out_specs=block_spec, check_vma=False)
```

```python
import functools

import jax
import jax.numpy as jnp
from jax import lax
from jax.experimental import pallas as pl
from jax.experimental.pallas import tpu as pltpu
from jax.sharding import PartitionSpec as P

MESH = pl.DeviceIdType.MESH
VMEM_BYTES = 58 << 20
BF = jnp.bfloat16
F32 = jnp.float32
N = 8192
PLANE, PIECE, BLK, ROWS, LANE = 2048, 1024, 512, 256, 128
Q = 4
Q0, Q1, Q2, Q3 = range(Q)
NEAR = (1, 3)
FAR_FIRST = (2, 1, 3, 0)
DIRECT = (Q2, Q3)
XM, XP, YP = 224, 448, 736
EARLY = 32
ROWS3 = ((0, EARLY), (32, 96), (128, 80), (208, 48))


def mcl_kernel(
    init_hbm, graph_hbm, out_ref,
    moved, got,
    g, a, stage, hold, acc1, acc2, s1a, s2a, s1b, s2b, s3, s4, early, scales,
    g_send, g_recv, d_recv, t_send, t_recv, h_recv, az_send, az_recv, az2_recv,
    a1_send, a1_recv, a1_recv2, a2_send, a2_recv, a2_recv2,
    r_send, r_recv1, r_recv2, e_send, e_recv, v_send, v_recv, o_send, o_recv, p_send, p_recv, i_sem,
):
    col, row = lax.axis_index("col"), lax.axis_index("row")
    z, y = lax.div(col, 4), lax.rem(col, 4)
    x, c = lax.div(row, 2), lax.rem(row, 2)

    def plus(v, d):
        return lax.rem(v + d, 4)

    def dev(dx=0, dy=0, dz=0, dc=0):
        return {"col": plus(z, dz) * 4 + plus(y, dy), "row": plus(x, dx) * 2 + lax.rem(c + dc, 2)}

    XPOS, XNEG, YPOS, YNEG = dev(dx=1), dev(dx=3), dev(dy=1), dev(dy=3)
    ZPOS, ZNEG, MATE = dev(dz=1), dev(dz=3), dev(dc=1)

    def send(src, dst, ssem, rsem, device):
        pltpu.make_async_remote_copy(
            src_ref=src, dst_ref=dst, send_sem=ssem, recv_sem=rsem, device_id=device, device_id_type=MESH
        ).start()

    def await_recv(ref, sem):
        pltpu.make_async_remote_copy(
            src_ref=ref, dst_ref=ref, send_sem=sem, recv_sem=sem, device_id=MATE, device_id_type=MESH
        ).wait_recv()

    def await_send(ref, sem):
        pltpu.make_async_remote_copy(
            src_ref=ref, dst_ref=ref, send_sem=sem, recv_sem=sem, device_id=MATE, device_id_type=MESH
        ).wait_send()

    barrier = pltpu.get_barrier_semaphore()
    peers = [XPOS, XNEG, YPOS, YNEG, ZPOS, ZNEG, MATE]
    for peer in peers:
        pl.semaphore_signal(barrier, inc=1, device_id=peer, device_id_type=MESH)

    init_ref, graph_ref = moved, got
    copies = []
    for q in range(Q + 1):
        lanes = pl.ds(q * LANE, LANE)
        parts = []
        for t in range(Q):
            rows = pl.ds(t * ROWS, ROWS)
            if q == Q:
                parts.append(pltpu.make_async_copy(init_hbm.at[rows], init_ref.at[t], i_sem.at[q, t]))
            else:
                parts.append(
                    pltpu.make_async_copy(graph_hbm.at[rows, lanes], graph_ref.at[t, :, lanes], i_sem.at[q, t])
                )
        copies.append(parts)
    for q in (Q0, Q, Q1, Q2, Q3):
        for copy in copies[q]:
            copy.start()

    def cast_graph(q):
        for copy in copies[q]:
            copy.wait()
        base = pl.multiple_of((x * 2 + c) * PIECE, PIECE)
        lanes = pl.ds(q * LANE, LANE)
        for qr in range(Q):
            for yy in range(2):
                block = graph_ref[yy * 2 + qr // 2, pl.ds(qr % 2 * LANE, LANE), lanes]
                g[q, y, pl.ds(base + qr * ROWS + yy * LANE, LANE), :] = block.astype(BF)

    def cast_init():
        for copy in copies[Q]:
            copy.wait()
        for q in range(Q):
            a[0, z, lax.div(y, 2), q, lax.rem(y, 2)] = init_ref[y, :, pl.ds(q * LANE, LANE)].astype(BF)
        for t in range(Q):
            for q in range(Q):
                stage[t, q] = init_ref[t, :, pl.ds(q * LANE, LANE)].astype(BF)

    cast_graph(Q0)
    pl.semaphore_wait(barrier, len(peers))

    def a0_block(dz, dy, lo=0, n=4):
        yy = plus(y, dy)
        return a.at[0, plus(z, dz), lax.div(yy, 2), pl.ds(lo, n), lax.rem(yy, 2)]

    def a0_spread(group, dys):
        for dy in dys:
            for where in (ZPOS, ZNEG):
                send(a0_block(0, dy), a0_block(0, dy), az_send, az_recv.at[group], where)

    def a0_wait_near():
        for k in range(2):
            await_recv(stage.at[0], t_recv.at[k])

    def a0_wait_far():
        await_recv(stage.at[0], t_recv.at[2])

    def a0_done():
        await_recv(a.at[0, 0], az2_recv)

    def a0_relay(group, dys):
        await_recv(a.at[0, 0, pl.ds(0, len(dys))], az_recv.at[group])
        for dy in dys:
            send(a0_block(3, dy, 0, 2), a0_block(3, dy, 0, 2), az_send, az2_recv, ZPOS)
            send(a0_block(1, dy, 2, 2), a0_block(1, dy, 2, 2), az_send, az2_recv, ZNEG)

    def a0_exchange():
        far = plus(y, 2)
        for side, where in enumerate((YPOS, YNEG)):
            send(stage.at[far, pl.ds(2 * side, 2)], hold.at[side], t_send, h_recv, where)
            send(stage.at[plus(y, NEAR[side])], a0_block(0, 0), t_send, t_recv.at[side], where)

    def a0_pass():
        await_recv(hold, h_recv)
        for side, where in enumerate((YPOS, YNEG)):
            ref = a0_block(0, NEAR[1 - side], 2 * side, 2)
            send(hold.at[side], ref, t_send, t_recv.at[2], where)

    def piece(q, dx, dy, lo=0, hi=PIECE):
        base = (plus(x, dx) * 2 + c) * PIECE
        return g.at[q, plus(y, dy), pl.ds(pl.multiple_of(base + lo, 16), hi - lo), :]

    def hop(q, depth, where, dx, dy, lo=0, hi=PIECE):
        ref = piece(q, dx, dy, lo, hi)
        send(ref, ref, g_send.at[q], g_recv.at[q, depth], where)

    def mate(q, *offsets, last=0):
        for dx, dy in offsets:
            ref = piece(q, dx, dy)
            send(ref, ref, g_send.at[q], d_recv.at[last, q], MATE)

    def arrived(q, depth):
        rows = (4096, 2 * (BLK + 2 * (PIECE - XP)) + 2 * (BLK + 2 * XP), 4096, PIECE)[depth]
        await_recv(g.at[q, 0, pl.ds(0, rows), :], g_recv.at[q, depth])

    def g1(q):
        for where in (XPOS, XNEG, YPOS, YNEG):
            hop(q, 0, where, 0, 0)
        mate(q, (0, 0))

    def g2(q):
        arrived(q, 0)
        hop(q, 1, XPOS, 3, 0, XM, YP)
        hop(q, 1, YPOS, 0, 3, XM, YP)
        for lo, hi in ((0, XM), (YP, PIECE)):
            hop(q, 1, XNEG, 1, 0, lo, hi)
            hop(q, 1, YNEG, 0, 1, lo, hi)
        for d in (1, 3):
            for where in (XPOS, XNEG):
                hop(q, 1, where, 0, d, XP, PIECE)
            for where in (YPOS, YNEG):
                hop(q, 1, where, d, 0, 0, XP)
        mate(q, (1, 0), (3, 0), (0, 1), (0, 3))

    def g3(q):
        arrived(q, 1)
        for where in (XPOS, XNEG):
            hop(q, 2, where, 0, 2, XP, PIECE)
        for where in (YPOS, YNEG):
            hop(q, 2, where, 2, 0, 0, XP)
        for d in (1, 3):
            hop(q, 2, XPOS, 3, d, XP, YP)
            hop(q, 2, XNEG, 1, d, YP, PIECE)
            hop(q, 2, YPOS, d, 3, XM, XP)
            hop(q, 2, YNEG, d, 1, 0, XM)
        mate(q, (2, 0), (0, 2), (1, 1), (1, 3), (3, 1), (3, 3))

    def g4(q):
        arrived(q, 2)
        hop(q, 3, XPOS, 3, 2, XP, YP)
        hop(q, 3, XNEG, 1, 2, YP, PIECE)
        hop(q, 3, YPOS, 2, 3, XM, XP)
        hop(q, 3, YNEG, 2, 1, 0, XM)
        mate(q, (1, 2), (3, 2), (2, 1), (2, 3))

    def g5(q):
        arrived(q, 3)
        mate(q, (2, 2), last=1)

    def g_most(q):
        await_recv(g.at[q, pl.ds(0, 3), pl.ds(0, 5 * PIECE)], d_recv.at[0, q])

    def g_whole(q):
        await_recv(g.at[q, 0, pl.ds(0, PIECE)], d_recv.at[1, q])

    def g_rows(nq, start, n):
        return jnp.concatenate([g[nq, t, pl.ds(start, n), :] for t in range(Q)], axis=1)

    def c1_part(q, zz):
        lhs = jnp.concatenate(
            [a[0, zz, cc, qr, yy] for cc in range(2) for qr in range(Q) for yy in range(2)], axis=1
        )
        acc1[q] += jnp.dot(lhs, g_rows(q, pl.multiple_of(zz * PLANE, PLANE), PLANE), preferred_element_type=F32)

    def c1_most(q):
        def step(i, carry):
            c1_part(q, plus(x, i + lax.div(i, 2)))
            return carry

        acc1[q] = jnp.zeros((ROWS, BLK), F32)
        lax.fori_loop(0, 3, step, 0)

    def c1_rest(q):
        c1_part(q, plus(x, 2))

    def square_sum(ref, q):
        v = ref[q]
        return jnp.sum(v * v, axis=0, keepdims=True)

    def sum_first(s1, i, k):
        me = x * 2 + c
        for dx in FAR_FIRST:
            for dc in range(2):
                if dx + dc:
                    send(s1.at[i, me], s1.at[i, me], r_send.at[0, k], r_recv1.at[k], dev(dx=dx, dc=dc))

    def sum_second(s1, s2, i, k):
        await_recv(s1.at[i, pl.ds(0, 7)], r_recv1.at[k])
        s2[i, y] = jnp.sum(s1[i], axis=0)
        for dy in FAR_FIRST[:3]:
            send(s2.at[i, y], s2.at[i, y], r_send.at[1, k], r_recv2.at[k], dev(dy=dy))

    def sum_last(s2, i, k):
        await_recv(s2.at[i, pl.ds(0, 3)], r_recv2.at[k])

    me_plane = y * 8 + x * 2 + c

    def to_plane(source, dst, ssem, rsem):
        for dy in FAR_FIRST:
            for dx in FAR_FIRST:
                for dc in range(2):
                    if dx + dy + dc:
                        send(source(dy), dst.at[me_plane], ssem, rsem, dev(dx=dx, dy=dy, dc=dc))

    def c1_sums(q):
        if q in DIRECT:
            k = DIRECT.index(q)
            s4[k, me_plane] = square_sum(acc1, q)
            to_plane(lambda dy: s4.at[k, me_plane], s4.at[k], p_send.at[k], p_recv.at[k])
        else:
            s1a[q, x * 2 + c] = square_sum(acc1, q)
            sum_first(s1a, q, q)

    def c1_second(q):
        if q not in DIRECT:
            sum_second(s1a, s2a, q, q)

    def c1_scale(q):
        if q in DIRECT:
            k = DIRECT.index(q)
            await_recv(s4.at[k, pl.ds(0, 31)], p_recv.at[k])
            return N / jnp.sum(s4[k], axis=0)
        sum_last(s2a, q, q)
        return N / jnp.sum(s2a[q], axis=0)

    def a1_chunk(dz, q, lo=0, n=2):
        return a.at[1, plus(z, dz), pl.ds(lo, n), q]

    def a1_spread(q):
        scale = c1_scale(q)
        for t in range(Q):
            v = acc1[q, :, pl.ds(t * LANE, LANE)]
            a[1, z, t // 2, q, t % 2] = (v * v * scale[:, t * LANE : t * LANE + LANE]).astype(BF)
        for half in range(2):
            for where, n in ((ZPOS, half), (ZNEG, 1 - half)):
                send(a1_chunk(0, q, n, 1), a1_chunk(0, q, n, 1), a1_send, a1_recv.at[half, q], where)

    def a1_relay(q):
        await_recv(a.at[1, 0, :, 0], a1_recv.at[0, q])
        send(a1_chunk(3, q, 0, 1), a1_chunk(3, q, 0, 1), a1_send, a1_recv2.at[q], ZPOS)
        send(a1_chunk(1, q, 1, 1), a1_chunk(1, q, 1, 1), a1_send, a1_recv2.at[q], ZNEG)

    def c2(q, dz, first=False):
        zz = plus(z, dz)
        lhs = jnp.concatenate([a[1, zz, cc, q, yy] for cc in range(2) for yy in range(2)], axis=1)
        base = pl.multiple_of(zz * PLANE, PLANE)
        for nq in range(Q):
            rhs = jnp.concatenate([g_rows(nq, base + cc * PIECE + q * ROWS, ROWS) for cc in range(2)], axis=0)
            prod = jnp.dot(lhs, rhs, preferred_element_type=F32)
            acc2[nq] = prod if first else acc2[nq] + prod

    def c2_near(q):
        await_recv(a.at[1, 0, :, 0], a1_recv.at[1, q])
        for dz in NEAR:
            c2(q, dz)

    def c2_far(q):
        await_recv(a.at[1, 0, :, 0], a1_recv2.at[q])
        c2(q, 2)

    def c2_sums():
        for q in range(Q):
            s1b[0, x * 2 + c, :, pl.ds(q * BLK, BLK)] = square_sum(acc2, q)
        sum_first(s1b, 0, 4)

    def c2_second():
        sum_second(s1b, s2b, 0, 4)

    def early_part(dz, lo=0, n=2):
        return early.at[plus(z, dz), pl.ds(lo, n)]

    def early_spread():
        for half in range(2):
            for where, n in ((ZPOS, half), (ZNEG, 1 - half)):
                src = acc2.at[pl.ds(2 * n, 2), pl.ds(0, EARLY), :]
                send(src, early_part(0, 2 * n), e_send, e_recv.at[half], where)

    def early_relay():
        await_recv(early.at[0], e_recv.at[0])
        send(early_part(3), early_part(3), e_send, e_recv.at[2], ZPOS)
        send(early_part(1, 2), early_part(1, 2), e_send, e_recv.at[2], ZNEG)

    def a2_scales():
        sum_last(s2b, 0, Q)
        scales[z] = N / jnp.sum(s2b[0], axis=0)
        for dz in (2, 1, 3):
            send(scales.at[z], scales.at[z], v_send, v_recv, dev(dz=dz))

    def scaled(v, zz, q, t, rows):
        lanes = pl.ds(q * BLK + t * LANE, LANE)
        a[2, zz, t // 2, q, t % 2, rows, :] = (v * v * scales[zz, :, lanes]).astype(BF)

    def early_scale(dz):
        zz = plus(z, dz)
        for q in range(Q):
            for t in range(Q):
                scaled(early[zz, q, :, pl.ds(t * LANE, LANE)], zz, q, t, pl.ds(0, EARLY))

    def early_near():
        await_recv(early.at[0], e_recv.at[1])
        await_recv(scales.at[pl.ds(0, 3)], v_recv)
        for dz in NEAR:
            early_scale(dz)
        for half in range(2):
            c3_first(Q0, half)

    def early_far():
        await_recv(early.at[0], e_recv.at[2])
        early_scale(2)
        c3_far(Q0)

    def a2_rows(dz, p, lo=0, n=2):
        start, rows = ROWS3[p]
        return a.at[2, plus(z, dz), pl.ds(lo, n), :, :, pl.ds(start, rows), :]

    def a2_scale(p):
        rows = pl.ds(*ROWS3[p])
        for q in range(Q):
            for t in range(Q):
                scaled(acc2[q, rows, pl.ds(t * LANE, LANE)], z, q, t, rows)

    def a2_spread(p):
        for half in range(2):
            for where, n in ((ZPOS, half), (ZNEG, 1 - half)):
                send(a2_rows(0, p, n, 1), a2_rows(0, p, n, 1), a2_send.at[p], a2_recv.at[half, p], where)

    def a2_relay(p):
        start, rows = ROWS3[p]
        await_recv(a.at[2, 0, :, :, :, pl.ds(start, rows), :], a2_recv.at[0, p])
        send(a2_rows(3, p, 0, 1), a2_rows(3, p, 0, 1), a2_send.at[p], a2_recv2.at[p], ZPOS)
        send(a2_rows(1, p, 1, 1), a2_rows(1, p, 1, 1), a2_send.at[p], a2_recv2.at[p], ZNEG)

    def c3_part(zz, start, rows, nq, halves=(0, 1)):
        lhs = jnp.concatenate(
            [a[2, zz, cc, qr, yy, pl.ds(start, rows), :] for cc in halves for qr in range(Q) for yy in range(2)],
            axis=1,
        )
        depth = len(halves) * PIECE
        base = pl.multiple_of(zz * PLANE + halves[0] * PIECE, PIECE)
        return jnp.dot(lhs, g_rows(nq, base, depth), preferred_element_type=F32)

    def c3_own():
        def step(nq, carry):
            acc1[nq] = c3_part(z, 0, ROWS, nq)
            return carry

        lax.fori_loop(0, 4, step, 0)

    def c3_first(p, half=0):
        start, rows = ROWS3[p]

        def step(nq, carry):
            part = c3_part(plus(z, 3), start, rows, nq, (half,))
            acc1[nq, pl.ds(start, rows), :] += part + c3_part(plus(z, 1), start, rows, nq, (1 - half,))
            return carry

        lax.fori_loop(0, Q, step, 0)

    def c3_near(p):
        start, rows = ROWS3[p]
        await_recv(a.at[2, 0, :, :, :, pl.ds(start, rows), :], a2_recv.at[1, p])
        c3_first(p, 1)

    def c3_far(p):
        start, rows = ROWS3[p]
        if p:
            await_recv(a.at[2, 0, :, :, :, pl.ds(start, rows), :], a2_recv2.at[p])
        for nq in range(Q):
            v = acc1[nq, pl.ds(start, rows), :] + c3_part(plus(z, 2), start, rows, nq)
            v = v * v
            part = jnp.sum(v, axis=0, keepdims=True)
            here = pl.ds(nq * LANE, LANE)
            for t in range(Q):
                cut = slice(t * LANE, t * LANE + LANE)
                moved[t, pl.ds(start, rows), here] = v[:, cut]
                if p == 0:
                    s3[t, :, here] = part[:, cut]
                else:
                    s3[t, :, here] += part[:, cut]
        if p == Q3:
            c3_sums()
        for dy in (2, 1, 3):
            send(
                moved.at[plus(y, dy), pl.ds(start, rows), :],
                got.at[y, pl.ds(start, rows), :],
                o_send, o_recv, dev(dy=dy),
            )

    def c3_sums():
        to_plane(lambda dy: s3.at[plus(y, dy)], s4.at[2], p_send.at[2], p_recv.at[2])
        s4[2, me_plane] = s3[y]

    def finish():
        await_recv(s4.at[2, pl.ds(0, 31)], p_recv.at[2])
        scale = N / jnp.sum(s4[2], axis=0)
        out_ref[y] = moved[y] * scale
        await_recv(got.at[pl.ds(0, 3)], o_recv)
        for dy in (1, 2, 3):
            t = plus(y, dy)
            out_ref[t] = got[t] * scale

    g1(Q0)
    cast_init()
    cast_graph(Q1)
    g1(Q1)
    a0_exchange()
    g2(Q0)
    g2(Q1)
    cast_graph(Q2)
    g1(Q2)
    a0_spread(0, (0,))
    a0_wait_near()
    a0_spread(1, NEAR)
    g3(Q0)
    a0_pass()
    g3(Q1)
    a0_relay(1, NEAR)
    g4(Q0)
    a0_relay(0, (0,))
    g2(Q2)
    a0_wait_far()
    a0_spread(2, (2,))
    g4(Q1)
    cast_graph(Q3)
    g1(Q3)
    g_most(Q0)
    g5(Q0)
    a0_relay(2, (2,))
    a0_done()
    g_whole(Q0)
    c1_most(Q0)
    c1_rest(Q0)
    c1_sums(Q0)
    g5(Q1)
    g_most(Q1)
    g3(Q2)
    g_whole(Q1)
    c1_most(Q1)
    c1_second(Q0)
    c1_rest(Q1)
    c1_sums(Q1)
    g2(Q3)
    a1_spread(Q0)
    c1_second(Q1)
    g4(Q2)
    g3(Q3)
    a1_relay(Q0)
    g5(Q2)
    a1_spread(Q1)
    g_whole(Q2)
    g_most(Q2)
    c1_most(Q2)
    c1_rest(Q2)
    c1_sums(Q2)
    g4(Q3)
    c1_second(Q2)
    a1_relay(Q1)
    g_most(Q3)
    c1_most(Q3)
    g5(Q3)
    a1_spread(Q2)
    g_whole(Q3)
    c1_rest(Q3)
    c1_sums(Q3)
    c1_second(Q3)
    a1_relay(Q2)
    c2(Q0, 0, True)
    a1_spread(Q3)
    c2(Q1, 0)
    c2_near(Q0)
    c2_far(Q0)
    c2(Q2, 0)
    c2_near(Q1)
    a1_relay(Q3)
    c2_far(Q1)
    c2_near(Q2)
    c2_near(Q3)
    c2(Q3, 0)
    c2_far(Q2)
    c2_far(Q3)
    early_spread()
    c2_sums()
    c2_second()
    early_relay()
    a2_scales()
    a2_scale(Q1)
    a2_spread(Q1)
    for p in (Q0, Q2, Q3):
        a2_scale(p)
    c3_own()
    early_near()
    a2_relay(Q1)
    a2_spread(Q2)
    early_far()
    c3_first(Q1)
    c3_near(Q1)
    c3_far(Q1)
    a2_relay(Q2)
    a2_spread(Q3)
    c3_first(Q2)
    c3_near(Q2)
    c3_far(Q2)
    a2_relay(Q3)
    c3_first(Q3)
    c3_near(Q3)
    c3_far(Q3)
    finish()

    for q in range(Q):
        await_send(g.at[q, :, pl.ds(0, 7936), :], g_send.at[q])
    await_send(stage, t_send)
    await_send(a.at[0, pl.ds(0, 3)], az_send)
    await_send(a.at[1, pl.ds(0, 3)], a1_send)
    await_send(early.at[pl.ds(0, 3)], e_send)
    await_send(scales.at[pl.ds(0, 3)], v_send)
    for p, (start, rows) in enumerate(ROWS3[1:], 1):
        await_send(a.at[2, pl.ds(0, 3), :, :, :, pl.ds(start, rows), :], a2_send.at[p])
    for s1, s2, base, n in ((s1a, s2a, 0, Q2), (s1b, s2b, Q, 1)):
        for i in range(n):
            await_send(s1.at[i, pl.ds(0, 7)], r_send.at[0, base + i])
            await_send(s2.at[i, pl.ds(0, 3)], r_send.at[1, base + i])
    await_send(got.at[pl.ds(0, 3)], o_send)
    for k in range(3):
        await_send(s4.at[k, pl.ds(0, 31)], p_send.at[k])


def solution(mesh):
    block_spec = P(("graph", "row"), "col")
    hbm = pl.BlockSpec(memory_space=pl.ANY)
    dma = pltpu.SemaphoreType.DMA

    def device_step(init_blk, graph_blk):
        result = pl.pallas_call(
            mcl_kernel,
            out_shape=pltpu.VMEM((Q, ROWS, BLK), F32),
            in_specs=[hbm, hbm],
            out_specs=pl.BlockSpec(memory_space=pltpu.VMEM),
            scratch_shapes=[
                pltpu.VMEM((Q, ROWS, BLK), F32), pltpu.VMEM((Q, ROWS, BLK), F32),
                pltpu.VMEM((4, 4, N, LANE), BF),
                pltpu.VMEM((3, 4, 2, 4, 2, ROWS, LANE), BF),
                pltpu.VMEM((4, 4, ROWS, LANE), BF),
                pltpu.VMEM((2, 2, ROWS, LANE), BF),
                pltpu.VMEM((4, ROWS, BLK), F32),
                pltpu.VMEM((4, ROWS, BLK), F32),
                pltpu.VMEM((4, 8, 1, BLK), F32),
                pltpu.VMEM((4, 4, 1, BLK), F32),
                pltpu.VMEM((1, 8, 1, PLANE), F32),
                pltpu.VMEM((1, 4, 1, PLANE), F32),
                pltpu.VMEM((Q, 1, BLK), F32), pltpu.VMEM((3, 32, 1, BLK), F32),
                pltpu.VMEM((Q, Q, EARLY, BLK), F32), pltpu.VMEM((Q, 1, PLANE), F32),
                dma((Q,)), dma((Q, Q)), dma((2, Q)),
                dma(()), dma((3,)), dma(()),
                dma(()), dma((3,)), dma(()),
                dma(()), dma((2, Q)), dma((Q,)),
                dma((Q,)), dma((2, Q)), dma((Q,)),
                dma((2, 5)), dma((5,)), dma((5,)),
                dma(()), dma((3,)), dma(()), dma(()),
                dma(()), dma(()),
                dma((3,)), dma((3,)), dma((Q + 1, Q)),
            ],
            compiler_params=pltpu.CompilerParams(
                collective_id=0, has_side_effects=True, vmem_limit_bytes=VMEM_BYTES
            ),
        )(init_blk, graph_blk)
        return result.reshape(init_blk.shape)

    return jax.shard_map(device_step, mesh=mesh, in_specs=(block_spec, block_spec), out_specs=block_spec, check_vma=False)
```

```python
import functools

import jax
import jax.numpy as jnp
from jax import lax
from jax.experimental import pallas as pl
from jax.experimental.pallas import tpu as pltpu
from jax.sharding import PartitionSpec as P

MESH = pl.DeviceIdType.MESH
VMEM_BYTES = 58 << 20
BF = jnp.bfloat16
F32 = jnp.float32
N = 8192
PLANE, PIECE, BLK, ROWS, LANE = 2048, 1024, 512, 256, 128
Q = 4
Q0, Q1, Q2, Q3 = range(Q)
NEAR = (1, 3)
FAR_FIRST = (2, 1, 3, 0)
DIRECT = (Q2, Q3)
XM, XP, YP = 224, 448, 736
EARLY = 32
ROWS3 = ((0, EARLY), (32, 112), (144, 64), (208, 48))


def mcl_kernel(
    init_hbm, graph_hbm, out_ref,
    moved, got,
    g, a, stage, hold, acc1, acc2, s1a, s2a, s1b, s2b, s3, s4, early, scales,
    g_send, g_recv, d_recv, t_send, t_recv, h_recv, az_send, az_recv, az2_recv,
    a1_send, a1_recv, a1_recv2, a2_send, a2_recv, a2_recv2,
    r_send, r_recv1, r_recv2, e_send, e_recv, v_send, v_recv, o_send, o_recv, p_send, p_recv, i_sem,
):
    col, row = lax.axis_index("col"), lax.axis_index("row")
    z, y = lax.div(col, 4), lax.rem(col, 4)
    x, c = lax.div(row, 2), lax.rem(row, 2)

    def plus(v, d):
        return lax.rem(v + d, 4)

    def dev(dx=0, dy=0, dz=0, dc=0):
        return {"col": plus(z, dz) * 4 + plus(y, dy), "row": plus(x, dx) * 2 + lax.rem(c + dc, 2)}

    XPOS, XNEG, YPOS, YNEG = dev(dx=1), dev(dx=3), dev(dy=1), dev(dy=3)
    ZPOS, ZNEG, MATE = dev(dz=1), dev(dz=3), dev(dc=1)

    def send(src, dst, ssem, rsem, device):
        pltpu.make_async_remote_copy(
            src_ref=src, dst_ref=dst, send_sem=ssem, recv_sem=rsem, device_id=device, device_id_type=MESH
        ).start()

    def await_recv(ref, sem):
        pltpu.make_async_remote_copy(
            src_ref=ref, dst_ref=ref, send_sem=sem, recv_sem=sem, device_id=MATE, device_id_type=MESH
        ).wait_recv()

    def await_send(ref, sem):
        pltpu.make_async_remote_copy(
            src_ref=ref, dst_ref=ref, send_sem=sem, recv_sem=sem, device_id=MATE, device_id_type=MESH
        ).wait_send()

    barrier = pltpu.get_barrier_semaphore()
    peers = [XPOS, XNEG, YPOS, YNEG, ZPOS, ZNEG, MATE]
    for peer in peers:
        pl.semaphore_signal(barrier, inc=1, device_id=peer, device_id_type=MESH)

    init_ref, graph_ref = moved, got
    copies = []
    for q in range(Q + 1):
        lanes = pl.ds(q * LANE, LANE)
        parts = []
        for t in range(Q):
            rows = pl.ds(t * ROWS, ROWS)
            if q == Q:
                parts.append(pltpu.make_async_copy(init_hbm.at[rows], init_ref.at[t], i_sem.at[q, t]))
            else:
                parts.append(
                    pltpu.make_async_copy(graph_hbm.at[rows, lanes], graph_ref.at[t, :, lanes], i_sem.at[q, t])
                )
        copies.append(parts)
    for q in (Q0, Q, Q1, Q2, Q3):
        for copy in copies[q]:
            copy.start()

    def cast_graph(q):
        for copy in copies[q]:
            copy.wait()
        base = pl.multiple_of((x * 2 + c) * PIECE, PIECE)
        lanes = pl.ds(q * LANE, LANE)
        for qr in range(Q):
            for yy in range(2):
                block = graph_ref[yy * 2 + qr // 2, pl.ds(qr % 2 * LANE, LANE), lanes]
                g[q, y, pl.ds(base + qr * ROWS + yy * LANE, LANE), :] = block.astype(BF)

    def cast_init():
        for copy in copies[Q]:
            copy.wait()
        for q in range(Q):
            a[0, z, lax.div(y, 2), q, lax.rem(y, 2)] = init_ref[y, :, pl.ds(q * LANE, LANE)].astype(BF)
        for t in range(Q):
            for q in range(Q):
                stage[t, q] = init_ref[t, :, pl.ds(q * LANE, LANE)].astype(BF)

    cast_graph(Q0)
    pl.semaphore_wait(barrier, len(peers))

    def a0_block(dz, dy, lo=0, n=4):
        yy = plus(y, dy)
        return a.at[0, plus(z, dz), lax.div(yy, 2), pl.ds(lo, n), lax.rem(yy, 2)]

    def a0_spread(group, dys):
        for dy in dys:
            for where in (ZPOS, ZNEG):
                send(a0_block(0, dy), a0_block(0, dy), az_send, az_recv.at[group], where)

    def a0_wait_near():
        for k in range(2):
            await_recv(stage.at[0], t_recv.at[k])

    def a0_wait_far():
        await_recv(stage.at[0], t_recv.at[2])

    def a0_done():
        await_recv(a.at[0, 0], az2_recv)

    def a0_relay(group, dys):
        await_recv(a.at[0, 0, pl.ds(0, len(dys))], az_recv.at[group])
        for dy in dys:
            send(a0_block(3, dy, 0, 2), a0_block(3, dy, 0, 2), az_send, az2_recv, ZPOS)
            send(a0_block(1, dy, 2, 2), a0_block(1, dy, 2, 2), az_send, az2_recv, ZNEG)

    def a0_exchange():
        far = plus(y, 2)
        for side, where in enumerate((YPOS, YNEG)):
            send(stage.at[far, pl.ds(2 * side, 2)], hold.at[side], t_send, h_recv, where)
            send(stage.at[plus(y, NEAR[side])], a0_block(0, 0), t_send, t_recv.at[side], where)

    def a0_pass():
        await_recv(hold, h_recv)
        for side, where in enumerate((YPOS, YNEG)):
            ref = a0_block(0, NEAR[1 - side], 2 * side, 2)
            send(hold.at[side], ref, t_send, t_recv.at[2], where)

    def piece(q, dx, dy, lo=0, hi=PIECE):
        base = (plus(x, dx) * 2 + c) * PIECE
        return g.at[q, plus(y, dy), pl.ds(pl.multiple_of(base + lo, 16), hi - lo), :]

    def hop(q, depth, where, dx, dy, lo=0, hi=PIECE):
        ref = piece(q, dx, dy, lo, hi)
        send(ref, ref, g_send.at[q], g_recv.at[q, depth], where)

    def mate(q, *offsets, last=0):
        for dx, dy in offsets:
            ref = piece(q, dx, dy)
            send(ref, ref, g_send.at[q], d_recv.at[last, q], MATE)

    def arrived(q, depth):
        rows = (4096, 2 * (BLK + 2 * (PIECE - XP)) + 2 * (BLK + 2 * XP), 4096, PIECE)[depth]
        await_recv(g.at[q, 0, pl.ds(0, rows), :], g_recv.at[q, depth])

    def g1(q):
        for where in (XPOS, XNEG, YPOS, YNEG):
            hop(q, 0, where, 0, 0)
        mate(q, (0, 0))

    def g2(q):
        arrived(q, 0)
        hop(q, 1, XPOS, 3, 0, XM, YP)
        hop(q, 1, YPOS, 0, 3, XM, YP)
        for lo, hi in ((0, XM), (YP, PIECE)):
            hop(q, 1, XNEG, 1, 0, lo, hi)
            hop(q, 1, YNEG, 0, 1, lo, hi)
        for d in (1, 3):
            for where in (XPOS, XNEG):
                hop(q, 1, where, 0, d, XP, PIECE)
            for where in (YPOS, YNEG):
                hop(q, 1, where, d, 0, 0, XP)
        mate(q, (1, 0), (3, 0), (0, 1), (0, 3))

    def g3(q):
        arrived(q, 1)
        for where in (XPOS, XNEG):
            hop(q, 2, where, 0, 2, XP, PIECE)
        for where in (YPOS, YNEG):
            hop(q, 2, where, 2, 0, 0, XP)
        for d in (1, 3):
            hop(q, 2, XPOS, 3, d, XP, YP)
            hop(q, 2, XNEG, 1, d, YP, PIECE)
            hop(q, 2, YPOS, d, 3, XM, XP)
            hop(q, 2, YNEG, d, 1, 0, XM)
        mate(q, (2, 0), (0, 2), (1, 1), (1, 3), (3, 1), (3, 3))

    def g4(q):
        arrived(q, 2)
        hop(q, 3, XPOS, 3, 2, XP, YP)
        hop(q, 3, XNEG, 1, 2, YP, PIECE)
        hop(q, 3, YPOS, 2, 3, XM, XP)
        hop(q, 3, YNEG, 2, 1, 0, XM)
        mate(q, (1, 2), (3, 2), (2, 1), (2, 3))

    def g5(q):
        arrived(q, 3)
        mate(q, (2, 2), last=1)

    def g_most(q):
        await_recv(g.at[q, pl.ds(0, 3), pl.ds(0, 5 * PIECE)], d_recv.at[0, q])

    def g_whole(q):
        await_recv(g.at[q, 0, pl.ds(0, PIECE)], d_recv.at[1, q])

    def g_rows(nq, start, n):
        return jnp.concatenate([g[nq, t, pl.ds(start, n), :] for t in range(Q)], axis=1)

    def c1_part(q, zz):
        lhs = jnp.concatenate(
            [a[0, zz, cc, qr, yy] for cc in range(2) for qr in range(Q) for yy in range(2)], axis=1
        )
        acc1[q] += jnp.dot(lhs, g_rows(q, pl.multiple_of(zz * PLANE, PLANE), PLANE), preferred_element_type=F32)

    def c1_most(q):
        def step(i, carry):
            c1_part(q, plus(x, i + lax.div(i, 2)))
            return carry

        acc1[q] = jnp.zeros((ROWS, BLK), F32)
        lax.fori_loop(0, 3, step, 0)

    def c1_rest(q):
        c1_part(q, plus(x, 2))

    def square_sum(ref, q):
        v = ref[q]
        return jnp.sum(v * v, axis=0, keepdims=True)

    def sum_first(s1, i, k):
        me = x * 2 + c
        for dx in FAR_FIRST:
            for dc in range(2):
                if dx + dc:
                    send(s1.at[i, me], s1.at[i, me], r_send.at[0, k], r_recv1.at[k], dev(dx=dx, dc=dc))

    def sum_second(s1, s2, i, k):
        await_recv(s1.at[i, pl.ds(0, 7)], r_recv1.at[k])
        s2[i, y] = jnp.sum(s1[i], axis=0)
        for dy in FAR_FIRST[:3]:
            send(s2.at[i, y], s2.at[i, y], r_send.at[1, k], r_recv2.at[k], dev(dy=dy))

    def sum_last(s2, i, k):
        await_recv(s2.at[i, pl.ds(0, 3)], r_recv2.at[k])

    me_plane = y * 8 + x * 2 + c

    def to_plane(source, dst, ssem, rsem):
        for dy in FAR_FIRST:
            for dx in FAR_FIRST:
                for dc in range(2):
                    if dx + dy + dc:
                        send(source(dy), dst.at[me_plane], ssem, rsem, dev(dx=dx, dy=dy, dc=dc))

    def c1_sums(q):
        if q in DIRECT:
            k = DIRECT.index(q)
            s4[k, me_plane] = square_sum(acc1, q)
            to_plane(lambda dy: s4.at[k, me_plane], s4.at[k], p_send.at[k], p_recv.at[k])
        else:
            s1a[q, x * 2 + c] = square_sum(acc1, q)
            sum_first(s1a, q, q)

    def c1_second(q):
        if q not in DIRECT:
            sum_second(s1a, s2a, q, q)

    def c1_scale(q):
        if q in DIRECT:
            k = DIRECT.index(q)
            await_recv(s4.at[k, pl.ds(0, 31)], p_recv.at[k])
            return N / jnp.sum(s4[k], axis=0)
        sum_last(s2a, q, q)
        return N / jnp.sum(s2a[q], axis=0)

    def a1_chunk(dz, q, lo=0, n=2):
        return a.at[1, plus(z, dz), pl.ds(lo, n), q]

    def a1_spread(q):
        scale = c1_scale(q)
        for t in range(Q):
            v = acc1[q, :, pl.ds(t * LANE, LANE)]
            a[1, z, t // 2, q, t % 2] = (v * v * scale[:, t * LANE : t * LANE + LANE]).astype(BF)
        for half in range(2):
            for where, n in ((ZPOS, half), (ZNEG, 1 - half)):
                send(a1_chunk(0, q, n, 1), a1_chunk(0, q, n, 1), a1_send, a1_recv.at[half, q], where)

    def a1_relay(q):
        await_recv(a.at[1, 0, :, 0], a1_recv.at[0, q])
        send(a1_chunk(3, q, 0, 1), a1_chunk(3, q, 0, 1), a1_send, a1_recv2.at[q], ZPOS)
        send(a1_chunk(1, q, 1, 1), a1_chunk(1, q, 1, 1), a1_send, a1_recv2.at[q], ZNEG)

    def c2(q, dz, first=False):
        zz = plus(z, dz)
        lhs = jnp.concatenate([a[1, zz, cc, q, yy] for cc in range(2) for yy in range(2)], axis=1)
        base = pl.multiple_of(zz * PLANE, PLANE)
        for nq in range(Q):
            rhs = jnp.concatenate([g_rows(nq, base + cc * PIECE + q * ROWS, ROWS) for cc in range(2)], axis=0)
            prod = jnp.dot(lhs, rhs, preferred_element_type=F32)
            acc2[nq] = prod if first else acc2[nq] + prod

    def c2_near(q):
        await_recv(a.at[1, 0, :, 0], a1_recv.at[1, q])
        for dz in NEAR:
            c2(q, dz)

    def c2_far(q):
        await_recv(a.at[1, 0, :, 0], a1_recv2.at[q])
        c2(q, 2)

    def c2_sums():
        for q in range(Q):
            s1b[0, x * 2 + c, :, pl.ds(q * BLK, BLK)] = square_sum(acc2, q)
        sum_first(s1b, 0, 4)

    def c2_second():
        sum_second(s1b, s2b, 0, 4)

    def early_part(dz, lo=0, n=2):
        return early.at[plus(z, dz), pl.ds(lo, n)]

    def early_spread():
        for half in range(2):
            for where, n in ((ZPOS, half), (ZNEG, 1 - half)):
                src = acc2.at[pl.ds(2 * n, 2), pl.ds(0, EARLY), :]
                send(src, early_part(0, 2 * n), e_send, e_recv.at[half], where)

    def early_relay():
        await_recv(early.at[0], e_recv.at[0])
        send(early_part(3), early_part(3), e_send, e_recv.at[2], ZPOS)
        send(early_part(1, 2), early_part(1, 2), e_send, e_recv.at[2], ZNEG)

    def a2_scales():
        sum_last(s2b, 0, Q)
        scales[z] = N / jnp.sum(s2b[0], axis=0)
        for dz in (2, 1, 3):
            send(scales.at[z], scales.at[z], v_send, v_recv, dev(dz=dz))

    def scaled(v, zz, q, t, rows):
        lanes = pl.ds(q * BLK + t * LANE, LANE)
        a[2, zz, t // 2, q, t % 2, rows, :] = (v * v * scales[zz, :, lanes]).astype(BF)

    def early_scale(dz):
        zz = plus(z, dz)
        for q in range(Q):
            for t in range(Q):
                scaled(early[zz, q, :, pl.ds(t * LANE, LANE)], zz, q, t, pl.ds(0, EARLY))

    def early_near():
        await_recv(early.at[0], e_recv.at[1])
        await_recv(scales.at[pl.ds(0, 3)], v_recv)
        for dz in NEAR:
            early_scale(dz)
        for half in range(2):
            c3_first(Q0, half)

    def early_far():
        await_recv(early.at[0], e_recv.at[2])
        early_scale(2)
        c3_far(Q0)

    def a2_rows(dz, p, lo=0, n=2):
        start, rows = ROWS3[p]
        return a.at[2, plus(z, dz), pl.ds(lo, n), :, :, pl.ds(start, rows), :]

    def a2_scale(p):
        rows = pl.ds(*ROWS3[p])
        for q in range(Q):
            for t in range(Q):
                scaled(acc2[q, rows, pl.ds(t * LANE, LANE)], z, q, t, rows)

    def a2_spread(p):
        for half in range(2):
            for where, n in ((ZPOS, half), (ZNEG, 1 - half)):
                send(a2_rows(0, p, n, 1), a2_rows(0, p, n, 1), a2_send.at[p], a2_recv.at[half, p], where)

    def a2_relay(p):
        start, rows = ROWS3[p]
        await_recv(a.at[2, 0, :, :, :, pl.ds(start, rows), :], a2_recv.at[0, p])
        send(a2_rows(3, p, 0, 1), a2_rows(3, p, 0, 1), a2_send.at[p], a2_recv2.at[p], ZPOS)
        send(a2_rows(1, p, 1, 1), a2_rows(1, p, 1, 1), a2_send.at[p], a2_recv2.at[p], ZNEG)

    def c3_part(zz, start, rows, nq, halves=(0, 1)):
        lhs = jnp.concatenate(
            [a[2, zz, cc, qr, yy, pl.ds(start, rows), :] for cc in halves for qr in range(Q) for yy in range(2)],
            axis=1,
        )
        depth = len(halves) * PIECE
        base = pl.multiple_of(zz * PLANE + halves[0] * PIECE, PIECE)
        return jnp.dot(lhs, g_rows(nq, base, depth), preferred_element_type=F32)

    def c3_own():
        def step(nq, carry):
            acc1[nq] = c3_part(z, 0, ROWS, nq)
            return carry

        lax.fori_loop(0, 4, step, 0)

    def c3_first(p, half=0):
        start, rows = ROWS3[p]

        def step(nq, carry):
            part = c3_part(plus(z, 3), start, rows, nq, (half,))
            acc1[nq, pl.ds(start, rows), :] += part + c3_part(plus(z, 1), start, rows, nq, (1 - half,))
            return carry

        lax.fori_loop(0, Q, step, 0)

    def c3_near(p):
        start, rows = ROWS3[p]
        await_recv(a.at[2, 0, :, :, :, pl.ds(start, rows), :], a2_recv.at[1, p])
        c3_first(p, 1)

    def c3_far(p):
        start, rows = ROWS3[p]
        if p:
            await_recv(a.at[2, 0, :, :, :, pl.ds(start, rows), :], a2_recv2.at[p])
        for nq in range(Q):
            v = acc1[nq, pl.ds(start, rows), :] + c3_part(plus(z, 2), start, rows, nq)
            v = v * v
            part = jnp.sum(v, axis=0, keepdims=True)
            here = pl.ds(nq * LANE, LANE)
            for t in range(Q):
                cut = slice(t * LANE, t * LANE + LANE)
                moved[t, pl.ds(start, rows), here] = v[:, cut]
                if p == 0:
                    s3[t, :, here] = part[:, cut]
                else:
                    s3[t, :, here] += part[:, cut]
        if p == Q3:
            c3_sums()
        for dy in (2, 1, 3):
            send(
                moved.at[plus(y, dy), pl.ds(start, rows), :],
                got.at[y, pl.ds(start, rows), :],
                o_send, o_recv, dev(dy=dy),
            )

    def c3_sums():
        to_plane(lambda dy: s3.at[plus(y, dy)], s4.at[2], p_send.at[2], p_recv.at[2])
        s4[2, me_plane] = s3[y]

    def finish():
        await_recv(s4.at[2, pl.ds(0, 31)], p_recv.at[2])
        scale = N / jnp.sum(s4[2], axis=0)
        out_ref[y] = moved[y] * scale
        await_recv(got.at[pl.ds(0, 3)], o_recv)
        for dy in (1, 2, 3):
            t = plus(y, dy)
            out_ref[t] = got[t] * scale

    g1(Q0)
    cast_init()
    cast_graph(Q1)
    g1(Q1)
    a0_exchange()
    g2(Q0)
    g2(Q1)
    cast_graph(Q2)
    g1(Q2)
    a0_spread(0, (0,))
    a0_wait_near()
    a0_spread(1, NEAR)
    g3(Q0)
    a0_pass()
    g3(Q1)
    a0_relay(1, NEAR)
    g4(Q0)
    a0_relay(0, (0,))
    g2(Q2)
    a0_wait_far()
    a0_spread(2, (2,))
    g4(Q1)
    cast_graph(Q3)
    g1(Q3)
    g_most(Q0)
    g5(Q0)
    a0_relay(2, (2,))
    a0_done()
    g_whole(Q0)
    c1_most(Q0)
    c1_rest(Q0)
    c1_sums(Q0)
    g5(Q1)
    g_most(Q1)
    g3(Q2)
    g_whole(Q1)
    c1_most(Q1)
    c1_second(Q0)
    c1_rest(Q1)
    c1_sums(Q1)
    g2(Q3)
    a1_spread(Q0)
    c1_second(Q1)
    g4(Q2)
    g3(Q3)
    a1_relay(Q0)
    g5(Q2)
    a1_spread(Q1)
    g_whole(Q2)
    g_most(Q2)
    c1_most(Q2)
    c1_rest(Q2)
    c1_sums(Q2)
    g4(Q3)
    c1_second(Q2)
    a1_relay(Q1)
    g_most(Q3)
    c1_most(Q3)
    g5(Q3)
    a1_spread(Q2)
    g_whole(Q3)
    c1_rest(Q3)
    c1_sums(Q3)
    c1_second(Q3)
    a1_relay(Q2)
    c2(Q0, 0, True)
    a1_spread(Q3)
    c2(Q1, 0)
    c2_near(Q0)
    c2_far(Q0)
    c2(Q2, 0)
    c2_near(Q1)
    a1_relay(Q3)
    c2_far(Q1)
    c2_near(Q2)
    c2_near(Q3)
    c2(Q3, 0)
    c2_far(Q2)
    c2_far(Q3)
    early_spread()
    c2_sums()
    c2_second()
    early_relay()
    a2_scales()
    a2_scale(Q1)
    a2_spread(Q1)
    for p in (Q0, Q2, Q3):
        a2_scale(p)
    c3_own()
    early_near()
    a2_relay(Q1)
    a2_spread(Q2)
    early_far()
    c3_first(Q1)
    c3_near(Q1)
    c3_far(Q1)
    a2_relay(Q2)
    a2_spread(Q3)
    c3_first(Q2)
    c3_near(Q2)
    c3_far(Q2)
    a2_relay(Q3)
    c3_first(Q3)
    c3_near(Q3)
    c3_far(Q3)
    finish()

    for q in range(Q):
        await_send(g.at[q, :, pl.ds(0, 7936), :], g_send.at[q])
    await_send(stage, t_send)
    await_send(a.at[0, pl.ds(0, 3)], az_send)
    await_send(a.at[1, pl.ds(0, 3)], a1_send)
    await_send(early.at[pl.ds(0, 3)], e_send)
    await_send(scales.at[pl.ds(0, 3)], v_send)
    for p, (start, rows) in enumerate(ROWS3[1:], 1):
        await_send(a.at[2, pl.ds(0, 3), :, :, :, pl.ds(start, rows), :], a2_send.at[p])
    for s1, s2, base, n in ((s1a, s2a, 0, Q2), (s1b, s2b, Q, 1)):
        for i in range(n):
            await_send(s1.at[i, pl.ds(0, 7)], r_send.at[0, base + i])
            await_send(s2.at[i, pl.ds(0, 3)], r_send.at[1, base + i])
    await_send(got.at[pl.ds(0, 3)], o_send)
    for k in range(3):
        await_send(s4.at[k, pl.ds(0, 31)], p_send.at[k])


def solution(mesh):
    block_spec = P(("graph", "row"), "col")
    hbm = pl.BlockSpec(memory_space=pl.ANY)
    dma = pltpu.SemaphoreType.DMA

    def device_step(init_blk, graph_blk):
        result = pl.pallas_call(
            mcl_kernel,
            out_shape=pltpu.VMEM((Q, ROWS, BLK), F32),
            in_specs=[hbm, hbm],
            out_specs=pl.BlockSpec(memory_space=pltpu.VMEM),
            scratch_shapes=[
                pltpu.VMEM((Q, ROWS, BLK), F32), pltpu.VMEM((Q, ROWS, BLK), F32),
                pltpu.VMEM((4, 4, N, LANE), BF),
                pltpu.VMEM((3, 4, 2, 4, 2, ROWS, LANE), BF),
                pltpu.VMEM((4, 4, ROWS, LANE), BF),
                pltpu.VMEM((2, 2, ROWS, LANE), BF),
                pltpu.VMEM((4, ROWS, BLK), F32),
                pltpu.VMEM((4, ROWS, BLK), F32),
                pltpu.VMEM((4, 8, 1, BLK), F32),
                pltpu.VMEM((4, 4, 1, BLK), F32),
                pltpu.VMEM((1, 8, 1, PLANE), F32),
                pltpu.VMEM((1, 4, 1, PLANE), F32),
                pltpu.VMEM((Q, 1, BLK), F32), pltpu.VMEM((3, 32, 1, BLK), F32),
                pltpu.VMEM((Q, Q, EARLY, BLK), F32), pltpu.VMEM((Q, 1, PLANE), F32),
                dma((Q,)), dma((Q, Q)), dma((2, Q)),
                dma(()), dma((3,)), dma(()),
                dma(()), dma((3,)), dma(()),
                dma(()), dma((2, Q)), dma((Q,)),
                dma((Q,)), dma((2, Q)), dma((Q,)),
                dma((2, 5)), dma((5,)), dma((5,)),
                dma(()), dma((3,)), dma(()), dma(()),
                dma(()), dma(()),
                dma((3,)), dma((3,)), dma((Q + 1, Q)),
            ],
            compiler_params=pltpu.CompilerParams(
                collective_id=0, has_side_effects=True, vmem_limit_bytes=VMEM_BYTES
            ),
        )(init_blk, graph_blk)
        return result.reshape(init_blk.shape)

    return jax.shard_map(device_step, mesh=mesh, in_specs=(block_spec, block_spec), out_specs=block_spec, check_vma=False)
```
